32 devices in a mesh: gx: 8 (over z, x), ma: 4 (over y, core).
Axes of the slice: x: 2, y: 2, z: 4, core: 2. Of those that a mesh axis runs over, the one named last changes fastest.
Arguments:
- recorded: float32 [4096, 128, 128], P('ma', 'gx'), may hold values from -51 to 51
- kernel: bfloat16 [2, 8, 4096, 4096], P(None, 'gx', 'ma'), may hold values from -1 to 1
- freq_bins: int32 [8], replicated, may hold values from 1 to 63
- window_start: int32 [4096, 128], P('ma', 'gx'), may hold values from 0 to 31
- window_stop: int32 [4096, 128], P('ma', 'gx'), may hold values from 97 to 128
Outputs:
- solution: float32 [4096, 128, 128], P('ma', 'gx')
- residual: float32 [4096, 128, 128], P('ma', 'gx')
- direction: float32 [4096, 128, 128], P('ma', 'gx')
The draws below stay inside these ranges and needn't reach their ends.
All inputs are finite; a program needn't handle non-finite values.
Results may differ from the reference program's by a relative error of at most 0.015.
Values may be sent and summed in bfloat16 or wider, within the bound.
A program may use at most 128 MiB of HBM per device.

```python
import math
import jax
import jax.numpy as jnp
from jax import lax

NR = 4096
NV = 4096
NT = 128
NS = 128
RAMP = 8
NF = 8


def draw_recorded(key, part):
    key_source = jax.random.fold_in(key, 11)
    key_receiver = jax.random.fold_in(key, 12)
    key_noise = jax.random.fold_in(key, 13)
    key_colour = jax.random.fold_in(key, 15)
    rising = 3.0 ** (jnp.arange(NS, dtype=jnp.float32) / NS)
    source_scale = rising * jnp.exp(jax.random.uniform(key_source, (NS,), jnp.float32) * math.log(10.0))
    receiver_scale = jnp.exp(jax.random.uniform(key_receiver, (NR,), jnp.float32) * math.log(4.0))
    base = jnp.clip(jax.random.normal(key_noise, (NR, NS, NT), jnp.float32), -3.0, 3.0)
    colour = jax.random.uniform(key_colour, (NS,), jnp.float32, -0.9, 0.9)
    delayed = jnp.roll(base, 1, axis=2)
    coloured = (base + colour[None, :, None] * delayed) / jnp.sqrt(1.0 + colour * colour)[None, :, None]
    return 0.1 * coloured * receiver_scale[:, None, None] * source_scale[None, :, None]


def draw_kernel(key, part):
    key_level = jax.random.fold_in(key, 21)
    key_entry = jax.random.fold_in(key, 22)
    level = jnp.exp(jax.random.uniform(key_level, (NF,), jnp.float32, math.log(0.3), math.log(3.0)))
    scale = level[None, :, None, None] / math.sqrt(2.0 * NV)
    entries = jnp.clip(jax.random.normal(key_entry, (2, NF, NR, NV), jnp.float32), -4.0, 4.0)
    return (entries * scale).astype(jnp.bfloat16)


def place_ends(values, own_key, smallest, largest):
    place = [jax.random.randint(jax.random.fold_in(own_key, axis), (), 0, length) for axis, length in enumerate(values.shape)]
    main_axis = values.shape.index(max(values.shape))
    next_to = place[:main_axis] + [(place[main_axis] + 1) % values.shape[main_axis]] + place[main_axis + 1:]
    return values.at[tuple(place)].set(smallest).at[tuple(next_to)].set(largest)


def setup_inputs(seed: int = 0) -> dict:
    keys = jax.random.split(jax.random.key(seed), 6)
    recorded = draw_recorded(jax.random.fold_in(keys[5], 71), 0)
    kernel = draw_kernel(jax.random.fold_in(keys[5], 71), 0)
    freq_bins = place_ends(jax.random.randint(keys[2], (NF,), 1, NT // 2), jax.random.fold_in(keys[2], 1), 1, (NT // 2) - 1).astype(jnp.int32)
    window_start = place_ends(jax.random.randint(keys[3], (NR, NS), 0, NT // 4), jax.random.fold_in(keys[3], 1), 0, (NT // 4) - 1).astype(jnp.int32)
    window_stop = place_ends(jax.random.randint(keys[4], (NR, NS), 3 * NT // 4 + 1, NT + 1), jax.random.fold_in(keys[4], 1), 3 * NT // 4 + 1, NT).astype(jnp.int32)
    return dict(recorded=recorded, kernel=kernel, freq_bins=freq_bins, window_start=window_start, window_stop=window_stop)


epsilon = 1e-06

def phase_table(freq_bins):
    samples = jnp.arange(NT, dtype=jnp.int32)
    angles = (freq_bins[:, None] * samples[None, :] % NT).astype(jnp.float32) * (2.0 * math.pi / NT)
    return jnp.stack([jnp.cos(angles), -jnp.sin(angles)]) * math.sqrt(2.0 / NT)

def taper_weights(window_start, window_stop):
    samples = jnp.arange(NT, dtype=jnp.float32)
    rising = jnp.clip((samples[None, None, :] - window_start[:, :, None].astype(jnp.float32) + 1.0) / RAMP, 0.0, 1.0)
    falling = jnp.clip((window_stop[:, :, None].astype(jnp.float32) - samples[None, None, :]) / RAMP, 0.0, 1.0)
    return rising * falling

def forward_transform(traces, table):
    return jnp.einsum('ast,cft->facs', traces, table, precision=lax.Precision.HIGHEST).astype(jnp.bfloat16)

def inverse_transform(spectra, table):
    return jnp.einsum('facs,cft->ast', spectra.astype(jnp.float32), table, precision=lax.Precision.HIGHEST)

def forward_apply(model_traces, kernel, table, weights):
    spectra = forward_transform(model_traces, table)

    def per_freq(index):
        gains = lax.dynamic_index_in_dim(kernel, index, 1, keepdims=False)
        incoming = lax.dynamic_index_in_dim(spectra, index, 0, keepdims=False)
        real_in = incoming[:, 0, :]
        imag_in = incoming[:, 1, :]
        real_out = jnp.dot(gains[0], real_in, preferred_element_type=jnp.float32) - jnp.dot(gains[1], imag_in, preferred_element_type=jnp.float32)
        imag_out = jnp.dot(gains[0], imag_in, preferred_element_type=jnp.float32) + jnp.dot(gains[1], real_in, preferred_element_type=jnp.float32)
        return jnp.stack([real_out, imag_out], 1).astype(jnp.bfloat16)
    result = lax.map(per_freq, jnp.arange(NF, dtype=jnp.int32))
    return weights * inverse_transform(result, table)

def adjoint_apply(data_traces, kernel, table, weights):
    spectra = forward_transform(weights * data_traces, table)

    def per_freq(index):
        gains = lax.dynamic_index_in_dim(kernel, index, 1, keepdims=False)
        incoming = lax.dynamic_index_in_dim(spectra, index, 0, keepdims=False)
        real_in = incoming[:, 0, :]
        imag_in = incoming[:, 1, :]
        real_out = jnp.dot(gains[0].T, real_in, preferred_element_type=jnp.float32) + jnp.dot(gains[1].T, imag_in, preferred_element_type=jnp.float32)
        imag_out = jnp.dot(gains[0].T, imag_in, preferred_element_type=jnp.float32) - jnp.dot(gains[1].T, real_in, preferred_element_type=jnp.float32)
        return jnp.stack([real_out, imag_out], 1).astype(jnp.bfloat16)
    result = lax.map(per_freq, jnp.arange(NF, dtype=jnp.int32))
    return inverse_transform(result, table)

def reference(recorded, kernel, freq_bins, window_start, window_stop):
    table = phase_table(freq_bins)
    weights = taper_weights(window_start, window_stop)
    gradient = adjoint_apply(recorded, kernel, table, weights)
    norm_start = jnp.sum(gradient * gradient)
    data_image = forward_apply(gradient, kernel, table, weights)
    norm_data = jnp.sum(data_image * data_image)
    step_size = norm_start / (norm_data + epsilon)
    solution = step_size * gradient
    residual = recorded - step_size * data_image
    gradient_new = adjoint_apply(residual, kernel, table, weights)
    norm_final = jnp.sum(gradient_new * gradient_new)
    direction = gradient_new + norm_final / (norm_start + epsilon) * gradient
    return (solution, residual, direction)
```

```python
import functools
import math

import jax
import jax.numpy as jnp
from jax import lax
from jax.experimental import pallas as pl
from jax.experimental.pallas import tpu as pltpu
from jax.sharding import PartitionSpec as P

RAMP = 8
MESH = pl.DeviceIdType.MESH

epsilon = 1e-06


def phase_table(freq_bins, length):
    samples = jnp.arange(length, dtype=jnp.int32)
    angles = (freq_bins[:, None] * samples[None, :] % length).astype(jnp.float32) * (
        2.0 * math.pi / length
    )
    return jnp.stack([jnp.cos(angles), -jnp.sin(angles)], 1) * math.sqrt(2.0 / length)


def taper_weights(window_start, window_stop, length):
    samples = jnp.arange(length, dtype=jnp.float32)
    rising = jnp.clip(
        (samples[None, None, :] - window_start[:, :, None].astype(jnp.float32) + 1.0) / RAMP,
        0.0,
        1.0,
    )
    falling = jnp.clip(
        (window_stop[:, :, None].astype(jnp.float32) - samples[None, None, :]) / RAMP, 0.0, 1.0
    )
    return rising * falling


def exchange_kernel(n, x_ref, o_ref, send_sem, recv_sem, own_sem):
    me = lax.axis_index("gx")
    barrier = pltpu.get_barrier_semaphore()
    for k in range(1, n):
        pl.semaphore_signal(
            barrier, inc=1, device_id={"gx": lax.rem(me + k, n)}, device_id_type=MESH
        )
    own = pltpu.make_async_copy(x_ref.at[me], o_ref.at[me], own_sem)
    own.start()
    pl.semaphore_wait(barrier, n - 1)
    copies = []
    for k in range(1, n):
        peer = lax.rem(me + k, n)
        copy = pltpu.make_async_remote_copy(
            src_ref=x_ref.at[peer],
            dst_ref=o_ref.at[me],
            send_sem=send_sem.at[k],
            recv_sem=recv_sem.at[k],
            device_id={"gx": peer},
            device_id_type=MESH,
        )
        copy.start()
        copies.append(copy)
    own.wait()
    for copy in copies:
        copy.wait()


def exchange(x, n, number):
    return pl.pallas_call(
        functools.partial(exchange_kernel, n),
        out_shape=jax.ShapeDtypeStruct(x.shape, x.dtype),
        in_specs=[pl.BlockSpec(memory_space=pltpu.VMEM)],
        out_specs=pl.BlockSpec(memory_space=pltpu.VMEM),
        scratch_shapes=[
            pltpu.SemaphoreType.DMA((n,)),
            pltpu.SemaphoreType.DMA((n,)),
            pltpu.SemaphoreType.DMA,
        ],
        compiler_params=pltpu.CompilerParams(collective_id=number, has_side_effects=True),
        name=f"exchange{number}",
    )(x)


def total_kernel(outer, inner, x_ref, o_ref, held, send_sem, recv_sem):
    n = outer * inner
    me = lax.axis_index("gx") * inner + lax.axis_index("ma")
    barrier = pltpu.get_barrier_semaphore()

    def place(k):
        peer = lax.rem(me + k, n)
        return (peer // inner, lax.rem(peer, inner))

    for k in range(1, n):
        pl.semaphore_signal(barrier, inc=1, device_id=place(k), device_id_type=MESH)
    pl.semaphore_wait(barrier, n - 1)
    copies = []
    for k in range(1, n):
        copy = pltpu.make_async_remote_copy(
            src_ref=x_ref,
            dst_ref=held.at[me],
            send_sem=send_sem.at[k],
            recv_sem=recv_sem.at[k],
            device_id=place(k),
            device_id_type=MESH,
        )
        copy.start()
        copies.append(copy)
    held[me] = x_ref[...]
    for copy in copies:
        copy.wait()
    o_ref[...] = jnp.sum(held[...], axis=0)


def total(x, outer, inner, number):
    n = outer * inner
    return pl.pallas_call(
        functools.partial(total_kernel, outer, inner),
        out_shape=jax.ShapeDtypeStruct(x.shape, x.dtype),
        in_specs=[pl.BlockSpec(memory_space=pltpu.VMEM)],
        out_specs=pl.BlockSpec(memory_space=pltpu.VMEM),
        scratch_shapes=[
            pltpu.VMEM((n,) + x.shape, x.dtype),
            pltpu.SemaphoreType.DMA((n,)),
            pltpu.SemaphoreType.DMA((n,)),
        ],
        compiler_params=pltpu.CompilerParams(collective_id=number, has_side_effects=True),
        name=f"total{number}",
    )(x)


def pairs(n, bit):
    return [(i, i ^ bit) for i in range(n)]


def scatter_sum(partial, n):
    rows, block = partial.shape[1:]
    me = lax.axis_index("ma")
    held = partial
    bit = 1
    while bit < n:
        own = (me // bit) % 2
        parts = held.reshape(-1, 2, rows, block)
        keep = lax.dynamic_index_in_dim(parts, own, 1, keepdims=False)
        send = lax.dynamic_index_in_dim(parts, 1 - own, 1, keepdims=False)
        got = lax.ppermute(send, "ma", pairs(n, bit))
        held = (keep.astype(jnp.float32) + got.astype(jnp.float32)).astype(jnp.bfloat16)
        bit *= 2
    return held.reshape(rows, block)


def gather_all(x, n):
    rows, block = x.shape
    me = lax.axis_index("ma")
    held = x.reshape(rows, 1, block)
    bit = n // 2
    while bit >= 1:
        own = (me // bit) % 2
        got = lax.ppermute(held, "ma", pairs(n, bit))
        first = jnp.where(own == 0, held, got)
        second = jnp.where(own == 0, got, held)
        held = jnp.stack([first, second], 2).reshape(rows, -1, block)
        bit //= 2
    return held.reshape(rows, n * block)


def to_spectra(traces, table):
    freqs = table.shape[0]
    flat = table.reshape(2 * freqs, table.shape[2]).astype(jnp.bfloat16)
    out = jnp.einsum(
        "ast,kt->ksa", traces.astype(jnp.bfloat16), flat, preferred_element_type=jnp.float32
    ).astype(jnp.bfloat16)
    return out.reshape(freqs, 2 * out.shape[1], out.shape[2])


def to_traces(spectra, table):
    freqs, double, points = spectra.shape
    sources = double // 2
    length = table.shape[2]
    depth = freqs * double
    across = spectra.reshape(depth, points).T
    owner = jnp.arange(depth, dtype=jnp.int32) % sources
    mask = (owner[None, :] == jnp.arange(sources, dtype=jnp.int32)[:, None]).astype(jnp.bfloat16)
    spread = (across[:, None, :] * mask[None]).reshape(points * sources, depth)
    tall = jnp.repeat(table.reshape(2 * freqs, length).astype(jnp.bfloat16), sources, axis=0)
    out = jnp.dot(spread, tall, preferred_element_type=jnp.float32)
    return out.reshape(points, sources, length)


def by_frequency(arrived, n):
    sources = arrived.shape[1] // 2
    points = arrived.shape[2]
    return arrived.reshape(n, 2, sources, points).transpose(1, 0, 2, 3).reshape(2, -1, points)


def by_source(spectra, n):
    points = spectra.shape[2]
    sources = spectra.shape[1] // n
    return spectra.reshape(2, n, sources, points).transpose(1, 0, 2, 3).reshape(n, -1, points)


def adjoint_kernel(d_ref, k_ref, o_ref):
    half = d_ref.shape[0] // 2
    data = d_ref[...]
    first = jnp.dot(data, k_ref[0], preferred_element_type=jnp.float32)
    second = jnp.dot(data, k_ref[1], preferred_element_type=jnp.float32)
    o_ref[0, :half] = (first[:half] + second[half:]).astype(o_ref.dtype)
    o_ref[0, half:] = (first[half:] - second[:half]).astype(o_ref.dtype)


def adjoint_product(data, flat_kernel, inner):
    sources, rows = data.shape[1], data.shape[2]
    columns = flat_kernel.shape[1]
    block = columns // inner
    tile = min(512, block)
    per_block = block // tile
    partial = pl.pallas_call(
        adjoint_kernel,
        grid=(columns // tile,),
        out_shape=jax.ShapeDtypeStruct((inner, 2 * sources, block), jnp.bfloat16),
        in_specs=[
            pl.BlockSpec((2 * sources, rows), lambda j: (0, 0)),
            pl.BlockSpec((2, rows, tile), lambda j: (0, 0, j)),
        ],
        out_specs=pl.BlockSpec(
            (1, 2 * sources, tile), lambda j: (j // per_block, 0, j % per_block)
        ),
        compiler_params=pltpu.CompilerParams(vmem_limit_bytes=60 * 1024 * 1024),
        cost_estimate=pl.CostEstimate(
            flops=8 * sources * rows * columns,
            bytes_accessed=4 * rows * columns + 4 * sources * (rows + columns),
            transcendentals=0,
        ),
        name="adjoint",
    )(data.reshape(2 * sources, rows), flat_kernel.reshape(2, rows, columns))
    return scatter_sum(partial, inner).reshape(2, sources, block)


def final_kernel(
    sums_ref, rec_ref, win_ref, g_ref, d_ref, h_ref, tall_ref, mask_ref, pick_ref,
    sol_ref, res_ref, dir_ref,
):
    tile, sources, length = rec_ref.shape
    norm_start, norm_data = sums_ref[0, 0], sums_ref[1, 0]
    cross, norm_change = sums_ref[2, 0], sums_ref[3, 0]
    step_size = norm_start / (norm_data + epsilon)
    norm_final = norm_start - 2.0 * step_size * cross + step_size * step_size * norm_change
    ratio = norm_final / (norm_start + epsilon)
    tall = tall_ref[...]

    def rows(values, mask):
        return (values[:, None, :] * mask[None]).reshape(tile * sources, -1).astype(jnp.bfloat16)

    def traces(ref):
        spread = rows(ref[...].astype(jnp.float32), mask_ref[...])
        out = jnp.dot(spread, tall, preferred_element_type=jnp.float32)
        return out.reshape(tile, sources, length)

    gradient = traces(g_ref)
    change = traces(h_ref)
    sol_ref[...] = step_size * gradient
    dir_ref[...] = (gradient - step_size * change) + ratio * gradient
    window = win_ref[...]
    ones = jnp.ones((window.shape[1], length), jnp.bfloat16)
    shape = (tile, sources, length)
    start = jnp.dot(rows(window, pick_ref[0]), ones, preferred_element_type=jnp.float32)
    stop = jnp.dot(rows(window, pick_ref[1]), ones, preferred_element_type=jnp.float32)
    samples = lax.broadcasted_iota(jnp.int32, shape, 2).astype(jnp.float32)
    rising = jnp.clip((samples - start.reshape(shape) + 1.0) / RAMP, 0.0, 1.0)
    falling = jnp.clip((stop.reshape(shape) - samples) / RAMP, 0.0, 1.0)
    image = (rising * falling) * traces(d_ref)
    res_ref[...] = rec_ref[...] - step_size * image


def final_step(sums, recorded, window_start, window_stop, returned, arrived, changed, table):
    points, sources, length = recorded.shape
    depth = returned.shape[0] * returned.shape[1]
    tile = min(128, points)

    def across(x):
        return x.reshape(depth, points).T

    place = jnp.arange(sources, dtype=jnp.int32)
    owner = jnp.arange(depth, dtype=jnp.int32) % sources
    mask = (owner[None, :] == place[:, None]).astype(jnp.float32)
    column = jnp.arange(2 * sources, dtype=jnp.int32)
    pick = jnp.stack(
        [column[None, :] == place[:, None], column[None, :] == place[:, None] + sources]
    ).astype(jnp.float32)
    tall = jnp.repeat(table.reshape(-1, length).astype(jnp.bfloat16), sources, axis=0)
    window = jnp.concatenate([window_start, window_stop], 1).astype(jnp.float32)
    whole3 = pl.BlockSpec((tile, sources, length), lambda i: (i, 0, 0))
    strip = pl.BlockSpec((tile, depth), lambda i: (i, 0))
    return pl.pallas_call(
        final_kernel,
        grid=(points // tile,),
        out_shape=[jax.ShapeDtypeStruct(recorded.shape, jnp.float32)] * 3,
        in_specs=[
            pl.BlockSpec(memory_space=pltpu.SMEM),
            whole3,
            pl.BlockSpec((tile, 2 * sources), lambda i: (i, 0)),
            strip,
            strip,
            strip,
            pl.BlockSpec((depth, length), lambda i: (0, 0)),
            pl.BlockSpec((sources, depth), lambda i: (0, 0)),
            pl.BlockSpec((2, sources, 2 * sources), lambda i: (0, 0, 0)),
        ],
        out_specs=[whole3] * 3,
        compiler_params=pltpu.CompilerParams(vmem_limit_bytes=48 * 1024 * 1024),
        cost_estimate=pl.CostEstimate(
            flops=8 * points * sources * depth * length,
            bytes_accessed=16 * points * sources * length,
            transcendentals=0,
        ),
        name="final",
    )(sums, recorded, window, across(returned), across(arrived), across(changed), tall, mask, pick)


def forward_product(model, flat_kernel, inner):
    sources = model.shape[1]
    incoming = gather_all(model.reshape(2 * sources, -1), inner)
    product = lax.dot_general(
        incoming, flat_kernel, (((1,), (1,)), ((), ())), preferred_element_type=jnp.float32
    )
    half = flat_kernel.shape[0] // 2
    real_part = product[:sources, :half] - product[sources:, half:]
    imaginary = product[sources:, :half] + product[:sources, half:]
    return jnp.stack([real_part, imaginary], 0).astype(jnp.bfloat16)


RECORDED, RETURNED, IMAGED, SECOND, CHANGED, MIXED = range(6)


def iteration_kernel(
    outer, inner, mixing, rec_ref, ker_ref, win_ref, tall_ref, across_ref, same_ref,
    returned_ref, imaged_ref, changed_ref, sums_ref,
    traces, gains, window, spread, gather, tapered, first_out, first_in, second_out, second_in,
    total, product, image_out, core_out, core_in, line_out, line_in, model, summed, normal,
    mixed_out, stats, stats_in, stats_all,
    trace_sem, gain_sem, out_sem, in_sem, core_out_sem, core_in_sem, line_out_sem, line_in_sem,
    share_out_sem, share_in_sem, stats_out_sem, stats_in_sem,
):
    n = outer
    sources, points, length = traces.shape
    chunks, _, double, width = first_out.shape
    pieces, piece = model.shape[1], model.shape[4]
    depth = n * double
    block = pieces * piece
    f32, bf16 = jnp.float32, jnp.bfloat16
    me, mine = lax.axis_index("gx"), lax.axis_index("ma")
    core = mine + 1 - 2 * lax.rem(mine, 2)
    line = lax.rem(mine + 2, 4)
    corner = lax.rem(core + 2, 4)

    def loop(start, stop, body):
        def step(i, carry):
            body(i)
            return carry

        lax.fori_loop(start, stop, step, 0)

    def part(i):
        return pl.ds(pl.multiple_of(i * width, width), width)

    def trace_copy(i, s):
        return pltpu.make_async_copy(
            rec_ref.at[part(i), s], traces.at[s, part(i)], trace_sem.at[i, s]
        )

    def gain_copy(i):
        return pltpu.make_async_copy(
            ker_ref.at[:, part(i)], gains.at[:, part(i)], gain_sem.at[i]
        )

    def across(number, src, dst, i, k, peer, slot):
        return pltpu.make_async_remote_copy(
            src_ref=src.at[i, peer],
            dst_ref=dst.at[i, slot],
            send_sem=out_sem.at[number, i, k],
            recv_sem=in_sem.at[number, i, k],
            device_id={"gx": peer},
            device_id_type=MESH,
        )

    def send_all(number, src, dst, i):
        def body(k):
            peer = lax.rem(me + k, n)
            across(number, src, dst, i, k, peer, me).start()

        loop(1, n, body)
        dst[i, me] = src[i, me]

    def receive_all(number, src, dst, i):
        def body(k):
            peer = lax.rem(me + n - k, n)
            across(number, src, dst, i, k, peer, peer).wait_recv()

        loop(1, n, body)

    def finish_all(number, src, dst, count):
        def outside(i):
            def body(k):
                peer = lax.rem(me + k, n)
                across(number, src, dst, i, k, peer, me).wait_send()

            loop(1, n, body)

        loop(0, count, outside)

    def core_copy(stage, which, p):
        return pltpu.make_async_remote_copy(
            src_ref=core_out.at[stage, which, p],
            dst_ref=core_in.at[stage, which, p],
            send_sem=core_out_sem.at[stage, which, p],
            recv_sem=core_in_sem.at[stage, which, p],
            device_id={"ma": core},
            device_id_type=MESH,
        )

    def line_copy(stage, p):
        return pltpu.make_async_remote_copy(
            src_ref=line_out.at[stage, p],
            dst_ref=line_in.at[stage, p],
            send_sem=line_out_sem.at[stage, p],
            recv_sem=line_in_sem.at[stage, p],
            device_id={"ma": line},
            device_id_type=MESH,
        )

    def share_copy(which, p):
        source, slot, peer = ((0, 1, core), (0, 2, line), (2, 3, core))[which]
        return pltpu.make_async_remote_copy(
            src_ref=model.at[source, p],
            dst_ref=model.at[slot, p],
            send_sem=share_out_sem.at[which, p],
            recv_sem=share_in_sem.at[which, p],
            device_id={"ma": peer},
            device_id_type=MESH,
        )

    barrier = pltpu.get_barrier_semaphore()

    def greet(k):
        pl.semaphore_signal(
            barrier, inc=1, device_id={"gx": lax.rem(me + k, n)}, device_id_type=MESH
        )

    loop(1, n, greet)
    for peer in (core, line):
        pl.semaphore_signal(barrier, inc=1, device_id={"ma": peer}, device_id_type=MESH)

    def load(i):
        loop(0, sources, lambda s: trace_copy(i, s).start())

    loop(0, chunks, load)
    for s in range(sources):
        rows = lax.broadcasted_iota(jnp.int32, (depth, length), 0)
        spread[:, s * length : (s + 1) * length] = jnp.where(
            lax.rem(rows, sources) == s, tall_ref[...], 0.0
        ).astype(bf16)
        columns = lax.broadcasted_iota(jnp.int32, (length, depth), 1)
        gather[s * length : (s + 1) * length] = jnp.where(
            lax.rem(columns, sources) == s, across_ref[...], 0.0
        ).astype(bf16)
    stats[...] = jnp.zeros_like(stats)
    pl.semaphore_wait(barrier, n + 1)

    samples = lax.broadcasted_iota(jnp.int32, (length, width), 0).astype(f32) * (1.0 / RAMP)

    def span(s):
        return pl.ds(pl.multiple_of(s * length, length), length)

    def transform(out, i):
        result = jnp.dot(spread[...], tapered[...], preferred_element_type=f32)
        out[i] = result.astype(bf16).reshape(n, double, width)

    def record(i):
        loop(0, sources, lambda s: trace_copy(i, s).wait())
        gain_copy(i).start()

        def taper(s):
            rising = jnp.clip(samples + win_ref[pl.ds(s, 1), part(i)], 0.0, 1.0)
            falling = jnp.clip(win_ref[pl.ds(sources + s, 1), part(i)] - samples, 0.0, 1.0)
            weight = rising * falling
            window[i, span(s)] = weight.astype(bf16)
            tapered[span(s)] = (weight * traces[s, part(i)].T).astype(bf16)

        loop(0, sources, taper)
        transform(first_out, i)
        send_all(RECORDED, first_out, first_in, i)

    loop(0, chunks, record)

    def turned(values, sign):
        half = double // 2
        low, high = values[:, :half], values[:, half:]
        pair = [high, -low] if sign > 0 else [-high, low]
        return jnp.concatenate(pair, 1).reshape(depth, values.shape[2])

    def adjoint_part(held, i, columns):
        data = held[i]
        return jnp.dot(
            data.reshape(depth, width), gains[0, part(i), columns], preferred_element_type=f32
        ) + jnp.dot(turned(data, 1), gains[1, part(i), columns], preferred_element_type=f32)

    def accumulate(held, i, first):
        def body(j):
            columns = pl.ds(pl.multiple_of(j * block, block), block)
            update = adjoint_part(held, i, columns)
            total[:, columns] = update if first else total[:, columns] + update

        loop(0, inner, body)

    def adjoint(number, src, held, stage, use):
        for i in range(chunks - 1):
            receive_all(number, src, held, i)
            if stage == 0:
                gain_copy(i).wait()
            accumulate(held, i, i == 0)
        last = chunks - 1
        receive_all(number, src, held, last)
        if stage == 0:
            gain_copy(last).wait()

        def tile(where, p):
            columns = pl.ds(pl.multiple_of(where * block + p * piece, piece), piece)
            update = adjoint_part(held, last, columns)
            return update if chunks == 1 else total[:, columns] + update

        def pack(values):
            return values.astype(bf16).reshape(n, double, piece)

        def to_core(which, where):
            def body(p):
                core_out[stage, which, p] = pack(tile(where, p))
                core_copy(stage, which, p).start()

            loop(0, pieces, body)

        def from_core(which, p):
            core_copy(stage, which, p).wait_recv()
            return core_in[stage, which, p].reshape(depth, piece).astype(f32)

        def to_line(p):
            values = tile(line, p)
            line_out[stage, p] = pack(values + from_core(0, p))
            line_copy(stage, p).start()

        def own(p):
            values = tile(mine, p)
            values = values + from_core(1, p)
            line_copy(stage, p).wait_recv()
            values = values + line_in[stage, p].reshape(depth, piece).astype(f32)
            use(p, pack(values))

        to_core(0, corner)
        loop(0, pieces, to_line)
        to_core(1, core)
        loop(0, pieces, own)

    def folded(values):
        rows, columns = values.shape
        parts = values.reshape(rows // 8, 8, columns).sum(0)
        out = parts[:, :128]
        for j in range(1, columns // 128):
            out = out + parts[:, j * 128 : (j + 1) * 128]
        return out

    def flat(values):
        return values.reshape(depth, values.shape[2]).astype(f32)

    def forward_part(slot, where, p, rows):
        columns = pl.ds(pl.multiple_of(where * block + p * piece, piece), piece)
        values = model[slot, p]
        dims = (((1,), (1,)), ((), ()))
        return lax.dot_general(
            gains[0, rows, columns],
            values.reshape(depth, piece),
            dims,
            preferred_element_type=f32,
        ) + lax.dot_general(
            gains[1, rows, columns], turned(values, -1), dims, preferred_element_type=f32
        )

    def forward(slot, where, p, first=False):
        tile_rows = 2 * width if chunks % 2 == 0 else width

        def body(i):
            rows = pl.ds(pl.multiple_of(i * tile_rows, tile_rows), tile_rows)
            update = forward_part(slot, where, p, rows)
            product[rows] = update if first else product[rows] + update

        loop(0, points // tile_rows, body)

    def share(p):
        share_copy(1, p).start()
        share_copy(0, p).start()

    if mixing:

        def keep(p, values):
            summed[p] = values
            send_all(RETURNED, summed, returned_ref, p)

        adjoint(RECORDED, first_out, first_in, 0, keep)

        def mix(p):
            receive_all(RETURNED, summed, returned_ref, p)
            arrived = returned_ref[p].reshape(depth, piece)
            values = jnp.dot(same_ref[...], arrived, preferred_element_type=f32)
            mixed_out[p] = values.astype(bf16).reshape(n, double, piece)
            send_all(MIXED, mixed_out, model.at[0], p)

        loop(0, pieces, mix)

        def spread_out(p):
            receive_all(MIXED, mixed_out, model.at[0], p)
            share(p)

        loop(0, pieces, spread_out)
    else:

        def keep(p, values):
            model[0, p] = values
            share(p)
            send_all(RETURNED, model.at[0], returned_ref, p)
            held = flat(values)
            stats[0] += folded(held * held)

        adjoint(RECORDED, first_out, first_in, 0, keep)

    product[...] = jnp.zeros_like(product)
    loop(0, pieces, lambda p: forward(0, mine, p))

    def from_share(p):
        share_copy(0, p).wait_recv()
        forward(1, core, p)

    loop(0, pieces, from_share)

    def relay(p):
        share_copy(1, p).wait_recv()
        share_copy(2, p).start()

    def from_line(p):
        relay(p)
        forward(2, line, p)
        share_copy(2, p).wait_recv()
        forward(3, corner, p)

    loop(0, pieces - 1, from_line)
    final = pieces - 1
    relay(final)
    forward(2, line, final)
    share_copy(2, final).wait_recv()

    def imaging(i):
        values = product[part(i)] + forward_part(3, corner, final, part(i))
        image_out[i] = values.T.astype(bf16).reshape(n, double, width)
        send_all(IMAGED, image_out, imaged_ref, i)

    loop(0, chunks, imaging)

    def again(i):
        receive_all(IMAGED, image_out, imaged_ref, i)
        arrived = imaged_ref[i].reshape(depth, width)

        def taper(s):
            weight = window[i, span(s)].astype(f32)
            values = jnp.dot(gather[span(s)], arrived, preferred_element_type=f32) * weight
            stats[1] += folded(values * values)
            tapered[span(s)] = (values * weight).astype(bf16)

        loop(0, sources, taper)
        transform(second_out, i)
        send_all(SECOND, second_out, second_in, i)

    loop(0, chunks, again)

    def change(p, values):
        normal[p] = values
        send_all(CHANGED, normal, changed_ref, p)
        if not mixing:
            held = flat(values)
            stats[2] += folded(held * flat(model[0, p]))
            stats[3] += folded(held * held)

    adjoint(SECOND, second_out, second_in, 1, change)
    if mixing:

        def norms(p):
            receive_all(CHANGED, normal, changed_ref, p)
            before = returned_ref[p].reshape(depth, piece)
            after = changed_ref[p].reshape(depth, piece)
            mixed_before = jnp.dot(same_ref[...], before, preferred_element_type=f32)
            mixed_after = jnp.dot(same_ref[...], after, preferred_element_type=f32)
            stats[0] += folded(before.astype(f32) * mixed_before)
            stats[2] += folded(after.astype(f32) * mixed_before)
            stats[3] += folded(after.astype(f32) * mixed_after)

        loop(0, pieces, norms)

    def stats_copy(which, src, peer):
        return pltpu.make_async_remote_copy(
            src_ref=src,
            dst_ref=stats_in.at[which],
            send_sem=stats_out_sem.at[which],
            recv_sem=stats_in_sem.at[which],
            device_id={"ma": peer},
            device_id_type=MESH,
        )

    def stats_across(k, peer, slot):
        return pltpu.make_async_remote_copy(
            src_ref=stats_in.at[3],
            dst_ref=stats_all.at[slot],
            send_sem=stats_out_sem.at[2 + k],
            recv_sem=stats_in_sem.at[2 + k],
            device_id={"gx": peer},
            device_id_type=MESH,
        )

    to_core = stats_copy(0, stats, core)
    to_core.start()
    to_core.wait_recv()
    stats_in[2] = stats[...] + stats_in[0]
    to_line = stats_copy(1, stats_in.at[2], line)
    to_line.start()
    to_line.wait_recv()
    stats_in[3] = stats_in[2] + stats_in[1]
    loop(1, n, lambda k: stats_across(k, lax.rem(me + k, n), me).start())
    stats_all[me] = stats_in[3]

    def stats_wait(k):
        peer = lax.rem(me + n - k, n)
        stats_across(k, peer, peer).wait_recv()

    loop(1, n, stats_wait)
    sums_ref[...] = jnp.sum(stats_all[...], axis=0)
    if not mixing:
        loop(0, pieces, lambda p: receive_all(RETURNED, model.at[0], returned_ref, p))
        loop(0, pieces, lambda p: receive_all(CHANGED, normal, changed_ref, p))

    to_core.wait_send()
    to_line.wait_send()
    loop(1, n, lambda k: stats_across(k, lax.rem(me + k, n), me).wait_send())
    finish_all(RECORDED, first_out, first_in, chunks)
    finish_all(RETURNED, summed if mixing else model.at[0], returned_ref, pieces)
    finish_all(IMAGED, image_out, imaged_ref, chunks)
    finish_all(SECOND, second_out, second_in, chunks)
    finish_all(CHANGED, normal, changed_ref, pieces)
    if mixing:
        finish_all(MIXED, mixed_out, model.at[0], pieces)

    def finish(p):
        for stage in range(2):
            core_copy(stage, 0, p).wait_send()
            core_copy(stage, 1, p).wait_send()
            line_copy(stage, p).wait_send()
        for which in range(3):
            share_copy(which, p).wait_send()

    loop(0, pieces, finish)


def iteration(outer, inner, mixing, recorded, kernel, windows, tall, across, same):
    points, sources, length = recorded.shape
    columns = kernel.shape[2]
    double = 2 * sources
    depth = outer * double
    block = columns // inner
    width, piece = min(256, points), min(256, block)
    chunks, pieces = points // width, block // piece
    f32, bf16 = jnp.float32, jnp.bfloat16
    by_chunk = (chunks, outer, double, width)
    by_piece = (pieces, outer, double, piece)
    vmem = pl.BlockSpec(memory_space=pltpu.VMEM)
    hbm = pl.BlockSpec(memory_space=pl.ANY)
    dma = pltpu.SemaphoreType.DMA
    exchanges = 6 if mixing else 5
    most = max(chunks, pieces)
    extra = by_piece if mixing else (1, 1, 16, 128)
    return pl.pallas_call(
        functools.partial(iteration_kernel, outer, inner, mixing),
        out_shape=[
            jax.ShapeDtypeStruct(by_piece, bf16),
            jax.ShapeDtypeStruct(by_chunk, bf16),
            jax.ShapeDtypeStruct(by_piece, bf16),
            jax.ShapeDtypeStruct((4, 8, 128), f32),
        ],
        in_specs=[hbm, hbm, vmem, vmem, vmem, vmem],
        out_specs=[vmem] * 4,
        scratch_shapes=[
            pltpu.VMEM((sources, points, length), f32),
            pltpu.VMEM((2, points, columns), bf16),
            pltpu.VMEM((chunks, sources * length, width), bf16),
            pltpu.VMEM((depth, sources * length), bf16),
            pltpu.VMEM((sources * length, depth), bf16),
            pltpu.VMEM((sources * length, width), bf16),
            pltpu.VMEM(by_chunk, bf16),
            pltpu.VMEM(by_chunk, bf16),
            pltpu.VMEM(by_chunk, bf16),
            pltpu.VMEM(by_chunk, bf16),
            pltpu.VMEM((depth, columns), f32),
            pltpu.VMEM((points, depth), f32),
            pltpu.VMEM(by_chunk, bf16),
            pltpu.VMEM((2, 2) + by_piece, bf16),
            pltpu.VMEM((2, 2) + by_piece, bf16),
            pltpu.VMEM((2,) + by_piece, bf16),
            pltpu.VMEM((2,) + by_piece, bf16),
            pltpu.VMEM((4,) + by_piece, bf16),
            pltpu.VMEM(extra, bf16),
            pltpu.VMEM(by_piece, bf16),
            pltpu.VMEM(extra, bf16),
            pltpu.VMEM((4, 8, 128), f32),
            pltpu.VMEM((4, 4, 8, 128), f32),
            pltpu.VMEM((outer, 4, 8, 128), f32),
            dma((chunks, sources)),
            dma((chunks,)),
            dma((exchanges, most, outer)),
            dma((exchanges, most, outer)),
            dma((2, 2, pieces)),
            dma((2, 2, pieces)),
            dma((2, pieces)),
            dma((2, pieces)),
            dma((3, pieces)),
            dma((3, pieces)),
            dma((2 + outer,)),
            dma((2 + outer,)),
        ],
        compiler_params=pltpu.CompilerParams(
            collective_id=6 if mixing else 5,
            has_side_effects=True,
            vmem_limit_bytes=67_000_000,
        ),
        name="iteration_mixed" if mixing else "iteration",
    )(recorded, kernel, windows, tall, across, same)


def write_kernel(
    sums_ref, rec_ref, win_ref, tall_ref, across_ref, ret_ref, ima_ref, cha_ref,
    sol_ref, res_ref, dir_ref,
    traces, spread, gather, solved, rest, ahead, in_sem, out_sem,
):
    sources, points, length = traces.shape
    chunks, outer, double, width = ima_ref.shape
    depth = outer * double
    f32, bf16 = jnp.float32, jnp.bfloat16

    def loop(start, stop, body):
        def step(i, carry):
            body(i)
            return carry

        lax.fori_loop(start, stop, step, 0)

    def part(i):
        return pl.ds(pl.multiple_of(i * width, width), width)

    def load(i, s):
        return pltpu.make_async_copy(
            rec_ref.at[part(i), s], traces.at[s, part(i)], in_sem.at[i, s]
        )

    def store(number, i, s):
        src, dst = ((solved, sol_ref), (ahead, dir_ref), (rest, res_ref))[number]
        return pltpu.make_async_copy(
            src.at[s, part(i)], dst.at[part(i), s], out_sem.at[number, i, s]
        )

    loop(0, chunks, lambda i: loop(0, sources, lambda s: load(i, s).start()))
    for s in range(sources):
        rows = lax.broadcasted_iota(jnp.int32, (depth, length), 0)
        spread[s] = jnp.where(lax.rem(rows, sources) == s, tall_ref[...], 0.0).astype(bf16)
        columns = lax.broadcasted_iota(jnp.int32, (length, depth), 1)
        gather[s] = jnp.where(lax.rem(columns, sources) == s, across_ref[...], 0.0).astype(bf16)
    norm_start, norm_data = jnp.sum(sums_ref[0]), jnp.sum(sums_ref[1])
    cross, norm_change = jnp.sum(sums_ref[2]), jnp.sum(sums_ref[3])
    step_size = norm_start / (norm_data + epsilon)
    norm_final = norm_start - 2.0 * step_size * cross + step_size * step_size * norm_change
    ratio = norm_final / (norm_start + epsilon)
    samples = lax.broadcasted_iota(jnp.int32, (length, width), 0).astype(f32) * (1.0 / RAMP)

    def chunk(i):
        before = ret_ref[i].reshape(depth, width).astype(f32).T.astype(bf16)
        after = cha_ref[i].reshape(depth, width).astype(f32).T.astype(bf16)
        arrived = ima_ref[i].reshape(depth, width)

        def one(s):
            gradient = jnp.dot(before, spread[s], preferred_element_type=f32)
            change = jnp.dot(after, spread[s], preferred_element_type=f32)
            solved[s, part(i)] = step_size * gradient
            ahead[s, part(i)] = (gradient - step_size * change) + ratio * gradient
            store(0, i, s).start()
            store(1, i, s).start()
            rising = jnp.clip(samples + win_ref[pl.ds(s, 1), part(i)], 0.0, 1.0)
            falling = jnp.clip(win_ref[pl.ds(sources + s, 1), part(i)] - samples, 0.0, 1.0)
            image = jnp.dot(gather[s], arrived, preferred_element_type=f32)
            image = (rising * falling) * image
            load(i, s).wait()
            rest[s, part(i)] = traces[s, part(i)] - step_size * image.T
            store(2, i, s).start()

        loop(0, sources, one)

    loop(0, chunks, chunk)

    def finish(i):
        def one(s):
            for number in range(3):
                store(number, i, s).wait()

        loop(0, sources, one)

    loop(0, chunks, finish)


def write(sums, recorded, windows, tall, across, returned, imaged, changed):
    points, sources, length = recorded.shape
    chunks, outer, double, width = imaged.shape
    depth = outer * double
    vmem = pl.BlockSpec(memory_space=pltpu.VMEM)
    hbm = pl.BlockSpec(memory_space=pl.ANY)
    f32, bf16 = jnp.float32, jnp.bfloat16
    staged = pltpu.VMEM((sources, points, length), f32)
    return pl.pallas_call(
        write_kernel,
        out_shape=[jax.ShapeDtypeStruct(recorded.shape, f32)] * 3,
        in_specs=[vmem, hbm] + [vmem] * 6,
        out_specs=[hbm] * 3,
        scratch_shapes=[
            staged,
            pltpu.VMEM((sources, depth, length), bf16),
            pltpu.VMEM((sources, length, depth), bf16),
            staged,
            staged,
            staged,
            pltpu.SemaphoreType.DMA((chunks, sources)),
            pltpu.SemaphoreType.DMA((3, chunks, sources)),
        ],
        compiler_params=pltpu.CompilerParams(vmem_limit_bytes=56 * 1024 * 1024),
        cost_estimate=pl.CostEstimate(
            flops=6 * points * sources * depth * length,
            bytes_accessed=16 * points * sources * length,
            transcendentals=0,
        ),
        name="write",
    )(sums, recorded, windows, tall, across, returned, imaged, changed)


def fused(outer, inner, recorded, kernel, freq_bins, window_start, window_stop):
    points, sources, length = recorded.shape
    double = 2 * sources
    depth = outer * double
    table = phase_table(freq_bins, length).astype(jnp.bfloat16).astype(jnp.float32)
    tall = jnp.repeat(table.reshape(-1, length), sources, axis=0)
    windows = jnp.concatenate(
        [(1 - window_start).astype(jnp.float32) / RAMP, window_stop.astype(jnp.float32) / RAMP], 1
    ).T
    same = freq_bins[:, None] == freq_bins[None, :]
    repeated = jnp.sum(same.astype(jnp.int32)) > freq_bins.shape[0]
    eye = jnp.eye(double, dtype=jnp.bfloat16)
    mixing = (same.astype(jnp.bfloat16)[:, None, :, None] * eye[None, :, None, :]).reshape(
        depth, depth
    )
    gains = kernel.reshape(2, kernel.shape[2], kernel.shape[3])
    operands = (recorded, gains, windows, tall, tall.T, mixing)
    returned, imaged, changed, sums = lax.cond(
        repeated,
        lambda *x: tuple(iteration(outer, inner, True, *x)),
        lambda *x: tuple(iteration(outer, inner, False, *x)),
        *operands,
    )
    return tuple(write(sums, recorded, windows, tall, tall.T, returned, imaged, changed))


def fits(outer, inner, recorded, kernel):
    points, sources, length = recorded.shape
    columns = kernel.shape[3]
    return (
        inner == 4
        and kernel.shape[1] == 1
        and columns == inner * points
        and sources % 16 == 0
        and length % 128 == 0
        and points % 256 == 0
        and (outer * 2 * sources) % 128 == 0
        and points * (4 * columns + 6 * sources * length) < 30_000_000
    )


def per_device(outer, inner, recorded, kernel, freq_bins, window_start, window_stop):
    if fits(outer, inner, recorded, kernel):
        return fused(outer, inner, recorded, kernel, freq_bins, window_start, window_stop)
    length = recorded.shape[2]
    table = phase_table(freq_bins, length)
    weights = taper_weights(window_start, window_stop, length)
    flat_kernel = kernel.reshape(2 * kernel.shape[2], kernel.shape[3])

    data = by_frequency(exchange(to_spectra(weights * recorded, table), outer, 0), outer)
    adjoint = adjoint_product(data, flat_kernel, inner)
    returned = lax.all_to_all(
        by_source(adjoint, outer), "gx", split_axis=0, concat_axis=0, tiled=True
    )

    same = freq_bins[:, None] == freq_bins[None, :]
    repeated = jnp.sum(same.astype(jnp.int32)) > freq_bins.shape[0]

    def combined(spectra):
        parts = lax.all_to_all(
            by_source(spectra, outer), "gx", split_axis=0, concat_axis=0, tiled=True
        )
        mixed = jnp.einsum(
            "gf,fxa->gxa",
            same.astype(jnp.bfloat16),
            parts,
            preferred_element_type=jnp.float32,
        ).astype(jnp.bfloat16)
        back = lax.all_to_all(mixed, "gx", split_axis=0, concat_axis=0, tiled=True)
        return by_frequency(back, outer)

    model = lax.cond(repeated, combined, lambda spectra: spectra, adjoint)
    outgoing = by_source(forward_product(model, flat_kernel, inner), outer)
    imaged = exchange(outgoing, outer, 1)
    image = weights * to_traces(imaged, table)
    second = by_frequency(exchange(to_spectra(weights * image, table), outer, 2), outer)
    normal = adjoint_product(second, flat_kernel, inner)
    changed = exchange(by_source(normal, outer), outer, 3)

    double, points = returned.shape[1:]
    depth = freq_bins.shape[0] * double
    eye = jnp.eye(double, dtype=jnp.bfloat16)
    mixing = (same.astype(jnp.bfloat16)[:, None, :, None] * eye[None, :, None, :]).reshape(
        depth, depth
    )
    flat_g = returned.reshape(depth, points)
    flat_h = changed.reshape(depth, points)
    mixed_g = jnp.dot(mixing, flat_g, preferred_element_type=jnp.float32)
    mixed_h = jnp.dot(mixing, flat_h, preferred_element_type=jnp.float32)
    sums = jnp.stack(
        [
            jnp.sum(flat_g.astype(jnp.float32) * mixed_g),
            jnp.sum(image * image),
            jnp.sum(mixed_g * flat_h.astype(jnp.float32)),
            jnp.sum(flat_h.astype(jnp.float32) * mixed_h),
        ]
    )
    sums = total(jnp.broadcast_to(jnp.tile(sums, 2)[:, None], (8, 128)), outer, inner, 4)
    if recorded.shape[1] % 8 == 0:
        return tuple(
            final_step(
                sums, recorded, window_start, window_stop, returned, imaged, changed, table
            )
        )
    gradient = to_traces(returned, table)
    change = to_traces(changed, table)
    norm_start, norm_data, cross, norm_change = sums[0, 0], sums[1, 0], sums[2, 0], sums[3, 0]
    step_size = norm_start / (norm_data + epsilon)
    norm_final = norm_start - 2.0 * step_size * cross + step_size * step_size * norm_change
    solution = step_size * gradient
    residual = recorded - step_size * image
    direction = gradient - step_size * change + norm_final / (norm_start + epsilon) * gradient
    return (solution, residual, direction)


def solution(mesh):
    in_specs = (P("ma", "gx", None), P(None, "gx", "ma", None), P(), P("ma", "gx"), P("ma", "gx"))
    out_specs = (P("ma", "gx", None), P("ma", "gx", None), P("ma", "gx", None))
    return jax.shard_map(
        functools.partial(per_device, mesh.shape["gx"], mesh.shape["ma"]),
        mesh=mesh,
        in_specs=in_specs,
        out_specs=out_specs,
        check_vma=False,
    )
```

```python
import functools
import math

import jax
import jax.numpy as jnp
from jax import lax
from jax.experimental import pallas as pl
from jax.experimental.pallas import tpu as pltpu
from jax.sharding import PartitionSpec as P

RAMP = 8
MESH = pl.DeviceIdType.MESH

epsilon = 1e-06


def phase_table(freq_bins, length):
    samples = jnp.arange(length, dtype=jnp.int32)
    angles = (freq_bins[:, None] * samples[None, :] % length).astype(jnp.float32) * (
        2.0 * math.pi / length
    )
    return jnp.stack([jnp.cos(angles), -jnp.sin(angles)], 1) * math.sqrt(2.0 / length)


def taper_weights(window_start, window_stop, length):
    samples = jnp.arange(length, dtype=jnp.float32)
    rising = jnp.clip(
        (samples[None, None, :] - window_start[:, :, None].astype(jnp.float32) + 1.0) / RAMP,
        0.0,
        1.0,
    )
    falling = jnp.clip(
        (window_stop[:, :, None].astype(jnp.float32) - samples[None, None, :]) / RAMP, 0.0, 1.0
    )
    return rising * falling


def exchange_kernel(n, x_ref, o_ref, send_sem, recv_sem, own_sem):
    me = lax.axis_index("gx")
    barrier = pltpu.get_barrier_semaphore()
    for k in range(1, n):
        pl.semaphore_signal(
            barrier, inc=1, device_id={"gx": lax.rem(me + k, n)}, device_id_type=MESH
        )
    own = pltpu.make_async_copy(x_ref.at[me], o_ref.at[me], own_sem)
    own.start()
    pl.semaphore_wait(barrier, n - 1)
    copies = []
    for k in range(1, n):
        peer = lax.rem(me + k, n)
        copy = pltpu.make_async_remote_copy(
            src_ref=x_ref.at[peer],
            dst_ref=o_ref.at[me],
            send_sem=send_sem.at[k],
            recv_sem=recv_sem.at[k],
            device_id={"gx": peer},
            device_id_type=MESH,
        )
        copy.start()
        copies.append(copy)
    own.wait()
    for copy in copies:
        copy.wait()


def exchange(x, n, number):
    return pl.pallas_call(
        functools.partial(exchange_kernel, n),
        out_shape=jax.ShapeDtypeStruct(x.shape, x.dtype),
        in_specs=[pl.BlockSpec(memory_space=pltpu.VMEM)],
        out_specs=pl.BlockSpec(memory_space=pltpu.VMEM),
        scratch_shapes=[
            pltpu.SemaphoreType.DMA((n,)),
            pltpu.SemaphoreType.DMA((n,)),
            pltpu.SemaphoreType.DMA,
        ],
        compiler_params=pltpu.CompilerParams(collective_id=number, has_side_effects=True),
        name=f"exchange{number}",
    )(x)


def total_kernel(outer, inner, x_ref, o_ref, held, send_sem, recv_sem):
    n = outer * inner
    me = lax.axis_index("gx") * inner + lax.axis_index("ma")
    barrier = pltpu.get_barrier_semaphore()

    def place(k):
        peer = lax.rem(me + k, n)
        return (peer // inner, lax.rem(peer, inner))

    for k in range(1, n):
        pl.semaphore_signal(barrier, inc=1, device_id=place(k), device_id_type=MESH)
    pl.semaphore_wait(barrier, n - 1)
    copies = []
    for k in range(1, n):
        copy = pltpu.make_async_remote_copy(
            src_ref=x_ref,
            dst_ref=held.at[me],
            send_sem=send_sem.at[k],
            recv_sem=recv_sem.at[k],
            device_id=place(k),
            device_id_type=MESH,
        )
        copy.start()
        copies.append(copy)
    held[me] = x_ref[...]
    for copy in copies:
        copy.wait()
    o_ref[...] = jnp.sum(held[...], axis=0)


def total(x, outer, inner, number):
    n = outer * inner
    return pl.pallas_call(
        functools.partial(total_kernel, outer, inner),
        out_shape=jax.ShapeDtypeStruct(x.shape, x.dtype),
        in_specs=[pl.BlockSpec(memory_space=pltpu.VMEM)],
        out_specs=pl.BlockSpec(memory_space=pltpu.VMEM),
        scratch_shapes=[
            pltpu.VMEM((n,) + x.shape, x.dtype),
            pltpu.SemaphoreType.DMA((n,)),
            pltpu.SemaphoreType.DMA((n,)),
        ],
        compiler_params=pltpu.CompilerParams(collective_id=number, has_side_effects=True),
        name=f"total{number}",
    )(x)


def pairs(n, bit):
    return [(i, i ^ bit) for i in range(n)]


def scatter_sum(partial, n):
    rows, block = partial.shape[1:]
    me = lax.axis_index("ma")
    held = partial
    bit = 1
    while bit < n:
        own = (me // bit) % 2
        parts = held.reshape(-1, 2, rows, block)
        keep = lax.dynamic_index_in_dim(parts, own, 1, keepdims=False)
        send = lax.dynamic_index_in_dim(parts, 1 - own, 1, keepdims=False)
        got = lax.ppermute(send, "ma", pairs(n, bit))
        held = (keep.astype(jnp.float32) + got.astype(jnp.float32)).astype(jnp.bfloat16)
        bit *= 2
    return held.reshape(rows, block)


def gather_all(x, n):
    rows, block = x.shape
    me = lax.axis_index("ma")
    held = x.reshape(rows, 1, block)
    bit = n // 2
    while bit >= 1:
        own = (me // bit) % 2
        got = lax.ppermute(held, "ma", pairs(n, bit))
        first = jnp.where(own == 0, held, got)
        second = jnp.where(own == 0, got, held)
        held = jnp.stack([first, second], 2).reshape(rows, -1, block)
        bit //= 2
    return held.reshape(rows, n * block)


def to_spectra(traces, table):
    freqs = table.shape[0]
    flat = table.reshape(2 * freqs, table.shape[2]).astype(jnp.bfloat16)
    out = jnp.einsum(
        "ast,kt->ksa", traces.astype(jnp.bfloat16), flat, preferred_element_type=jnp.float32
    ).astype(jnp.bfloat16)
    return out.reshape(freqs, 2 * out.shape[1], out.shape[2])


def to_traces(spectra, table):
    freqs, double, points = spectra.shape
    sources = double // 2
    length = table.shape[2]
    depth = freqs * double
    across = spectra.reshape(depth, points).T
    owner = jnp.arange(depth, dtype=jnp.int32) % sources
    mask = (owner[None, :] == jnp.arange(sources, dtype=jnp.int32)[:, None]).astype(jnp.bfloat16)
    spread = (across[:, None, :] * mask[None]).reshape(points * sources, depth)
    tall = jnp.repeat(table.reshape(2 * freqs, length).astype(jnp.bfloat16), sources, axis=0)
    out = jnp.dot(spread, tall, preferred_element_type=jnp.float32)
    return out.reshape(points, sources, length)


def by_frequency(arrived, n):
    sources = arrived.shape[1] // 2
    points = arrived.shape[2]
    return arrived.reshape(n, 2, sources, points).transpose(1, 0, 2, 3).reshape(2, -1, points)


def by_source(spectra, n):
    points = spectra.shape[2]
    sources = spectra.shape[1] // n
    return spectra.reshape(2, n, sources, points).transpose(1, 0, 2, 3).reshape(n, -1, points)


def adjoint_kernel(d_ref, k_ref, o_ref):
    half = d_ref.shape[0] // 2
    data = d_ref[...]
    first = jnp.dot(data, k_ref[0], preferred_element_type=jnp.float32)
    second = jnp.dot(data, k_ref[1], preferred_element_type=jnp.float32)
    o_ref[0, :half] = (first[:half] + second[half:]).astype(o_ref.dtype)
    o_ref[0, half:] = (first[half:] - second[:half]).astype(o_ref.dtype)


def adjoint_product(data, flat_kernel, inner):
    sources, rows = data.shape[1], data.shape[2]
    columns = flat_kernel.shape[1]
    block = columns // inner
    tile = min(512, block)
    per_block = block // tile
    partial = pl.pallas_call(
        adjoint_kernel,
        grid=(columns // tile,),
        out_shape=jax.ShapeDtypeStruct((inner, 2 * sources, block), jnp.bfloat16),
        in_specs=[
            pl.BlockSpec((2 * sources, rows), lambda j: (0, 0)),
            pl.BlockSpec((2, rows, tile), lambda j: (0, 0, j)),
        ],
        out_specs=pl.BlockSpec(
            (1, 2 * sources, tile), lambda j: (j // per_block, 0, j % per_block)
        ),
        compiler_params=pltpu.CompilerParams(vmem_limit_bytes=60 * 1024 * 1024),
        cost_estimate=pl.CostEstimate(
            flops=8 * sources * rows * columns,
            bytes_accessed=4 * rows * columns + 4 * sources * (rows + columns),
            transcendentals=0,
        ),
        name="adjoint",
    )(data.reshape(2 * sources, rows), flat_kernel.reshape(2, rows, columns))
    return scatter_sum(partial, inner).reshape(2, sources, block)


def final_kernel(
    sums_ref, rec_ref, win_ref, g_ref, d_ref, h_ref, tall_ref, mask_ref, pick_ref,
    sol_ref, res_ref, dir_ref,
):
    tile, sources, length = rec_ref.shape
    norm_start, norm_data = sums_ref[0, 0], sums_ref[1, 0]
    cross, norm_change = sums_ref[2, 0], sums_ref[3, 0]
    step_size = norm_start / (norm_data + epsilon)
    norm_final = norm_start - 2.0 * step_size * cross + step_size * step_size * norm_change
    ratio = norm_final / (norm_start + epsilon)
    tall = tall_ref[...]

    def rows(values, mask):
        return (values[:, None, :] * mask[None]).reshape(tile * sources, -1).astype(jnp.bfloat16)

    def traces(ref):
        spread = rows(ref[...].astype(jnp.float32), mask_ref[...])
        out = jnp.dot(spread, tall, preferred_element_type=jnp.float32)
        return out.reshape(tile, sources, length)

    gradient = traces(g_ref)
    change = traces(h_ref)
    sol_ref[...] = step_size * gradient
    dir_ref[...] = (gradient - step_size * change) + ratio * gradient
    window = win_ref[...]
    ones = jnp.ones((window.shape[1], length), jnp.bfloat16)
    shape = (tile, sources, length)
    start = jnp.dot(rows(window, pick_ref[0]), ones, preferred_element_type=jnp.float32)
    stop = jnp.dot(rows(window, pick_ref[1]), ones, preferred_element_type=jnp.float32)
    samples = lax.broadcasted_iota(jnp.int32, shape, 2).astype(jnp.float32)
    rising = jnp.clip((samples - start.reshape(shape) + 1.0) / RAMP, 0.0, 1.0)
    falling = jnp.clip((stop.reshape(shape) - samples) / RAMP, 0.0, 1.0)
    image = (rising * falling) * traces(d_ref)
    res_ref[...] = rec_ref[...] - step_size * image


def final_step(sums, recorded, window_start, window_stop, returned, arrived, changed, table):
    points, sources, length = recorded.shape
    depth = returned.shape[0] * returned.shape[1]
    tile = min(128, points)

    def across(x):
        return x.reshape(depth, points).T

    place = jnp.arange(sources, dtype=jnp.int32)
    owner = jnp.arange(depth, dtype=jnp.int32) % sources
    mask = (owner[None, :] == place[:, None]).astype(jnp.float32)
    column = jnp.arange(2 * sources, dtype=jnp.int32)
    pick = jnp.stack(
        [column[None, :] == place[:, None], column[None, :] == place[:, None] + sources]
    ).astype(jnp.float32)
    tall = jnp.repeat(table.reshape(-1, length).astype(jnp.bfloat16), sources, axis=0)
    window = jnp.concatenate([window_start, window_stop], 1).astype(jnp.float32)
    whole3 = pl.BlockSpec((tile, sources, length), lambda i: (i, 0, 0))
    strip = pl.BlockSpec((tile, depth), lambda i: (i, 0))
    return pl.pallas_call(
        final_kernel,
        grid=(points // tile,),
        out_shape=[jax.ShapeDtypeStruct(recorded.shape, jnp.float32)] * 3,
        in_specs=[
            pl.BlockSpec(memory_space=pltpu.SMEM),
            whole3,
            pl.BlockSpec((tile, 2 * sources), lambda i: (i, 0)),
            strip,
            strip,
            strip,
            pl.BlockSpec((depth, length), lambda i: (0, 0)),
            pl.BlockSpec((sources, depth), lambda i: (0, 0)),
            pl.BlockSpec((2, sources, 2 * sources), lambda i: (0, 0, 0)),
        ],
        out_specs=[whole3] * 3,
        compiler_params=pltpu.CompilerParams(vmem_limit_bytes=48 * 1024 * 1024),
        cost_estimate=pl.CostEstimate(
            flops=8 * points * sources * depth * length,
            bytes_accessed=16 * points * sources * length,
            transcendentals=0,
        ),
        name="final",
    )(sums, recorded, window, across(returned), across(arrived), across(changed), tall, mask, pick)


def forward_product(model, flat_kernel, inner):
    sources = model.shape[1]
    incoming = gather_all(model.reshape(2 * sources, -1), inner)
    product = lax.dot_general(
        incoming, flat_kernel, (((1,), (1,)), ((), ())), preferred_element_type=jnp.float32
    )
    half = flat_kernel.shape[0] // 2
    real_part = product[:sources, :half] - product[sources:, half:]
    imaginary = product[sources:, :half] + product[:sources, half:]
    return jnp.stack([real_part, imaginary], 0).astype(jnp.bfloat16)


RECORDED, RETURNED, IMAGED, SECOND, CHANGED, MIXED = range(6)
PARTS = 2
GROUP = 4


def loop(start, stop, body):
    def step(i, carry):
        body(i)
        return carry

    lax.fori_loop(start, stop, step, 0)


def iota(shape, axis):
    return lax.broadcasted_iota(jnp.int32, shape, axis)


def folded(values):
    rows, columns = values.shape
    parts = values.reshape(rows // 8, 8, columns).sum(0)
    out = parts[:, :128]
    for j in range(1, columns // 128):
        out = out + parts[:, j * 128 : (j + 1) * 128]
    return out


def iteration_kernel(
    outer, inner, mixing, bins_ref, rec_ref, ker_ref, start_ref, stop_ref,
    returned_ref, imaged_ref, changed_ref, sums_ref, win_ref, spread_ref, gather_ref,
    traces, gains, window, win, spread, gather, tapered, first_out, first_in, second_out,
    second_in, total, product, image_out, image_in, core_out, core_in, line_out, line_in, model,
    summed, summed_in, normal, normal_in, mixed_out, same, stats, stats_in, stats_all,
    trace_sem, gain_sem, keep_sem, out_sem, in_sem, core_out_sem, core_in_sem, line_out_sem,
    line_in_sem, share_out_sem, share_in_sem, stats_out_sem, stats_in_sem,
):
    n = outer
    sources, points, length = traces.shape
    halves, chunks, _, double, width = first_out.shape
    pieces, piece = model.shape[2], model.shape[5]
    count = sources // halves
    depth = n * double
    block = pieces * piece
    f32, bf16 = jnp.float32, jnp.bfloat16
    me, mine = lax.axis_index("gx"), lax.axis_index("ma")
    core = mine + 1 - 2 * lax.rem(mine, 2)
    line = lax.rem(mine + 2, 4)
    corner = lax.rem(core + 2, 4)
    both = range(halves)
    sent = summed if mixing else model.at[:, 0]

    def part(i):
        return pl.ds(pl.multiple_of(i * width, width), width)

    def trace_copy(h, i, s):
        s = h * count + s
        return pltpu.make_async_copy(
            rec_ref.at[part(i), s], traces.at[s, part(i)], trace_sem.at[h, i]
        )

    def trace_wait(h, i):
        place = traces.at[h * count : (h + 1) * count, part(i)]
        pltpu.make_async_copy(place, place, trace_sem.at[h, i]).wait()

    def gain_copy(i):
        return pltpu.make_async_copy(
            ker_ref.at[:, part(i)], gains.at[:, part(i)], gain_sem.at[i]
        )

    kept = (
        (summed_in, returned_ref),
        (image_in, imaged_ref),
        (normal_in, changed_ref),
        (win, win_ref),
        (spread, spread_ref),
        (gather, gather_ref),
    )

    def keep_copy(number):
        src, dst = kept[number]
        return pltpu.make_async_copy(src, dst, keep_sem.at[number])

    def across(number, src, dst, i, peer, slot):
        return pltpu.make_async_remote_copy(
            src_ref=src.at[i, peer],
            dst_ref=dst.at[i, slot],
            send_sem=out_sem.at[number],
            recv_sem=in_sem.at[number, i],
            device_id={"gx": peer},
            device_id_type=MESH,
        )

    def send_all(number, h, src, dst, i):
        src, dst, number = src.at[h], dst.at[h], number * halves + h

        def body(k):
            peer = lax.rem(me + k, n)
            across(number, src, dst, i, peer, me).start()

        loop(1, n, body)
        dst[i, me] = src[i, me]

    def receive_all(number, h, src, dst, i):
        number = number * halves + h
        others = pl.ds(0, n - 1)
        pltpu.make_async_remote_copy(
            src_ref=src.at[h, i, others],
            dst_ref=dst.at[h, i, others],
            send_sem=out_sem.at[number],
            recv_sem=in_sem.at[number, i],
            device_id={"gx": lax.rem(me + 1, n)},
            device_id_type=MESH,
        ).wait_recv()

    def finish_all(number, src, dst, many):
        others = pl.ds(0, n - 1)
        for h in both:
            pltpu.make_async_remote_copy(
                src_ref=src.at[h, :, others],
                dst_ref=dst.at[h, :, others],
                send_sem=out_sem.at[number * halves + h],
                recv_sem=in_sem.at[number * halves + h, 0],
                device_id={"gx": lax.rem(me + 1, n)},
                device_id_type=MESH,
            ).wait_send()

    def core_copy(h, stage, which, p):
        return pltpu.make_async_remote_copy(
            src_ref=core_out.at[h, stage, which, p],
            dst_ref=core_in.at[h, stage, which, p],
            send_sem=core_out_sem,
            recv_sem=core_in_sem.at[h, stage, which, p],
            device_id={"ma": core},
            device_id_type=MESH,
        )

    def line_copy(h, stage, p):
        return pltpu.make_async_remote_copy(
            src_ref=line_out.at[h, stage, p],
            dst_ref=line_in.at[h, stage, p],
            send_sem=line_out_sem,
            recv_sem=line_in_sem.at[h, stage, p],
            device_id={"ma": line},
            device_id_type=MESH,
        )

    def share_copy(h, which, p):
        source, slot, peer = ((0, 1, core), (0, 2, line), (2, 3, core))[which]
        return pltpu.make_async_remote_copy(
            src_ref=model.at[h, source, p],
            dst_ref=model.at[h, slot, p],
            send_sem=share_out_sem.at[which],
            recv_sem=share_in_sem.at[h, which, p],
            device_id={"ma": peer},
            device_id_type=MESH,
        )

    barrier = pltpu.get_barrier_semaphore()

    def greet(k):
        pl.semaphore_signal(
            barrier, inc=1, device_id={"gx": lax.rem(me + k, n)}, device_id_type=MESH
        )

    loop(1, n, greet)
    for peer in (core, line):
        pl.semaphore_signal(barrier, inc=1, device_id={"ma": peer}, device_id_type=MESH)

    for h in both:
        loop(0, chunks, lambda i: loop(0, count, lambda s: trace_copy(h, i, s).start()))

    owners = iota((n, length), 0)
    bins = jnp.zeros_like(owners)
    for f in range(n):
        bins = jnp.where(owners == f, bins_ref[f], bins)
    angles = lax.rem(bins * iota((n, length), 1), length).astype(f32) * (2.0 * math.pi / length)
    scale = math.sqrt(2.0 / length)
    real, imaginary = jnp.cos(angles) * scale, -jnp.sin(angles) * scale
    rows = []
    for f in range(n):
        for values in (real, imaginary):
            rows.append(jnp.broadcast_to(values[f : f + 1], (count, length)))
    tall = jnp.concatenate(rows, 0)
    wide = tall.T
    row_place = lax.rem(iota((depth, length), 0), count)
    column_place = lax.rem(iota((length, depth), 1), count)
    for s in range(count):
        here = slice(s * length, (s + 1) * length)
        spread[:, here] = jnp.where(row_place == s, tall, 0.0).astype(bf16)
        gather[here] = jnp.where(column_place == s, wide, 0.0).astype(bf16)
    win[:sources] = (1 - start_ref[...]).astype(f32) * (1.0 / RAMP)
    win[sources:] = stop_ref[...].astype(f32) * (1.0 / RAMP)
    stats[...] = jnp.zeros_like(stats)
    if mixing:
        sides = []
        for axis in range(2):
            owner = iota((depth, depth), axis) // double
            values = jnp.zeros_like(owner)
            for f in range(n):
                values = jnp.where(owner == f, bins_ref[f], values)
            sides.append((values, lax.rem(iota((depth, depth), axis), double)))
        alike = (sides[0][0] == sides[1][0]) & (sides[0][1] == sides[1][1])
        same[...] = jnp.where(alike, 1.0, 0.0).astype(bf16)
    pl.semaphore_wait(barrier, n + 1)

    samples = iota((length, width), 0).astype(f32) * (1.0 / RAMP)

    def span(s, many=1):
        return pl.ds(pl.multiple_of(s * length, length), many * length)

    def transform(out, h, i):
        result = jnp.dot(spread[...], tapered[...], preferred_element_type=f32)
        out[h, i] = result.astype(bf16).reshape(n, double, width)

    def record(h, i):
        trace_wait(h, i)
        if h == 0:
            gain_copy(i).start()
        for k in range(count):
            s = h * count + k
            rising = jnp.clip(samples + win[s : s + 1, part(i)], 0.0, 1.0)
            falling = jnp.clip(win[sources + s : sources + s + 1, part(i)] - samples, 0.0, 1.0)
            weight = rising * falling
            window[i, span(s)] = weight.astype(bf16)
            tapered[k * length : (k + 1) * length] = (weight * traces[s, part(i)].T).astype(bf16)
        transform(first_out, h, i)
        send_all(RECORDED, h, first_out, first_in, i)

    def turned(values, sign):
        half = double // 2
        wide_values = values.astype(f32)
        low, high = wide_values[:, :half], wide_values[:, half:]
        pair = [high, -low] if sign > 0 else [-high, low]
        return jnp.concatenate(pair, 1).reshape(depth, values.shape[2]).astype(bf16)

    def adjoint_part(held, h, i, columns):
        data = held[h, i]
        return jnp.dot(
            data.reshape(depth, width), gains[0, part(i), columns], preferred_element_type=f32
        ) + jnp.dot(turned(data, 1), gains[1, part(i), columns], preferred_element_type=f32)

    rounds = ((RECORDED, first_out, first_in), (SECOND, second_out, second_in))

    def accumulate(stage, h, i):
        number, src, held = rounds[stage]
        receive_all(number, h, src, held, i)
        if stage == 0 and h == 0:
            gain_copy(i).wait()

        def body(j):
            columns = pl.ds(pl.multiple_of(j * block, block), block)
            update = adjoint_part(held, h, i, columns)
            total[h, :, columns] = update if i == 0 else total[h, :, columns] + update

        loop(0, inner, body)

    last = chunks - 1

    def pack(values):
        return values.astype(bf16).reshape(n, double, piece)

    def tile(stage, h, where, p):
        columns = pl.ds(pl.multiple_of(where * block + p * piece, piece), piece)
        update = adjoint_part(rounds[stage][2], h, last, columns)
        return update if chunks == 1 else total[h, :, columns] + update

    def from_core(stage, h, which, p):
        core_copy(h, stage, which, p).wait_recv()
        return core_in[h, stage, which, p].reshape(depth, piece).astype(f32)

    def reduce_out(stage, h):
        number, src, held = rounds[stage]
        receive_all(number, h, src, held, last)
        if stage == 0 and h == 0:
            gain_copy(last).wait()

        def to_core(which, where):
            def body(p):
                core_out[h, stage, which, p] = pack(tile(stage, h, where, p))
                core_copy(h, stage, which, p).start()

            loop(0, pieces, body)

        def to_line(p):
            values = tile(stage, h, line, p)
            line_out[h, stage, p] = pack(values + from_core(stage, h, 0, p))
            line_copy(h, stage, p).start()

        to_core(0, corner)
        loop(0, pieces, to_line)
        to_core(1, core)

    def reduced(stage, h, p):
        values = tile(stage, h, mine, p)
        values = values + from_core(stage, h, 1, p)
        line_copy(h, stage, p).wait_recv()
        return pack(values + line_in[h, stage, p].reshape(depth, piece).astype(f32))

    def flat(values):
        return values.reshape(depth, values.shape[2]).astype(f32)

    def forward_part(h, slot, where, p, rows):
        columns = pl.ds(pl.multiple_of(where * block + p * piece, piece), piece)
        values = model[h, slot, p]
        dims = (((1,), (1,)), ((), ()))
        return lax.dot_general(
            gains[0, rows, columns],
            values.reshape(depth, piece),
            dims,
            preferred_element_type=f32,
        ) + lax.dot_general(
            gains[1, rows, columns], turned(values, -1), dims, preferred_element_type=f32
        )

    def forward(h, slot, where, p):
        tile_rows = 2 * width if chunks % 2 == 0 else width

        def body(i):
            rows = pl.ds(pl.multiple_of(i * tile_rows, tile_rows), tile_rows)
            product[h, rows] += forward_part(h, slot, where, p, rows)

        loop(0, points // tile_rows, body)

    def share(h, p):
        share_copy(h, 1, p).start()
        share_copy(h, 0, p).start()

    def keep(h, p):
        values = reduced(0, h, p)
        if mixing:
            summed[h, p] = values
            send_all(RETURNED, h, sent, summed_in, p)
        else:
            model[h, 0, p] = values
            share(h, p)
            send_all(RETURNED, h, sent, summed_in, p)
            held = flat(values)
            stats[0] += folded(held * held)

    def mix(h, p):
        receive_all(RETURNED, h, sent, summed_in, p)
        arrived = summed_in[h, p].reshape(depth, piece)
        values = jnp.dot(same[...], arrived, preferred_element_type=f32)
        mixed_out[h, p] = values.astype(bf16).reshape(n, double, piece)
        send_all(MIXED, h, mixed_out, model.at[:, 0], p)

    def unmix(h, p):
        receive_all(MIXED, h, mixed_out, model.at[:, 0], p)
        share(h, p)

    def own_forward(h):
        product[h] = jnp.zeros_like(product[h])
        loop(0, pieces, lambda p: forward(h, 0, mine, p))

        def from_share(p):
            share_copy(h, 0, p).wait_recv()
            forward(h, 1, core, p)

        loop(0, pieces, from_share)

    def relay(h, p):
        share_copy(h, 1, p).wait_recv()
        share_copy(h, 2, p).start()
        forward(h, 2, line, p)
        share_copy(h, 2, p).wait_recv()

    def from_line(h, p):
        relay(h, p)
        forward(h, 3, corner, p)

    final = pieces - 1

    def imaging(h):
        relay(h, final)

        def body(i):
            values = product[h, part(i)] + forward_part(h, 3, corner, final, part(i))
            image_out[h, i] = values.T.astype(bf16).reshape(n, double, width)
            send_all(IMAGED, h, image_out, image_in, i)

        loop(0, chunks, body)

    def again(h, i):
        receive_all(IMAGED, h, image_out, image_in, i)
        arrived = image_in[h, i].reshape(depth, width)
        for j in range(0, count, GROUP):
            weight = window[i, span(h * count + j, GROUP)].astype(f32)
            rows = slice(j * length, (j + GROUP) * length)
            values = jnp.dot(gather[rows], arrived, preferred_element_type=f32) * weight
            stats[1] += folded(values * values)
            tapered[rows] = (values * weight).astype(bf16)
        transform(second_out, h, i)
        send_all(SECOND, h, second_out, second_in, i)

    def change(h, p):
        values = reduced(1, h, p)
        normal[h, p] = values
        send_all(CHANGED, h, normal, normal_in, p)
        if not mixing:
            held = flat(values)
            stats[2] += folded(held * flat(model[h, 0, p]))
            stats[3] += folded(held * held)

    for h in both:
        loop(0, chunks, lambda i: record(h, i))
    for number in (3, 4, 5):
        keep_copy(number).start()
    for i in range(last):
        accumulate(0, 0, i)
    reduce_out(0, 0)
    for h in both:
        if h + 1 < halves:
            for i in range(last):
                accumulate(0, h + 1, i)
        loop(0, pieces, lambda p: keep(h, p))
        if mixing:
            loop(0, pieces, lambda p: mix(h, p))
        if h + 1 < halves:
            reduce_out(0, h + 1)
        if mixing:
            loop(0, pieces, lambda p: unmix(h, p))
        own_forward(h)
        for p in range(max(chunks, pieces)):
            if h and p < chunks:
                again(h - 1, p)
            if p < final:
                from_line(h, p)
        imaging(h)
    for h in both:
        for i in range(last):
            if h:
                break
            accumulate(1, h, i)
        if h == 0:
            reduce_out(1, h)
            for p in range(max(chunks, pieces)):
                if p < chunks:
                    again(halves - 1, p)
                if halves > 1 and p < pieces:
                    change(h, p)
        else:
            for i in range(last):
                accumulate(1, h, i)
            reduce_out(1, h)
            loop(0, pieces, lambda p: change(h, p))
    keep_copy(1).start()
    if mixing:

        def norms(h, p):
            receive_all(CHANGED, h, normal, normal_in, p)
            before = summed_in[h, p].reshape(depth, piece)
            after = normal_in[h, p].reshape(depth, piece)
            mixed_before = jnp.dot(same[...], before, preferred_element_type=f32)
            mixed_after = jnp.dot(same[...], after, preferred_element_type=f32)
            stats[0] += folded(before.astype(f32) * mixed_before)
            stats[2] += folded(after.astype(f32) * mixed_before)
            stats[3] += folded(after.astype(f32) * mixed_after)

        keep_copy(0).start()
        for h in both:
            loop(0, pieces, lambda p: norms(h, p))
    else:
        for h in both:
            loop(0, pieces, lambda p: receive_all(RETURNED, h, sent, summed_in, p))
        keep_copy(0).start()

    def stats_copy(which, src, peer):
        return pltpu.make_async_remote_copy(
            src_ref=src,
            dst_ref=stats_in.at[which],
            send_sem=stats_out_sem.at[which],
            recv_sem=stats_in_sem.at[which],
            device_id={"ma": peer},
            device_id_type=MESH,
        )

    def stats_across(peer, slot):
        return pltpu.make_async_remote_copy(
            src_ref=stats_in.at[3],
            dst_ref=stats_all.at[slot],
            send_sem=stats_out_sem.at[2],
            recv_sem=stats_in_sem.at[2],
            device_id={"gx": peer},
            device_id_type=MESH,
        )

    to_core = stats_copy(0, stats, core)
    to_core.start()
    to_core.wait_recv()
    stats_in[2] = stats[...] + stats_in[0]
    to_line = stats_copy(1, stats_in.at[2], line)
    to_line.start()
    to_line.wait_recv()
    stats_in[3] = stats_in[2] + stats_in[1]
    loop(1, n, lambda k: stats_across(lax.rem(me + k, n), me).start())
    stats_all[me] = stats_in[3]
    others = stats_all.at[pl.ds(0, n - 1)]
    every = pltpu.make_async_remote_copy(
        src_ref=others,
        dst_ref=others,
        send_sem=stats_out_sem.at[2],
        recv_sem=stats_in_sem.at[2],
        device_id={"gx": lax.rem(me + 1, n)},
        device_id_type=MESH,
    )
    if not mixing:
        for h in both:
            loop(0, pieces, lambda p: receive_all(CHANGED, h, normal, normal_in, p))
    keep_copy(2).start()
    every.wait_recv()
    sums_ref[...] = jnp.sum(stats_all[...], axis=0)

    to_core.wait_send()
    to_line.wait_send()
    every.wait_send()
    finish_all(RECORDED, first_out, first_in, chunks)
    finish_all(RETURNED, sent, summed_in, pieces)
    finish_all(IMAGED, image_out, image_in, chunks)
    finish_all(SECOND, second_out, second_in, chunks)
    finish_all(CHANGED, normal, normal_in, pieces)
    if mixing:
        finish_all(MIXED, mixed_out, model.at[:, 0], pieces)

    def finish(src, dst, sem, peer):
        pltpu.make_async_remote_copy(
            src_ref=src,
            dst_ref=dst,
            send_sem=sem,
            recv_sem=stats_in_sem.at[0],
            device_id={"ma": peer},
            device_id_type=MESH,
        ).wait_send()

    finish(core_out, core_in, core_out_sem, core)
    finish(line_out, line_in, line_out_sem, line)
    for which, peer in ((0, core), (1, line), (2, core)):
        finish(model.at[:, 0], model.at[:, 1], share_out_sem.at[which], peer)
    for number in range(6):
        keep_copy(number).wait()


def iteration(outer, inner, mixing, freq_bins, recorded, kernel, window_start, window_stop):
    points, sources, length = recorded.shape
    columns = kernel.shape[2]
    halves = PARTS
    count = sources // halves
    double = 2 * count
    depth = outer * double
    block = columns // inner
    width, piece = min(256, points), min(256, block)
    chunks, pieces = points // width, block // piece
    f32, bf16 = jnp.float32, jnp.bfloat16
    by_chunk = (halves, chunks, outer, double, width)
    by_piece = (halves, pieces, outer, double, piece)
    stack = by_piece[1:]
    vmem = pl.BlockSpec(memory_space=pltpu.VMEM)
    hbm = pl.BlockSpec(memory_space=pl.ANY)
    dma = pltpu.SemaphoreType.DMA
    exchanges = 6 if mixing else 5
    extra = by_piece if mixing else (halves, 1, 1, 16, 128)
    return pl.pallas_call(
        functools.partial(iteration_kernel, outer, inner, mixing),
        out_shape=[
            jax.ShapeDtypeStruct(by_piece, bf16),
            jax.ShapeDtypeStruct(by_chunk, bf16),
            jax.ShapeDtypeStruct(by_piece, bf16),
            jax.ShapeDtypeStruct((4, 8, 128), f32),
            jax.ShapeDtypeStruct((2 * sources, points), f32),
            jax.ShapeDtypeStruct((depth, count * length), bf16),
            jax.ShapeDtypeStruct((count * length, depth), bf16),
        ],
        in_specs=[pl.BlockSpec(memory_space=pltpu.SMEM), hbm, hbm, vmem, vmem],
        out_specs=[hbm, hbm, hbm, vmem, hbm, hbm, hbm],
        scratch_shapes=[
            pltpu.VMEM((sources, points, length), f32),
            pltpu.VMEM((2, points, columns), bf16),
            pltpu.VMEM((chunks, sources * length, width), bf16),
            pltpu.VMEM((2 * sources, points), f32),
            pltpu.VMEM((depth, count * length), bf16),
            pltpu.VMEM((count * length, depth), bf16),
            pltpu.VMEM((count * length, width), bf16),
            pltpu.VMEM(by_chunk, bf16),
            pltpu.VMEM(by_chunk, bf16),
            pltpu.VMEM(by_chunk, bf16),
            pltpu.VMEM(by_chunk, bf16),
            pltpu.VMEM((halves, depth, columns), f32),
            pltpu.VMEM((halves, points, depth), f32),
            pltpu.VMEM(by_chunk, bf16),
            pltpu.VMEM(by_chunk, bf16),
            pltpu.VMEM((halves, 2, 2) + stack, bf16),
            pltpu.VMEM((halves, 2, 2) + stack, bf16),
            pltpu.VMEM((halves, 2) + stack, bf16),
            pltpu.VMEM((halves, 2) + stack, bf16),
            pltpu.VMEM((halves, 4) + stack, bf16),
            pltpu.VMEM(extra, bf16),
            pltpu.VMEM(by_piece, bf16),
            pltpu.VMEM(by_piece, bf16),
            pltpu.VMEM(by_piece, bf16),
            pltpu.VMEM(extra, bf16),
            pltpu.VMEM((depth, depth) if mixing else (16, 128), bf16),
            pltpu.VMEM((4, 8, 128), f32),
            pltpu.VMEM((4, 4, 8, 128), f32),
            pltpu.VMEM((outer, 4, 8, 128), f32),
            dma((halves, chunks)),
            dma((chunks,)),
            dma((6,)),
            dma((exchanges * halves,)),
            dma((exchanges * halves, max(chunks, pieces))),
            dma,
            dma((halves, 2, 2, pieces)),
            dma,
            dma((halves, 2, pieces)),
            dma((3,)),
            dma((halves, 3, pieces)),
            dma((3,)),
            dma((3,)),
        ],
        compiler_params=pltpu.CompilerParams(
            collective_id=6 if mixing else 5,
            has_side_effects=True,
            vmem_limit_bytes=67_000_000,
        ),
        name="iteration_mixed" if mixing else "iteration",
    )(freq_bins, recorded, kernel, window_start, window_stop)


def write_kernel(
    sums_ref, rec_ref, win_ref, spread_ref, gather_ref, ret_ref, ima_ref, cha_ref,
    sol_ref, res_ref, dir_ref, traces, solved, rest, ahead, in_sem, out_sem,
):
    sources, points, length = traces.shape
    halves, chunks, outer, double, width = ima_ref.shape
    depth = outer * double
    count = sources // halves
    f32, bf16 = jnp.float32, jnp.bfloat16

    def part(i):
        return pl.ds(pl.multiple_of(i * width, width), width)

    def load(i, s):
        return pltpu.make_async_copy(
            rec_ref.at[part(i), s], traces.at[s, part(i)], in_sem.at[i]
        )

    staged = ((solved, sol_ref), (ahead, dir_ref), (rest, res_ref))

    def store(number, i, s):
        src, dst = staged[number]
        return pltpu.make_async_copy(
            src.at[s, part(i)], dst.at[part(i), s], out_sem.at[number]
        )

    loop(0, chunks, lambda i: loop(0, sources, lambda s: load(i, s).start()))
    norm_start, norm_data = jnp.sum(sums_ref[0]), jnp.sum(sums_ref[1])
    cross, norm_change = jnp.sum(sums_ref[2]), jnp.sum(sums_ref[3])
    step_size = norm_start / (norm_data + epsilon)
    norm_final = norm_start - 2.0 * step_size * cross + step_size * step_size * norm_change
    ratio = norm_final / (norm_start + epsilon)
    samples = iota((length, width), 0).astype(f32) * (1.0 / RAMP)

    def chunk(i):
        place = traces.at[:, part(i)]
        pltpu.make_async_copy(place, place, in_sem.at[i]).wait()
        for h in range(halves):
            before = ret_ref[h, i].reshape(depth, width).astype(f32).T.astype(bf16)
            after = cha_ref[h, i].reshape(depth, width).astype(f32).T.astype(bf16)
            arrived = ima_ref[h, i].reshape(depth, width)

            def pair(j):
                spans = pl.ds(pl.multiple_of(j * 2 * length, length), 2 * length)
                table = spread_ref[:, spans]
                first = h * count + 2 * j
                for r in range(0, width, 128):
                    rows = pl.ds(pl.multiple_of(i * width + r, 128), 128)
                    gradient = jnp.dot(before[r : r + 128], table, preferred_element_type=f32)
                    change = jnp.dot(after[r : r + 128], table, preferred_element_type=f32)
                    for k in range(2):
                        here = slice(k * length, (k + 1) * length)
                        g, c = gradient[:, here], change[:, here]
                        solved[first + k, rows] = step_size * g
                        ahead[first + k, rows] = (g - step_size * c) + ratio * g
                for k in range(2):
                    s = first + k
                    store(0, i, s).start()
                    store(1, i, s).start()
                    rising = jnp.clip(samples + win_ref[pl.ds(s, 1), part(i)], 0.0, 1.0)
                    falling = jnp.clip(
                        win_ref[pl.ds(sources + s, 1), part(i)] - samples, 0.0, 1.0
                    )
                    spans = pl.ds(pl.multiple_of((2 * j + k) * length, length), length)
                    image = jnp.dot(gather_ref[spans], arrived, preferred_element_type=f32)
                    image = (rising * falling) * image
                    rest[s, part(i)] = traces[s, part(i)] - step_size * image.T
                    store(2, i, s).start()

            loop(0, count // 2, pair)

    loop(0, chunks, chunk)
    for number in range(3):
        src = staged[number][0]
        pltpu.make_async_copy(src, src, out_sem.at[number]).wait()


def write(recorded, returned, imaged, changed, sums, windows, spread, gather):
    points, sources, length = recorded.shape
    halves, chunks, outer, double, width = imaged.shape
    depth = outer * double
    vmem = pl.BlockSpec(memory_space=pltpu.VMEM)
    hbm = pl.BlockSpec(memory_space=pl.ANY)
    f32 = jnp.float32
    staged = pltpu.VMEM((sources, points, length), f32)
    return pl.pallas_call(
        write_kernel,
        out_shape=[jax.ShapeDtypeStruct(recorded.shape, f32)] * 3,
        in_specs=[vmem, hbm] + [vmem] * 6,
        out_specs=[hbm] * 3,
        scratch_shapes=[
            staged,
            staged,
            staged,
            staged,
            pltpu.SemaphoreType.DMA((chunks,)),
            pltpu.SemaphoreType.DMA((3,)),
        ],
        compiler_params=pltpu.CompilerParams(vmem_limit_bytes=56 * 1024 * 1024),
        cost_estimate=pl.CostEstimate(
            flops=6 * points * sources * depth * length,
            bytes_accessed=16 * points * sources * length,
            transcendentals=0,
        ),
        name="write",
    )(sums, recorded, windows, spread, gather, returned, imaged, changed)


def fused(outer, inner, recorded, kernel, freq_bins, window_start, window_stop):
    same = freq_bins[:, None] == freq_bins[None, :]
    repeated = jnp.sum(same.astype(jnp.int32)) > freq_bins.shape[0]
    gains = kernel.reshape(2, kernel.shape[2], kernel.shape[3])
    results = lax.cond(
        repeated,
        lambda *x: tuple(iteration(outer, inner, True, *x)),
        lambda *x: tuple(iteration(outer, inner, False, *x)),
        freq_bins, recorded, gains, window_start.T, window_stop.T,
    )
    return tuple(write(recorded, *results))


def fits(outer, inner, recorded, kernel):
    points, sources, length = recorded.shape
    columns = kernel.shape[3]
    return (
        inner == 4
        and kernel.shape[1] == 1
        and columns == inner * points
        and sources % (PARTS * 8) == 0
        and length % 128 == 0
        and points % 256 == 0
        and outer * 2 * (sources // PARTS) % 128 == 0
        and points * (4 * columns + 6 * sources * length) < 30_000_000
    )


def per_device(outer, inner, recorded, kernel, freq_bins, window_start, window_stop):
    if fits(outer, inner, recorded, kernel):
        return fused(outer, inner, recorded, kernel, freq_bins, window_start, window_stop)
    length = recorded.shape[2]
    table = phase_table(freq_bins, length)
    weights = taper_weights(window_start, window_stop, length)
    flat_kernel = kernel.reshape(2 * kernel.shape[2], kernel.shape[3])

    data = by_frequency(exchange(to_spectra(weights * recorded, table), outer, 0), outer)
    adjoint = adjoint_product(data, flat_kernel, inner)
    returned = lax.all_to_all(
        by_source(adjoint, outer), "gx", split_axis=0, concat_axis=0, tiled=True
    )

    same = freq_bins[:, None] == freq_bins[None, :]
    repeated = jnp.sum(same.astype(jnp.int32)) > freq_bins.shape[0]

    def combined(spectra):
        parts = lax.all_to_all(
            by_source(spectra, outer), "gx", split_axis=0, concat_axis=0, tiled=True
        )
        mixed = jnp.einsum(
            "gf,fxa->gxa",
            same.astype(jnp.bfloat16),
            parts,
            preferred_element_type=jnp.float32,
        ).astype(jnp.bfloat16)
        back = lax.all_to_all(mixed, "gx", split_axis=0, concat_axis=0, tiled=True)
        return by_frequency(back, outer)

    model = lax.cond(repeated, combined, lambda spectra: spectra, adjoint)
    outgoing = by_source(forward_product(model, flat_kernel, inner), outer)
    imaged = exchange(outgoing, outer, 1)
    image = weights * to_traces(imaged, table)
    second = by_frequency(exchange(to_spectra(weights * image, table), outer, 2), outer)
    normal = adjoint_product(second, flat_kernel, inner)
    changed = exchange(by_source(normal, outer), outer, 3)

    double, points = returned.shape[1:]
    depth = freq_bins.shape[0] * double
    eye = jnp.eye(double, dtype=jnp.bfloat16)
    mixing = (same.astype(jnp.bfloat16)[:, None, :, None] * eye[None, :, None, :]).reshape(
        depth, depth
    )
    flat_g = returned.reshape(depth, points)
    flat_h = changed.reshape(depth, points)
    mixed_g = jnp.dot(mixing, flat_g, preferred_element_type=jnp.float32)
    mixed_h = jnp.dot(mixing, flat_h, preferred_element_type=jnp.float32)
    sums = jnp.stack(
        [
            jnp.sum(flat_g.astype(jnp.float32) * mixed_g),
            jnp.sum(image * image),
            jnp.sum(mixed_g * flat_h.astype(jnp.float32)),
            jnp.sum(flat_h.astype(jnp.float32) * mixed_h),
        ]
    )
    sums = total(jnp.broadcast_to(jnp.tile(sums, 2)[:, None], (8, 128)), outer, inner, 4)
    if recorded.shape[1] % 8 == 0:
        return tuple(
            final_step(
                sums, recorded, window_start, window_stop, returned, imaged, changed, table
            )
        )
    gradient = to_traces(returned, table)
    change = to_traces(changed, table)
    norm_start, norm_data, cross, norm_change = sums[0, 0], sums[1, 0], sums[2, 0], sums[3, 0]
    step_size = norm_start / (norm_data + epsilon)
    norm_final = norm_start - 2.0 * step_size * cross + step_size * step_size * norm_change
    solution = step_size * gradient
    residual = recorded - step_size * image
    direction = gradient - step_size * change + norm_final / (norm_start + epsilon) * gradient
    return (solution, residual, direction)


def solution(mesh):
    in_specs = (P("ma", "gx", None), P(None, "gx", "ma", None), P(), P("ma", "gx"), P("ma", "gx"))
    out_specs = (P("ma", "gx", None), P("ma", "gx", None), P("ma", "gx", None))
    return jax.shard_map(
        functools.partial(per_device, mesh.shape["gx"], mesh.shape["ma"]),
        mesh=mesh,
        in_specs=in_specs,
        out_specs=out_specs,
        check_vma=False,
    )
```

```python
import functools
import math

import jax
import jax.numpy as jnp
from jax import lax
from jax.experimental import pallas as pl
from jax.experimental.pallas import tpu as pltpu
from jax.sharding import PartitionSpec as P

RAMP = 8
MESH = pl.DeviceIdType.MESH

epsilon = 1e-06


def phase_table(freq_bins, length):
    samples = jnp.arange(length, dtype=jnp.int32)
    angles = (freq_bins[:, None] * samples[None, :] % length).astype(jnp.float32) * (
        2.0 * math.pi / length
    )
    return jnp.stack([jnp.cos(angles), -jnp.sin(angles)], 1) * math.sqrt(2.0 / length)


def taper_weights(window_start, window_stop, length):
    samples = jnp.arange(length, dtype=jnp.float32)
    rising = jnp.clip(
        (samples[None, None, :] - window_start[:, :, None].astype(jnp.float32) + 1.0) / RAMP,
        0.0,
        1.0,
    )
    falling = jnp.clip(
        (window_stop[:, :, None].astype(jnp.float32) - samples[None, None, :]) / RAMP, 0.0, 1.0
    )
    return rising * falling


def exchange_kernel(n, x_ref, o_ref, send_sem, recv_sem, own_sem):
    me = lax.axis_index("gx")
    barrier = pltpu.get_barrier_semaphore()
    for k in range(1, n):
        pl.semaphore_signal(
            barrier, inc=1, device_id={"gx": lax.rem(me + k, n)}, device_id_type=MESH
        )
    own = pltpu.make_async_copy(x_ref.at[me], o_ref.at[me], own_sem)
    own.start()
    pl.semaphore_wait(barrier, n - 1)
    copies = []
    for k in range(1, n):
        peer = lax.rem(me + k, n)
        copy = pltpu.make_async_remote_copy(
            src_ref=x_ref.at[peer],
            dst_ref=o_ref.at[me],
            send_sem=send_sem.at[k],
            recv_sem=recv_sem.at[k],
            device_id={"gx": peer},
            device_id_type=MESH,
        )
        copy.start()
        copies.append(copy)
    own.wait()
    for copy in copies:
        copy.wait()


def exchange(x, n, number):
    return pl.pallas_call(
        functools.partial(exchange_kernel, n),
        out_shape=jax.ShapeDtypeStruct(x.shape, x.dtype),
        in_specs=[pl.BlockSpec(memory_space=pltpu.VMEM)],
        out_specs=pl.BlockSpec(memory_space=pltpu.VMEM),
        scratch_shapes=[
            pltpu.SemaphoreType.DMA((n,)),
            pltpu.SemaphoreType.DMA((n,)),
            pltpu.SemaphoreType.DMA,
        ],
        compiler_params=pltpu.CompilerParams(collective_id=number, has_side_effects=True),
        name=f"exchange{number}",
    )(x)


def total_kernel(outer, inner, x_ref, o_ref, held, send_sem, recv_sem):
    n = outer * inner
    me = lax.axis_index("gx") * inner + lax.axis_index("ma")
    barrier = pltpu.get_barrier_semaphore()

    def place(k):
        peer = lax.rem(me + k, n)
        return (peer // inner, lax.rem(peer, inner))

    for k in range(1, n):
        pl.semaphore_signal(barrier, inc=1, device_id=place(k), device_id_type=MESH)
    pl.semaphore_wait(barrier, n - 1)
    copies = []
    for k in range(1, n):
        copy = pltpu.make_async_remote_copy(
            src_ref=x_ref,
            dst_ref=held.at[me],
            send_sem=send_sem.at[k],
            recv_sem=recv_sem.at[k],
            device_id=place(k),
            device_id_type=MESH,
        )
        copy.start()
        copies.append(copy)
    held[me] = x_ref[...]
    for copy in copies:
        copy.wait()
    o_ref[...] = jnp.sum(held[...], axis=0)


def total(x, outer, inner, number):
    n = outer * inner
    return pl.pallas_call(
        functools.partial(total_kernel, outer, inner),
        out_shape=jax.ShapeDtypeStruct(x.shape, x.dtype),
        in_specs=[pl.BlockSpec(memory_space=pltpu.VMEM)],
        out_specs=pl.BlockSpec(memory_space=pltpu.VMEM),
        scratch_shapes=[
            pltpu.VMEM((n,) + x.shape, x.dtype),
            pltpu.SemaphoreType.DMA((n,)),
            pltpu.SemaphoreType.DMA((n,)),
        ],
        compiler_params=pltpu.CompilerParams(collective_id=number, has_side_effects=True),
        name=f"total{number}",
    )(x)


def pairs(n, bit):
    return [(i, i ^ bit) for i in range(n)]


def scatter_sum(partial, n):
    rows, block = partial.shape[1:]
    me = lax.axis_index("ma")
    held = partial
    bit = 1
    while bit < n:
        own = (me // bit) % 2
        parts = held.reshape(-1, 2, rows, block)
        keep = lax.dynamic_index_in_dim(parts, own, 1, keepdims=False)
        send = lax.dynamic_index_in_dim(parts, 1 - own, 1, keepdims=False)
        got = lax.ppermute(send, "ma", pairs(n, bit))
        held = (keep.astype(jnp.float32) + got.astype(jnp.float32)).astype(jnp.bfloat16)
        bit *= 2
    return held.reshape(rows, block)


def gather_all(x, n):
    rows, block = x.shape
    me = lax.axis_index("ma")
    held = x.reshape(rows, 1, block)
    bit = n // 2
    while bit >= 1:
        own = (me // bit) % 2
        got = lax.ppermute(held, "ma", pairs(n, bit))
        first = jnp.where(own == 0, held, got)
        second = jnp.where(own == 0, got, held)
        held = jnp.stack([first, second], 2).reshape(rows, -1, block)
        bit //= 2
    return held.reshape(rows, n * block)


def to_spectra(traces, table):
    freqs = table.shape[0]
    flat = table.reshape(2 * freqs, table.shape[2]).astype(jnp.bfloat16)
    out = jnp.einsum(
        "ast,kt->ksa", traces.astype(jnp.bfloat16), flat, preferred_element_type=jnp.float32
    ).astype(jnp.bfloat16)
    return out.reshape(freqs, 2 * out.shape[1], out.shape[2])


def to_traces(spectra, table):
    freqs, double, points = spectra.shape
    sources = double // 2
    length = table.shape[2]
    depth = freqs * double
    across = spectra.reshape(depth, points).T
    owner = jnp.arange(depth, dtype=jnp.int32) % sources
    mask = (owner[None, :] == jnp.arange(sources, dtype=jnp.int32)[:, None]).astype(jnp.bfloat16)
    spread = (across[:, None, :] * mask[None]).reshape(points * sources, depth)
    tall = jnp.repeat(table.reshape(2 * freqs, length).astype(jnp.bfloat16), sources, axis=0)
    out = jnp.dot(spread, tall, preferred_element_type=jnp.float32)
    return out.reshape(points, sources, length)


def by_frequency(arrived, n):
    sources = arrived.shape[1] // 2
    points = arrived.shape[2]
    return arrived.reshape(n, 2, sources, points).transpose(1, 0, 2, 3).reshape(2, -1, points)


def by_source(spectra, n):
    points = spectra.shape[2]
    sources = spectra.shape[1] // n
    return spectra.reshape(2, n, sources, points).transpose(1, 0, 2, 3).reshape(n, -1, points)


def adjoint_kernel(d_ref, k_ref, o_ref):
    half = d_ref.shape[0] // 2
    data = d_ref[...]
    first = jnp.dot(data, k_ref[0], preferred_element_type=jnp.float32)
    second = jnp.dot(data, k_ref[1], preferred_element_type=jnp.float32)
    o_ref[0, :half] = (first[:half] + second[half:]).astype(o_ref.dtype)
    o_ref[0, half:] = (first[half:] - second[:half]).astype(o_ref.dtype)


def adjoint_product(data, flat_kernel, inner):
    sources, rows = data.shape[1], data.shape[2]
    columns = flat_kernel.shape[1]
    block = columns // inner
    tile = min(512, block)
    per_block = block // tile
    partial = pl.pallas_call(
        adjoint_kernel,
        grid=(columns // tile,),
        out_shape=jax.ShapeDtypeStruct((inner, 2 * sources, block), jnp.bfloat16),
        in_specs=[
            pl.BlockSpec((2 * sources, rows), lambda j: (0, 0)),
            pl.BlockSpec((2, rows, tile), lambda j: (0, 0, j)),
        ],
        out_specs=pl.BlockSpec(
            (1, 2 * sources, tile), lambda j: (j // per_block, 0, j % per_block)
        ),
        compiler_params=pltpu.CompilerParams(vmem_limit_bytes=60 * 1024 * 1024),
        cost_estimate=pl.CostEstimate(
            flops=8 * sources * rows * columns,
            bytes_accessed=4 * rows * columns + 4 * sources * (rows + columns),
            transcendentals=0,
        ),
        name="adjoint",
    )(data.reshape(2 * sources, rows), flat_kernel.reshape(2, rows, columns))
    return scatter_sum(partial, inner).reshape(2, sources, block)


def final_kernel(
    sums_ref, rec_ref, win_ref, g_ref, d_ref, h_ref, tall_ref, mask_ref, pick_ref,
    sol_ref, res_ref, dir_ref,
):
    tile, sources, length = rec_ref.shape
    norm_start, norm_data = sums_ref[0, 0], sums_ref[1, 0]
    cross, norm_change = sums_ref[2, 0], sums_ref[3, 0]
    step_size = norm_start / (norm_data + epsilon)
    norm_final = norm_start - 2.0 * step_size * cross + step_size * step_size * norm_change
    ratio = norm_final / (norm_start + epsilon)
    tall = tall_ref[...]

    def rows(values, mask):
        return (values[:, None, :] * mask[None]).reshape(tile * sources, -1).astype(jnp.bfloat16)

    def traces(ref):
        spread = rows(ref[...].astype(jnp.float32), mask_ref[...])
        out = jnp.dot(spread, tall, preferred_element_type=jnp.float32)
        return out.reshape(tile, sources, length)

    gradient = traces(g_ref)
    change = traces(h_ref)
    sol_ref[...] = step_size * gradient
    dir_ref[...] = (gradient - step_size * change) + ratio * gradient
    window = win_ref[...]
    ones = jnp.ones((window.shape[1], length), jnp.bfloat16)
    shape = (tile, sources, length)
    start = jnp.dot(rows(window, pick_ref[0]), ones, preferred_element_type=jnp.float32)
    stop = jnp.dot(rows(window, pick_ref[1]), ones, preferred_element_type=jnp.float32)
    samples = lax.broadcasted_iota(jnp.int32, shape, 2).astype(jnp.float32)
    rising = jnp.clip((samples - start.reshape(shape) + 1.0) / RAMP, 0.0, 1.0)
    falling = jnp.clip((stop.reshape(shape) - samples) / RAMP, 0.0, 1.0)
    image = (rising * falling) * traces(d_ref)
    res_ref[...] = rec_ref[...] - step_size * image


def final_step(sums, recorded, window_start, window_stop, returned, arrived, changed, table):
    points, sources, length = recorded.shape
    depth = returned.shape[0] * returned.shape[1]
    tile = min(128, points)

    def across(x):
        return x.reshape(depth, points).T

    place = jnp.arange(sources, dtype=jnp.int32)
    owner = jnp.arange(depth, dtype=jnp.int32) % sources
    mask = (owner[None, :] == place[:, None]).astype(jnp.float32)
    column = jnp.arange(2 * sources, dtype=jnp.int32)
    pick = jnp.stack(
        [column[None, :] == place[:, None], column[None, :] == place[:, None] + sources]
    ).astype(jnp.float32)
    tall = jnp.repeat(table.reshape(-1, length).astype(jnp.bfloat16), sources, axis=0)
    window = jnp.concatenate([window_start, window_stop], 1).astype(jnp.float32)
    whole3 = pl.BlockSpec((tile, sources, length), lambda i: (i, 0, 0))
    strip = pl.BlockSpec((tile, depth), lambda i: (i, 0))
    return pl.pallas_call(
        final_kernel,
        grid=(points // tile,),
        out_shape=[jax.ShapeDtypeStruct(recorded.shape, jnp.float32)] * 3,
        in_specs=[
            pl.BlockSpec(memory_space=pltpu.SMEM),
            whole3,
            pl.BlockSpec((tile, 2 * sources), lambda i: (i, 0)),
            strip,
            strip,
            strip,
            pl.BlockSpec((depth, length), lambda i: (0, 0)),
            pl.BlockSpec((sources, depth), lambda i: (0, 0)),
            pl.BlockSpec((2, sources, 2 * sources), lambda i: (0, 0, 0)),
        ],
        out_specs=[whole3] * 3,
        compiler_params=pltpu.CompilerParams(vmem_limit_bytes=48 * 1024 * 1024),
        cost_estimate=pl.CostEstimate(
            flops=8 * points * sources * depth * length,
            bytes_accessed=16 * points * sources * length,
            transcendentals=0,
        ),
        name="final",
    )(sums, recorded, window, across(returned), across(arrived), across(changed), tall, mask, pick)


def forward_product(model, flat_kernel, inner):
    sources = model.shape[1]
    incoming = gather_all(model.reshape(2 * sources, -1), inner)
    product = lax.dot_general(
        incoming, flat_kernel, (((1,), (1,)), ((), ())), preferred_element_type=jnp.float32
    )
    half = flat_kernel.shape[0] // 2
    real_part = product[:sources, :half] - product[sources:, half:]
    imaginary = product[sources:, :half] + product[:sources, half:]
    return jnp.stack([real_part, imaginary], 0).astype(jnp.bfloat16)


RECORDED, RETURNED, IMAGED, SECOND, CHANGED, MIXED = range(6)
PARTS = 2
GROUP = 4


def loop(start, stop, body):
    def step(i, carry):
        body(i)
        return carry

    lax.fori_loop(start, stop, step, 0)


def iota(shape, axis):
    return lax.broadcasted_iota(jnp.int32, shape, axis)


def folded(values):
    rows, columns = values.shape
    parts = values.reshape(rows // 8, 8, columns).sum(0)
    out = parts[:, :128]
    for j in range(1, columns // 128):
        out = out + parts[:, j * 128 : (j + 1) * 128]
    return out


def iteration_kernel(
    outer, inner, mixing, bins_ref, rec_ref, ker_ref, start_ref, stop_ref,
    returned_ref, imaged_ref, changed_ref, sums_ref, win_ref, spread_ref, gather_ref,
    traces, gains, window, win, spread, gather, tapered, first_out, first_in, second_out,
    second_in, total, product, image_out, image_in, core_out, core_in, line_out, line_in, model,
    summed, summed_in, normal, normal_in, mixed_out, same, stats, stats_in, stats_all,
    trace_sem, gain_sem, keep_sem, out_sem, in_sem, core_out_sem, core_in_sem, line_out_sem,
    line_in_sem, share_out_sem, share_in_sem, stats_out_sem, stats_in_sem,
):
    n = outer
    sources, points, length = traces.shape
    halves, chunks, _, double, width = first_out.shape
    pieces, piece = model.shape[2], model.shape[5]
    count = sources // halves
    depth = n * double
    block = pieces * piece
    f32, bf16 = jnp.float32, jnp.bfloat16
    me, mine = lax.axis_index("gx"), lax.axis_index("ma")
    core = mine + 1 - 2 * lax.rem(mine, 2)
    line = lax.rem(mine + 2, 4)
    corner = lax.rem(core + 2, 4)
    both = range(halves)
    sent = summed if mixing else model.at[:, 0]

    def part(i):
        return pl.ds(pl.multiple_of(i * width, width), width)

    def trace_copy(h, i, s):
        s = h * count + s
        return pltpu.make_async_copy(
            rec_ref.at[part(i), s], traces.at[s, part(i)], trace_sem.at[h, i]
        )

    def trace_wait(h, i):
        place = traces.at[h * count : (h + 1) * count, part(i)]
        pltpu.make_async_copy(place, place, trace_sem.at[h, i]).wait()

    def gain_copy(i):
        return pltpu.make_async_copy(
            ker_ref.at[:, part(i)], gains.at[:, part(i)], gain_sem.at[i]
        )

    kept = (
        (summed_in, returned_ref),
        (image_in, imaged_ref),
        (normal_in, changed_ref),
        (win, win_ref),
        (spread, spread_ref),
        (gather, gather_ref),
    )

    def keep_copy(number):
        src, dst = kept[number]
        return pltpu.make_async_copy(src, dst, keep_sem.at[number])

    def across(number, src, dst, i, peer, slot):
        return pltpu.make_async_remote_copy(
            src_ref=src.at[i, peer],
            dst_ref=dst.at[i, slot],
            send_sem=out_sem.at[number],
            recv_sem=in_sem.at[number, i],
            device_id={"gx": peer},
            device_id_type=MESH,
        )

    def send_all(number, h, src, dst, i):
        src, dst, number = src.at[h], dst.at[h], number * halves + h

        def body(k):
            peer = lax.rem(me + k, n)
            across(number, src, dst, i, peer, me).start()

        loop(1, n, body)
        dst[i, me] = src[i, me]

    def receive_all(number, h, src, dst, i):
        number = number * halves + h
        others = pl.ds(0, n - 1)
        pltpu.make_async_remote_copy(
            src_ref=src.at[h, i, others],
            dst_ref=dst.at[h, i, others],
            send_sem=out_sem.at[number],
            recv_sem=in_sem.at[number, i],
            device_id={"gx": lax.rem(me + 1, n)},
            device_id_type=MESH,
        ).wait_recv()

    def finish_all(number, src, dst, many):
        others = pl.ds(0, n - 1)
        for h in both:
            pltpu.make_async_remote_copy(
                src_ref=src.at[h, :, others],
                dst_ref=dst.at[h, :, others],
                send_sem=out_sem.at[number * halves + h],
                recv_sem=in_sem.at[number * halves + h, 0],
                device_id={"gx": lax.rem(me + 1, n)},
                device_id_type=MESH,
            ).wait_send()

    def core_copy(h, stage, which, p):
        return pltpu.make_async_remote_copy(
            src_ref=core_out.at[h, stage, which, p],
            dst_ref=core_in.at[h, stage, which, p],
            send_sem=core_out_sem,
            recv_sem=core_in_sem.at[h, stage, which, p],
            device_id={"ma": core},
            device_id_type=MESH,
        )

    def line_copy(h, stage, p):
        return pltpu.make_async_remote_copy(
            src_ref=line_out.at[h, stage, p],
            dst_ref=line_in.at[h, stage, p],
            send_sem=line_out_sem,
            recv_sem=line_in_sem.at[h, stage, p],
            device_id={"ma": line},
            device_id_type=MESH,
        )

    def share_copy(h, which, p):
        source, slot, peer = ((0, 1, core), (0, 2, line), (2, 3, core))[which]
        return pltpu.make_async_remote_copy(
            src_ref=model.at[h, source, p],
            dst_ref=model.at[h, slot, p],
            send_sem=share_out_sem.at[which],
            recv_sem=share_in_sem.at[h, which, p],
            device_id={"ma": peer},
            device_id_type=MESH,
        )

    barrier = pltpu.get_barrier_semaphore()

    def greet(k):
        pl.semaphore_signal(
            barrier, inc=1, device_id={"gx": lax.rem(me + k, n)}, device_id_type=MESH
        )

    loop(1, n, greet)
    for peer in (core, line, corner):
        pl.semaphore_signal(barrier, inc=1, device_id={"ma": peer}, device_id_type=MESH)

    for h in both:
        loop(0, chunks, lambda i: loop(0, count, lambda s: trace_copy(h, i, s).start()))

    owners = iota((n, length), 0)
    bins = jnp.zeros_like(owners)
    for f in range(n):
        bins = jnp.where(owners == f, bins_ref[f], bins)
    angles = lax.rem(bins * iota((n, length), 1), length).astype(f32) * (2.0 * math.pi / length)
    scale = math.sqrt(2.0 / length)
    real, imaginary = jnp.cos(angles) * scale, -jnp.sin(angles) * scale
    rows = []
    for f in range(n):
        for values in (real, imaginary):
            rows.append(jnp.broadcast_to(values[f : f + 1], (count, length)))
    tall = jnp.concatenate(rows, 0)
    wide = tall.T
    row_place = lax.rem(iota((depth, length), 0), count)
    column_place = lax.rem(iota((length, depth), 1), count)
    for s in range(count):
        here = slice(s * length, (s + 1) * length)
        spread[:, here] = jnp.where(row_place == s, tall, 0.0).astype(bf16)
        gather[here] = jnp.where(column_place == s, wide, 0.0).astype(bf16)
    win[:sources] = (1 - start_ref[...]).astype(f32) * (1.0 / RAMP)
    win[sources:] = stop_ref[...].astype(f32) * (1.0 / RAMP)
    stats[...] = jnp.zeros_like(stats)
    if mixing:
        sides = []
        for axis in range(2):
            owner = iota((depth, depth), axis) // double
            values = jnp.zeros_like(owner)
            for f in range(n):
                values = jnp.where(owner == f, bins_ref[f], values)
            sides.append((values, lax.rem(iota((depth, depth), axis), double)))
        alike = (sides[0][0] == sides[1][0]) & (sides[0][1] == sides[1][1])
        same[...] = jnp.where(alike, 1.0, 0.0).astype(bf16)

    samples = iota((length, width), 0).astype(f32) * (1.0 / RAMP)

    def span(s, many=1):
        return pl.ds(pl.multiple_of(s * length, length), many * length)

    def transform(out, h, i):
        result = jnp.dot(spread[...], tapered[...], preferred_element_type=f32)
        out[h, i] = result.astype(bf16).reshape(n, double, width)

    def prepare(h, i):
        trace_wait(h, i)
        if h == 0:
            gain_copy(i).start()
        for k in range(count):
            s = h * count + k
            rising = jnp.clip(samples + win[s : s + 1, part(i)], 0.0, 1.0)
            falling = jnp.clip(win[sources + s : sources + s + 1, part(i)] - samples, 0.0, 1.0)
            weight = rising * falling
            window[i, span(s)] = weight.astype(bf16)
            tapered[k * length : (k + 1) * length] = (weight * traces[s, part(i)].T).astype(bf16)
        transform(first_out, h, i)

    def record(h, i):
        prepare(h, i)
        send_all(RECORDED, h, first_out, first_in, i)

    def turned(values, sign):
        half = double // 2
        wide_values = values.astype(f32)
        low, high = wide_values[:, :half], wide_values[:, half:]
        pair = [high, -low] if sign > 0 else [-high, low]
        return jnp.concatenate(pair, 1).reshape(depth, values.shape[2]).astype(bf16)

    def adjoint_part(held, h, i, columns):
        data = held[h, i]
        return jnp.dot(
            data.reshape(depth, width), gains[0, part(i), columns], preferred_element_type=f32
        ) + jnp.dot(turned(data, 1), gains[1, part(i), columns], preferred_element_type=f32)

    rounds = ((RECORDED, first_out, first_in), (SECOND, second_out, second_in))

    def accumulate(stage, h, i):
        number, src, held = rounds[stage]
        receive_all(number, h, src, held, i)
        if stage == 0 and h == 0:
            gain_copy(i).wait()

        def body(j):
            columns = pl.ds(pl.multiple_of(j * block, block), block)
            update = adjoint_part(held, h, i, columns)
            total[h, :, columns] = update if i == 0 else total[h, :, columns] + update

        loop(0, inner, body)

    last = chunks - 1

    def pack(values):
        return values.astype(bf16).reshape(n, double, piece)

    def whole(where):
        return pl.ds(pl.multiple_of(where * block, block), block)

    def close(stage, h, where):
        update = adjoint_part(rounds[stage][2], h, last, whole(where))
        return update if chunks == 1 else total[h, :, whole(where)] + update

    def column(where, p):
        return pl.ds(pl.multiple_of(where * block + p * piece, piece), piece)

    def from_core(stage, h, which, p):
        core_copy(h, stage, which, p).wait_recv()
        return core_in[h, stage, which, p].reshape(depth, piece).astype(f32)

    def reduce_out(stage, h):
        number, src, held = rounds[stage]
        receive_all(number, h, src, held, last)
        if stage == 0 and h == 0:
            gain_copy(last).wait()

        def to_core(which, where):
            values = close(stage, h, where)
            for p in range(pieces):
                core_out[h, stage, which, p] = pack(values[:, p * piece : (p + 1) * piece])
                core_copy(h, stage, which, p).start()

        def to_line(p):
            values = total[h, :, column(line, p)] + from_core(stage, h, 0, p)
            line_out[h, stage, p] = pack(values)
            line_copy(h, stage, p).start()

        to_core(0, corner)
        total[h, :, whole(line)] = close(stage, h, line)
        to_core(1, core)
        loop(0, pieces, to_line)
        total[h, :, whole(mine)] = close(stage, h, mine)

    def reduced(stage, h, p):
        values = total[h, :, column(mine, p)] + from_core(stage, h, 1, p)
        line_copy(h, stage, p).wait_recv()
        return pack(values + line_in[h, stage, p].reshape(depth, piece).astype(f32))

    def flat(values):
        return values.reshape(depth, values.shape[2]).astype(f32)

    def forward_part(h, slot, where, many, rows):
        dims = (((1,), (1,)), ((), ()))
        out = None
        for p in many:
            values = model[h, slot, p]
            for number, side in enumerate((values.reshape(depth, piece), turned(values, -1))):
                update = lax.dot_general(
                    gains[number, rows, column(where, p)], side, dims,
                    preferred_element_type=f32,
                )
                out = update if out is None else out + update
        return out

    def forward(h, slot, where, many, first=False):
        tile_rows = 2 * width if chunks % 2 == 0 else width

        def body(i):
            rows = pl.ds(pl.multiple_of(i * tile_rows, tile_rows), tile_rows)
            update = forward_part(h, slot, where, many, rows)
            product[h, rows] = update if first else product[h, rows] + update

        loop(0, points // tile_rows, body)

    def share(h, p):
        share_copy(h, 1, p).start()
        share_copy(h, 0, p).start()

    def keep(h, p):
        values = reduced(0, h, p)
        if mixing:
            summed[h, p] = values
            send_all(RETURNED, h, sent, summed_in, p)
        else:
            model[h, 0, p] = values
            share(h, p)
            if h == 0:
                send_all(RETURNED, h, sent, summed_in, p)
            held = flat(values)
            stats[0] += folded(held * held)

    def mix(h, p):
        receive_all(RETURNED, h, sent, summed_in, p)
        arrived = summed_in[h, p].reshape(depth, piece)
        values = jnp.dot(same[...], arrived, preferred_element_type=f32)
        mixed_out[h, p] = values.astype(bf16).reshape(n, double, piece)
        send_all(MIXED, h, mixed_out, model.at[:, 0], p)

    def unmix(h, p):
        receive_all(MIXED, h, mixed_out, model.at[:, 0], p)
        share(h, p)

    def own_forward(h):
        forward(h, 0, mine, range(pieces), first=True)
        for p in range(pieces):
            share_copy(h, 0, p).wait_recv()
        forward(h, 1, core, range(pieces))

    def relay(h, p):
        share_copy(h, 1, p).wait_recv()
        share_copy(h, 2, p).start()

    def from_line(h, p):
        relay(h, p)
        if p % 2:
            forward(h, 2, line, (p - 1, p))
        elif p == pieces - 1:
            forward(h, 2, line, (p,))

    def imaging(h):
        for p in range(pieces):
            share_copy(h, 2, p).wait_recv()

        def body(i):
            values = product[h, part(i)] + forward_part(h, 3, corner, range(pieces), part(i))
            image_out[h, i] = values.T.astype(bf16).reshape(n, double, width)
            send_all(IMAGED, h, image_out, image_in, i)

        loop(0, chunks, body)

    def again(h, i):
        receive_all(IMAGED, h, image_out, image_in, i)
        arrived = image_in[h, i].reshape(depth, width)
        for j in range(0, count, GROUP):
            weight = window[i, span(h * count + j, GROUP)].astype(f32)
            rows = slice(j * length, (j + GROUP) * length)
            values = jnp.dot(gather[rows], arrived, preferred_element_type=f32) * weight
            stats[1] += folded(values * values)
            tapered[rows] = (values * weight).astype(bf16)
        transform(second_out, h, i)
        send_all(SECOND, h, second_out, second_in, i)

    def change(h, p):
        values = reduced(1, h, p)
        normal[h, p] = values
        send_all(CHANGED, h, normal, normal_in, p)
        if not mixing:
            held = flat(values)
            stats[2] += folded(held * flat(model[h, 0, p]))
            stats[3] += folded(held * held)

    prepare(0, 0)
    pl.semaphore_wait(barrier, n + 2)
    send_all(RECORDED, 0, first_out, first_in, 0)
    for h in both:
        loop(0 if h else 1, chunks, lambda i: record(h, i))
    for number in (3, 4, 5):
        keep_copy(number).start()
    for i in range(last):
        accumulate(0, 0, i)
    reduce_out(0, 0)
    def each(body, h):
        loop(0, pieces, lambda p: body(h, p))

    for h in both:
        more = h + 1 < halves
        if more:
            for i in range(last):
                accumulate(0, h + 1, i)
        if not mixing or h == 0:
            each(keep, h)
        if more:
            reduce_out(0, h + 1)
        if mixing:
            if h == 0:
                each(mix, h)
            if more:
                each(keep, h + 1)
            each(unmix, h)
            if more:
                each(mix, h + 1)
        own_forward(h)
        for p in range(max(chunks, pieces)):
            if h and p < chunks:
                again(h - 1, p)
            if p < pieces:
                from_line(h, p)
        imaging(h)
    other = halves - 1
    for i in range(last):
        accumulate(1, 0, i)
        if i and i <= chunks // 2:
            again(other, i - 1)
    reduce_out(1, 0)
    for i in range(chunks // 2 if last > chunks // 2 else max(last - 1, 0), chunks):
        again(other, i)
    for h in both:
        if h:
            for i in range(last):
                accumulate(1, h, i)
            reduce_out(1, h)
        each(change, h)
        if h == 0 and not mixing:
            for k in range(1, halves):
                loop(0, pieces, lambda p: send_all(RETURNED, k, sent, summed_in, p))
    keep_copy(1).start()
    if mixing:

        def norms(h, p):
            receive_all(CHANGED, h, normal, normal_in, p)
            before = summed_in[h, p].reshape(depth, piece)
            after = normal_in[h, p].reshape(depth, piece)
            mixed_before = jnp.dot(same[...], before, preferred_element_type=f32)
            mixed_after = jnp.dot(same[...], after, preferred_element_type=f32)
            stats[0] += folded(before.astype(f32) * mixed_before)
            stats[2] += folded(after.astype(f32) * mixed_before)
            stats[3] += folded(after.astype(f32) * mixed_after)

        keep_copy(0).start()
        for h in both:
            loop(0, pieces, lambda p: norms(h, p))
    else:
        for h in both:
            loop(0, pieces, lambda p: receive_all(RETURNED, h, sent, summed_in, p))
        keep_copy(0).start()

    def stats_copy(which, peer):
        return pltpu.make_async_remote_copy(
            src_ref=stats,
            dst_ref=stats_in.at[which],
            send_sem=stats_out_sem.at[which],
            recv_sem=stats_in_sem.at[which],
            device_id={"ma": peer},
            device_id_type=MESH,
        )

    near = [stats_copy(which, peer) for which, peer in enumerate((core, line, corner))]
    for copy in near:
        copy.start()
    for copy in near:
        copy.wait_recv()
    stats_in[3] = (stats[...] + stats_in[0]) + (stats_in[1] + stats_in[2])

    def stats_across(peer, slot):
        return pltpu.make_async_remote_copy(
            src_ref=stats_in.at[3],
            dst_ref=stats_all.at[slot],
            send_sem=stats_out_sem.at[3],
            recv_sem=stats_in_sem.at[3],
            device_id={"gx": peer},
            device_id_type=MESH,
        )

    loop(1, n, lambda k: stats_across(lax.rem(me + k, n), me).start())
    stats_all[me] = stats_in[3]
    others = stats_all.at[pl.ds(0, n - 1)]
    every = pltpu.make_async_remote_copy(
        src_ref=others,
        dst_ref=others,
        send_sem=stats_out_sem.at[3],
        recv_sem=stats_in_sem.at[3],
        device_id={"gx": lax.rem(me + 1, n)},
        device_id_type=MESH,
    )
    if not mixing:
        for h in both:
            loop(0, pieces, lambda p: receive_all(CHANGED, h, normal, normal_in, p))
    keep_copy(2).start()
    every.wait_recv()
    sums_ref[...] = jnp.sum(stats_all[...], axis=0)

    for copy in near:
        copy.wait_send()
    every.wait_send()
    finish_all(RECORDED, first_out, first_in, chunks)
    finish_all(RETURNED, sent, summed_in, pieces)
    finish_all(IMAGED, image_out, image_in, chunks)
    finish_all(SECOND, second_out, second_in, chunks)
    finish_all(CHANGED, normal, normal_in, pieces)
    if mixing:
        finish_all(MIXED, mixed_out, model.at[:, 0], pieces)

    def finish(src, dst, sem, peer):
        pltpu.make_async_remote_copy(
            src_ref=src,
            dst_ref=dst,
            send_sem=sem,
            recv_sem=stats_in_sem.at[0],
            device_id={"ma": peer},
            device_id_type=MESH,
        ).wait_send()

    finish(core_out, core_in, core_out_sem, core)
    finish(line_out, line_in, line_out_sem, line)
    for which, peer in ((0, core), (1, line), (2, core)):
        finish(model.at[:, 0], model.at[:, 1], share_out_sem.at[which], peer)
    for number in range(6):
        keep_copy(number).wait()


def iteration(outer, inner, mixing, freq_bins, recorded, kernel, window_start, window_stop):
    points, sources, length = recorded.shape
    columns = kernel.shape[2]
    halves = PARTS
    count = sources // halves
    double = 2 * count
    depth = outer * double
    block = columns // inner
    width, piece = min(256, points), min(256, block)
    chunks, pieces = points // width, block // piece
    f32, bf16 = jnp.float32, jnp.bfloat16
    by_chunk = (halves, chunks, outer, double, width)
    by_piece = (halves, pieces, outer, double, piece)
    stack = by_piece[1:]
    vmem = pl.BlockSpec(memory_space=pltpu.VMEM)
    hbm = pl.BlockSpec(memory_space=pl.ANY)
    dma = pltpu.SemaphoreType.DMA
    exchanges = 6 if mixing else 5
    extra = by_piece if mixing else (halves, 1, 1, 16, 128)
    return pl.pallas_call(
        functools.partial(iteration_kernel, outer, inner, mixing),
        out_shape=[
            jax.ShapeDtypeStruct(by_piece, bf16),
            jax.ShapeDtypeStruct(by_chunk, bf16),
            jax.ShapeDtypeStruct(by_piece, bf16),
            jax.ShapeDtypeStruct((4, 8, 128), f32),
            jax.ShapeDtypeStruct((2 * sources, points), f32),
            jax.ShapeDtypeStruct((depth, count * length), bf16),
            jax.ShapeDtypeStruct((count * length, depth), bf16),
        ],
        in_specs=[pl.BlockSpec(memory_space=pltpu.SMEM), hbm, hbm, vmem, vmem],
        out_specs=[hbm, hbm, hbm, vmem, hbm, hbm, hbm],
        scratch_shapes=[
            pltpu.VMEM((sources, points, length), f32),
            pltpu.VMEM((2, points, columns), bf16),
            pltpu.VMEM((chunks, sources * length, width), bf16),
            pltpu.VMEM((2 * sources, points), f32),
            pltpu.VMEM((depth, count * length), bf16),
            pltpu.VMEM((count * length, depth), bf16),
            pltpu.VMEM((count * length, width), bf16),
            pltpu.VMEM(by_chunk, bf16),
            pltpu.VMEM(by_chunk, bf16),
            pltpu.VMEM(by_chunk, bf16),
            pltpu.VMEM(by_chunk, bf16),
            pltpu.VMEM((halves, depth, columns), f32),
            pltpu.VMEM((halves, points, depth), f32),
            pltpu.VMEM(by_chunk, bf16),
            pltpu.VMEM(by_chunk, bf16),
            pltpu.VMEM((halves, 2, 2) + stack, bf16),
            pltpu.VMEM((halves, 2, 2) + stack, bf16),
            pltpu.VMEM((halves, 2) + stack, bf16),
            pltpu.VMEM((halves, 2) + stack, bf16),
            pltpu.VMEM((halves, 4) + stack, bf16),
            pltpu.VMEM(extra, bf16),
            pltpu.VMEM(by_piece, bf16),
            pltpu.VMEM(by_piece, bf16),
            pltpu.VMEM(by_piece, bf16),
            pltpu.VMEM(extra, bf16),
            pltpu.VMEM((depth, depth) if mixing else (16, 128), bf16),
            pltpu.VMEM((4, 8, 128), f32),
            pltpu.VMEM((4, 4, 8, 128), f32),
            pltpu.VMEM((outer, 4, 8, 128), f32),
            dma((halves, chunks)),
            dma((chunks,)),
            dma((6,)),
            dma((exchanges * halves,)),
            dma((exchanges * halves, max(chunks, pieces))),
            dma,
            dma((halves, 2, 2, pieces)),
            dma,
            dma((halves, 2, pieces)),
            dma((3,)),
            dma((halves, 3, pieces)),
            dma((4,)),
            dma((4,)),
        ],
        compiler_params=pltpu.CompilerParams(
            collective_id=6 if mixing else 5,
            has_side_effects=True,
            vmem_limit_bytes=67_000_000,
        ),
        name="iteration_mixed" if mixing else "iteration",
    )(freq_bins, recorded, kernel, window_start, window_stop)


def write_kernel(
    sums_ref, rec_ref, win_ref, spread_ref, gather_ref, ret_ref, ima_ref, cha_ref,
    sol_ref, res_ref, dir_ref, traces, solved, rest, ahead, in_sem, out_sem,
):
    sources, points, length = traces.shape
    halves, chunks, outer, double, width = ima_ref.shape
    depth = outer * double
    count = sources // halves
    f32, bf16 = jnp.float32, jnp.bfloat16

    def part(i):
        return pl.ds(pl.multiple_of(i * width, width), width)

    def load(i, s):
        return pltpu.make_async_copy(
            rec_ref.at[part(i), s], traces.at[s, part(i)], in_sem.at[i]
        )

    staged = ((solved, sol_ref), (ahead, dir_ref), (rest, res_ref))

    def store(number, i, s):
        src, dst = staged[number]
        return pltpu.make_async_copy(
            src.at[s, part(i)], dst.at[part(i), s], out_sem.at[number]
        )

    loop(0, chunks, lambda i: loop(0, sources, lambda s: load(i, s).start()))
    norm_start, norm_data = jnp.sum(sums_ref[0]), jnp.sum(sums_ref[1])
    cross, norm_change = jnp.sum(sums_ref[2]), jnp.sum(sums_ref[3])
    step_size = norm_start / (norm_data + epsilon)
    norm_final = norm_start - 2.0 * step_size * cross + step_size * step_size * norm_change
    ratio = norm_final / (norm_start + epsilon)
    samples = iota((length, width), 0).astype(f32) * (1.0 / RAMP)

    def chunk(i):
        place = traces.at[:, part(i)]
        pltpu.make_async_copy(place, place, in_sem.at[i]).wait()
        for h in range(halves):
            before = ret_ref[h, i].reshape(depth, width).astype(f32).T.astype(bf16)
            after = cha_ref[h, i].reshape(depth, width).astype(f32).T.astype(bf16)
            arrived = ima_ref[h, i].reshape(depth, width)

            def pair(j):
                spans = pl.ds(pl.multiple_of(j * 2 * length, length), 2 * length)
                table = spread_ref[:, spans]
                first = h * count + 2 * j
                for r in range(0, width, 128):
                    rows = pl.ds(pl.multiple_of(i * width + r, 128), 128)
                    gradient = jnp.dot(before[r : r + 128], table, preferred_element_type=f32)
                    change = jnp.dot(after[r : r + 128], table, preferred_element_type=f32)
                    for k in range(2):
                        here = slice(k * length, (k + 1) * length)
                        g, c = gradient[:, here], change[:, here]
                        solved[first + k, rows] = step_size * g
                        ahead[first + k, rows] = (g - step_size * c) + ratio * g
                for k in range(2):
                    s = first + k
                    store(0, i, s).start()
                    store(1, i, s).start()
                    rising = jnp.clip(samples + win_ref[pl.ds(s, 1), part(i)], 0.0, 1.0)
                    falling = jnp.clip(
                        win_ref[pl.ds(sources + s, 1), part(i)] - samples, 0.0, 1.0
                    )
                    spans = pl.ds(pl.multiple_of((2 * j + k) * length, length), length)
                    image = jnp.dot(gather_ref[spans], arrived, preferred_element_type=f32)
                    image = (rising * falling) * image
                    rest[s, part(i)] = traces[s, part(i)] - step_size * image.T
                    store(2, i, s).start()

            def some(j):
                for k in range(2):
                    pair(2 * j + k)

            loop(0, count // 4, some)

    loop(0, chunks, chunk)
    for number in range(3):
        src = staged[number][0]
        pltpu.make_async_copy(src, src, out_sem.at[number]).wait()


def write(recorded, returned, imaged, changed, sums, windows, spread, gather):
    points, sources, length = recorded.shape
    halves, chunks, outer, double, width = imaged.shape
    depth = outer * double
    vmem = pl.BlockSpec(memory_space=pltpu.VMEM)
    hbm = pl.BlockSpec(memory_space=pl.ANY)
    f32 = jnp.float32
    staged = pltpu.VMEM((sources, points, length), f32)
    return pl.pallas_call(
        write_kernel,
        out_shape=[jax.ShapeDtypeStruct(recorded.shape, f32)] * 3,
        in_specs=[vmem, hbm] + [vmem] * 6,
        out_specs=[hbm] * 3,
        scratch_shapes=[
            staged,
            staged,
            staged,
            staged,
            pltpu.SemaphoreType.DMA((chunks,)),
            pltpu.SemaphoreType.DMA((3,)),
        ],
        compiler_params=pltpu.CompilerParams(vmem_limit_bytes=56 * 1024 * 1024),
        cost_estimate=pl.CostEstimate(
            flops=6 * points * sources * depth * length,
            bytes_accessed=16 * points * sources * length,
            transcendentals=0,
        ),
        name="write",
    )(sums, recorded, windows, spread, gather, returned, imaged, changed)


def fused(outer, inner, recorded, kernel, freq_bins, window_start, window_stop):
    same = freq_bins[:, None] == freq_bins[None, :]
    repeated = jnp.sum(same.astype(jnp.int32)) > freq_bins.shape[0]
    gains = kernel.reshape(2, kernel.shape[2], kernel.shape[3])
    results = lax.cond(
        repeated,
        lambda *x: tuple(iteration(outer, inner, True, *x)),
        lambda *x: tuple(iteration(outer, inner, False, *x)),
        freq_bins, recorded, gains, window_start.T, window_stop.T,
    )
    return tuple(write(recorded, *results))


def fits(outer, inner, recorded, kernel):
    points, sources, length = recorded.shape
    columns = kernel.shape[3]
    return (
        inner == 4
        and kernel.shape[1] == 1
        and columns == inner * points
        and sources % (PARTS * 8) == 0
        and length % 128 == 0
        and points % 256 == 0
        and outer * 2 * (sources // PARTS) % 128 == 0
        and points * (4 * columns + 6 * sources * length) < 30_000_000
    )


def per_device(outer, inner, recorded, kernel, freq_bins, window_start, window_stop):
    if fits(outer, inner, recorded, kernel):
        return fused(outer, inner, recorded, kernel, freq_bins, window_start, window_stop)
    length = recorded.shape[2]
    table = phase_table(freq_bins, length)
    weights = taper_weights(window_start, window_stop, length)
    flat_kernel = kernel.reshape(2 * kernel.shape[2], kernel.shape[3])

    data = by_frequency(exchange(to_spectra(weights * recorded, table), outer, 0), outer)
    adjoint = adjoint_product(data, flat_kernel, inner)
    returned = lax.all_to_all(
        by_source(adjoint, outer), "gx", split_axis=0, concat_axis=0, tiled=True
    )

    same = freq_bins[:, None] == freq_bins[None, :]
    repeated = jnp.sum(same.astype(jnp.int32)) > freq_bins.shape[0]

    def combined(spectra):
        parts = lax.all_to_all(
            by_source(spectra, outer), "gx", split_axis=0, concat_axis=0, tiled=True
        )
        mixed = jnp.einsum(
            "gf,fxa->gxa",
            same.astype(jnp.bfloat16),
            parts,
            preferred_element_type=jnp.float32,
        ).astype(jnp.bfloat16)
        back = lax.all_to_all(mixed, "gx", split_axis=0, concat_axis=0, tiled=True)
        return by_frequency(back, outer)

    model = lax.cond(repeated, combined, lambda spectra: spectra, adjoint)
    outgoing = by_source(forward_product(model, flat_kernel, inner), outer)
    imaged = exchange(outgoing, outer, 1)
    image = weights * to_traces(imaged, table)
    second = by_frequency(exchange(to_spectra(weights * image, table), outer, 2), outer)
    normal = adjoint_product(second, flat_kernel, inner)
    changed = exchange(by_source(normal, outer), outer, 3)

    double, points = returned.shape[1:]
    depth = freq_bins.shape[0] * double
    eye = jnp.eye(double, dtype=jnp.bfloat16)
    mixing = (same.astype(jnp.bfloat16)[:, None, :, None] * eye[None, :, None, :]).reshape(
        depth, depth
    )
    flat_g = returned.reshape(depth, points)
    flat_h = changed.reshape(depth, points)
    mixed_g = jnp.dot(mixing, flat_g, preferred_element_type=jnp.float32)
    mixed_h = jnp.dot(mixing, flat_h, preferred_element_type=jnp.float32)
    sums = jnp.stack(
        [
            jnp.sum(flat_g.astype(jnp.float32) * mixed_g),
            jnp.sum(image * image),
            jnp.sum(mixed_g * flat_h.astype(jnp.float32)),
            jnp.sum(flat_h.astype(jnp.float32) * mixed_h),
        ]
    )
    sums = total(jnp.broadcast_to(jnp.tile(sums, 2)[:, None], (8, 128)), outer, inner, 4)
    if recorded.shape[1] % 8 == 0:
        return tuple(
            final_step(
                sums, recorded, window_start, window_stop, returned, imaged, changed, table
            )
        )
    gradient = to_traces(returned, table)
    change = to_traces(changed, table)
    norm_start, norm_data, cross, norm_change = sums[0, 0], sums[1, 0], sums[2, 0], sums[3, 0]
    step_size = norm_start / (norm_data + epsilon)
    norm_final = norm_start - 2.0 * step_size * cross + step_size * step_size * norm_change
    solution = step_size * gradient
    residual = recorded - step_size * image
    direction = gradient - step_size * change + norm_final / (norm_start + epsilon) * gradient
    return (solution, residual, direction)


def solution(mesh):
    in_specs = (P("ma", "gx", None), P(None, "gx", "ma", None), P(), P("ma", "gx"), P("ma", "gx"))
    out_specs = (P("ma", "gx", None), P("ma", "gx", None), P("ma", "gx", None))
    return jax.shard_map(
        functools.partial(per_device, mesh.shape["gx"], mesh.shape["ma"]),
        mesh=mesh,
        in_specs=in_specs,
        out_specs=out_specs,
        check_vma=False,
    )
```

```python
import functools
import math

import jax
import jax.numpy as jnp
from jax import lax
from jax.experimental import pallas as pl
from jax.experimental.pallas import tpu as pltpu
from jax.sharding import PartitionSpec as P

RAMP = 8
MESH = pl.DeviceIdType.MESH

epsilon = 1e-06


def phase_table(freq_bins, length):
    samples = jnp.arange(length, dtype=jnp.int32)
    angles = (freq_bins[:, None] * samples[None, :] % length).astype(jnp.float32) * (
        2.0 * math.pi / length
    )
    return jnp.stack([jnp.cos(angles), -jnp.sin(angles)], 1) * math.sqrt(2.0 / length)


def taper_weights(window_start, window_stop, length):
    samples = jnp.arange(length, dtype=jnp.float32)
    rising = jnp.clip(
        (samples[None, None, :] - window_start[:, :, None].astype(jnp.float32) + 1.0) / RAMP,
        0.0,
        1.0,
    )
    falling = jnp.clip(
        (window_stop[:, :, None].astype(jnp.float32) - samples[None, None, :]) / RAMP, 0.0, 1.0
    )
    return rising * falling


def exchange_kernel(n, x_ref, o_ref, send_sem, recv_sem, own_sem):
    me = lax.axis_index("gx")
    barrier = pltpu.get_barrier_semaphore()
    for k in range(1, n):
        pl.semaphore_signal(
            barrier, inc=1, device_id={"gx": lax.rem(me + k, n)}, device_id_type=MESH
        )
    own = pltpu.make_async_copy(x_ref.at[me], o_ref.at[me], own_sem)
    own.start()
    pl.semaphore_wait(barrier, n - 1)
    copies = []
    for k in range(1, n):
        peer = lax.rem(me + k, n)
        copy = pltpu.make_async_remote_copy(
            src_ref=x_ref.at[peer],
            dst_ref=o_ref.at[me],
            send_sem=send_sem.at[k],
            recv_sem=recv_sem.at[k],
            device_id={"gx": peer},
            device_id_type=MESH,
        )
        copy.start()
        copies.append(copy)
    own.wait()
    for copy in copies:
        copy.wait()


def exchange(x, n, number):
    return pl.pallas_call(
        functools.partial(exchange_kernel, n),
        out_shape=jax.ShapeDtypeStruct(x.shape, x.dtype),
        in_specs=[pl.BlockSpec(memory_space=pltpu.VMEM)],
        out_specs=pl.BlockSpec(memory_space=pltpu.VMEM),
        scratch_shapes=[
            pltpu.SemaphoreType.DMA((n,)),
            pltpu.SemaphoreType.DMA((n,)),
            pltpu.SemaphoreType.DMA,
        ],
        compiler_params=pltpu.CompilerParams(collective_id=number, has_side_effects=True),
        name=f"exchange{number}",
    )(x)


def total_kernel(outer, inner, x_ref, o_ref, held, send_sem, recv_sem):
    n = outer * inner
    me = lax.axis_index("gx") * inner + lax.axis_index("ma")
    barrier = pltpu.get_barrier_semaphore()

    def place(k):
        peer = lax.rem(me + k, n)
        return (peer // inner, lax.rem(peer, inner))

    for k in range(1, n):
        pl.semaphore_signal(barrier, inc=1, device_id=place(k), device_id_type=MESH)
    pl.semaphore_wait(barrier, n - 1)
    copies = []
    for k in range(1, n):
        copy = pltpu.make_async_remote_copy(
            src_ref=x_ref,
            dst_ref=held.at[me],
            send_sem=send_sem.at[k],
            recv_sem=recv_sem.at[k],
            device_id=place(k),
            device_id_type=MESH,
        )
        copy.start()
        copies.append(copy)
    held[me] = x_ref[...]
    for copy in copies:
        copy.wait()
    o_ref[...] = jnp.sum(held[...], axis=0)


def total(x, outer, inner, number):
    n = outer * inner
    return pl.pallas_call(
        functools.partial(total_kernel, outer, inner),
        out_shape=jax.ShapeDtypeStruct(x.shape, x.dtype),
        in_specs=[pl.BlockSpec(memory_space=pltpu.VMEM)],
        out_specs=pl.BlockSpec(memory_space=pltpu.VMEM),
        scratch_shapes=[
            pltpu.VMEM((n,) + x.shape, x.dtype),
            pltpu.SemaphoreType.DMA((n,)),
            pltpu.SemaphoreType.DMA((n,)),
        ],
        compiler_params=pltpu.CompilerParams(collective_id=number, has_side_effects=True),
        name=f"total{number}",
    )(x)


def pairs(n, bit):
    return [(i, i ^ bit) for i in range(n)]


def scatter_sum(partial, n):
    rows, block = partial.shape[1:]
    me = lax.axis_index("ma")
    held = partial
    bit = 1
    while bit < n:
        own = (me // bit) % 2
        parts = held.reshape(-1, 2, rows, block)
        keep = lax.dynamic_index_in_dim(parts, own, 1, keepdims=False)
        send = lax.dynamic_index_in_dim(parts, 1 - own, 1, keepdims=False)
        got = lax.ppermute(send, "ma", pairs(n, bit))
        held = (keep.astype(jnp.float32) + got.astype(jnp.float32)).astype(jnp.bfloat16)
        bit *= 2
    return held.reshape(rows, block)


def gather_all(x, n):
    rows, block = x.shape
    me = lax.axis_index("ma")
    held = x.reshape(rows, 1, block)
    bit = n // 2
    while bit >= 1:
        own = (me // bit) % 2
        got = lax.ppermute(held, "ma", pairs(n, bit))
        first = jnp.where(own == 0, held, got)
        second = jnp.where(own == 0, got, held)
        held = jnp.stack([first, second], 2).reshape(rows, -1, block)
        bit //= 2
    return held.reshape(rows, n * block)


def to_spectra(traces, table):
    freqs = table.shape[0]
    flat = table.reshape(2 * freqs, table.shape[2]).astype(jnp.bfloat16)
    out = jnp.einsum(
        "ast,kt->ksa", traces.astype(jnp.bfloat16), flat, preferred_element_type=jnp.float32
    ).astype(jnp.bfloat16)
    return out.reshape(freqs, 2 * out.shape[1], out.shape[2])


def to_traces(spectra, table):
    freqs, double, points = spectra.shape
    sources = double // 2
    length = table.shape[2]
    depth = freqs * double
    across = spectra.reshape(depth, points).T
    owner = jnp.arange(depth, dtype=jnp.int32) % sources
    mask = (owner[None, :] == jnp.arange(sources, dtype=jnp.int32)[:, None]).astype(jnp.bfloat16)
    spread = (across[:, None, :] * mask[None]).reshape(points * sources, depth)
    tall = jnp.repeat(table.reshape(2 * freqs, length).astype(jnp.bfloat16), sources, axis=0)
    out = jnp.dot(spread, tall, preferred_element_type=jnp.float32)
    return out.reshape(points, sources, length)


def by_frequency(arrived, n):
    sources = arrived.shape[1] // 2
    points = arrived.shape[2]
    return arrived.reshape(n, 2, sources, points).transpose(1, 0, 2, 3).reshape(2, -1, points)


def by_source(spectra, n):
    points = spectra.shape[2]
    sources = spectra.shape[1] // n
    return spectra.reshape(2, n, sources, points).transpose(1, 0, 2, 3).reshape(n, -1, points)


def adjoint_kernel(d_ref, k_ref, o_ref):
    half = d_ref.shape[0] // 2
    data = d_ref[...]
    first = jnp.dot(data, k_ref[0], preferred_element_type=jnp.float32)
    second = jnp.dot(data, k_ref[1], preferred_element_type=jnp.float32)
    o_ref[0, :half] = (first[:half] + second[half:]).astype(o_ref.dtype)
    o_ref[0, half:] = (first[half:] - second[:half]).astype(o_ref.dtype)


def adjoint_product(data, flat_kernel, inner):
    sources, rows = data.shape[1], data.shape[2]
    columns = flat_kernel.shape[1]
    block = columns // inner
    tile = min(512, block)
    per_block = block // tile
    partial = pl.pallas_call(
        adjoint_kernel,
        grid=(columns // tile,),
        out_shape=jax.ShapeDtypeStruct((inner, 2 * sources, block), jnp.bfloat16),
        in_specs=[
            pl.BlockSpec((2 * sources, rows), lambda j: (0, 0)),
            pl.BlockSpec((2, rows, tile), lambda j: (0, 0, j)),
        ],
        out_specs=pl.BlockSpec(
            (1, 2 * sources, tile), lambda j: (j // per_block, 0, j % per_block)
        ),
        compiler_params=pltpu.CompilerParams(vmem_limit_bytes=60 * 1024 * 1024),
        cost_estimate=pl.CostEstimate(
            flops=8 * sources * rows * columns,
            bytes_accessed=4 * rows * columns + 4 * sources * (rows + columns),
            transcendentals=0,
        ),
        name="adjoint",
    )(data.reshape(2 * sources, rows), flat_kernel.reshape(2, rows, columns))
    return scatter_sum(partial, inner).reshape(2, sources, block)


def final_kernel(
    sums_ref, rec_ref, win_ref, g_ref, d_ref, h_ref, tall_ref, mask_ref, pick_ref,
    sol_ref, res_ref, dir_ref,
):
    tile, sources, length = rec_ref.shape
    norm_start, norm_data = sums_ref[0, 0], sums_ref[1, 0]
    cross, norm_change = sums_ref[2, 0], sums_ref[3, 0]
    step_size = norm_start / (norm_data + epsilon)
    norm_final = norm_start - 2.0 * step_size * cross + step_size * step_size * norm_change
    ratio = norm_final / (norm_start + epsilon)
    tall = tall_ref[...]

    def rows(values, mask):
        return (values[:, None, :] * mask[None]).reshape(tile * sources, -1).astype(jnp.bfloat16)

    def traces(ref):
        spread = rows(ref[...].astype(jnp.float32), mask_ref[...])
        out = jnp.dot(spread, tall, preferred_element_type=jnp.float32)
        return out.reshape(tile, sources, length)

    gradient = traces(g_ref)
    change = traces(h_ref)
    sol_ref[...] = step_size * gradient
    dir_ref[...] = (gradient - step_size * change) + ratio * gradient
    window = win_ref[...]
    ones = jnp.ones((window.shape[1], length), jnp.bfloat16)
    shape = (tile, sources, length)
    start = jnp.dot(rows(window, pick_ref[0]), ones, preferred_element_type=jnp.float32)
    stop = jnp.dot(rows(window, pick_ref[1]), ones, preferred_element_type=jnp.float32)
    samples = lax.broadcasted_iota(jnp.int32, shape, 2).astype(jnp.float32)
    rising = jnp.clip((samples - start.reshape(shape) + 1.0) / RAMP, 0.0, 1.0)
    falling = jnp.clip((stop.reshape(shape) - samples) / RAMP, 0.0, 1.0)
    image = (rising * falling) * traces(d_ref)
    res_ref[...] = rec_ref[...] - step_size * image


def final_step(sums, recorded, window_start, window_stop, returned, arrived, changed, table):
    points, sources, length = recorded.shape
    depth = returned.shape[0] * returned.shape[1]
    tile = min(128, points)

    def across(x):
        return x.reshape(depth, points).T

    place = jnp.arange(sources, dtype=jnp.int32)
    owner = jnp.arange(depth, dtype=jnp.int32) % sources
    mask = (owner[None, :] == place[:, None]).astype(jnp.float32)
    column = jnp.arange(2 * sources, dtype=jnp.int32)
    pick = jnp.stack(
        [column[None, :] == place[:, None], column[None, :] == place[:, None] + sources]
    ).astype(jnp.float32)
    tall = jnp.repeat(table.reshape(-1, length).astype(jnp.bfloat16), sources, axis=0)
    window = jnp.concatenate([window_start, window_stop], 1).astype(jnp.float32)
    whole3 = pl.BlockSpec((tile, sources, length), lambda i: (i, 0, 0))
    strip = pl.BlockSpec((tile, depth), lambda i: (i, 0))
    return pl.pallas_call(
        final_kernel,
        grid=(points // tile,),
        out_shape=[jax.ShapeDtypeStruct(recorded.shape, jnp.float32)] * 3,
        in_specs=[
            pl.BlockSpec(memory_space=pltpu.SMEM),
            whole3,
            pl.BlockSpec((tile, 2 * sources), lambda i: (i, 0)),
            strip,
            strip,
            strip,
            pl.BlockSpec((depth, length), lambda i: (0, 0)),
            pl.BlockSpec((sources, depth), lambda i: (0, 0)),
            pl.BlockSpec((2, sources, 2 * sources), lambda i: (0, 0, 0)),
        ],
        out_specs=[whole3] * 3,
        compiler_params=pltpu.CompilerParams(vmem_limit_bytes=48 * 1024 * 1024),
        cost_estimate=pl.CostEstimate(
            flops=8 * points * sources * depth * length,
            bytes_accessed=16 * points * sources * length,
            transcendentals=0,
        ),
        name="final",
    )(sums, recorded, window, across(returned), across(arrived), across(changed), tall, mask, pick)


def forward_product(model, flat_kernel, inner):
    sources = model.shape[1]
    incoming = gather_all(model.reshape(2 * sources, -1), inner)
    product = lax.dot_general(
        incoming, flat_kernel, (((1,), (1,)), ((), ())), preferred_element_type=jnp.float32
    )
    half = flat_kernel.shape[0] // 2
    real_part = product[:sources, :half] - product[sources:, half:]
    imaginary = product[sources:, :half] + product[:sources, half:]
    return jnp.stack([real_part, imaginary], 0).astype(jnp.bfloat16)


RECORDED, RETURNED, IMAGED, SECOND, CHANGED, MIXED = range(6)
PARTS = 2
GROUP = 4


def loop(start, stop, body):
    def step(i, carry):
        body(i)
        return carry

    lax.fori_loop(start, stop, step, 0)


def iota(shape, axis):
    return lax.broadcasted_iota(jnp.int32, shape, axis)


def folded(values):
    rows, columns = values.shape
    parts = values.reshape(rows // 8, 8, columns).sum(0)
    out = parts[:, :128]
    for j in range(1, columns // 128):
        out = out + parts[:, j * 128 : (j + 1) * 128]
    return out


def iteration_kernel(
    outer, inner, mixing, bins_ref, rec_ref, ker_ref, start_ref, stop_ref,
    returned_ref, imaged_ref, changed_ref, sums_ref, win_ref, spread_ref, gather_ref,
    traces, gains, window, win, spread, gather, tapered, first_out, first_in, second_out,
    second_in, total, product, image_out, image_in, core_out, core_in, line_out, line_in, model,
    summed, summed_in, normal, normal_in, mixed_out, same, stats, stats_in, stats_all,
    trace_sem, gain_sem, keep_sem, out_sem, in_sem, core_out_sem, core_in_sem, line_out_sem,
    line_in_sem, share_out_sem, share_in_sem, stats_out_sem, stats_in_sem,
):
    n = outer
    sources, points, length = traces.shape
    halves, chunks, _, double, width = first_out.shape
    pieces, piece = model.shape[2], model.shape[5]
    count = sources // halves
    depth = n * double
    block = pieces * piece
    f32, bf16 = jnp.float32, jnp.bfloat16
    me, mine = lax.axis_index("gx"), lax.axis_index("ma")
    core = mine + 1 - 2 * lax.rem(mine, 2)
    line = lax.rem(mine + 2, 4)
    corner = lax.rem(core + 2, 4)
    both = range(halves)
    sent = summed if mixing else model.at[:, 0]

    def part(i):
        return pl.ds(pl.multiple_of(i * width, width), width)

    def trace_copy(h, i, s):
        s = h * count + s
        return pltpu.make_async_copy(
            rec_ref.at[part(i), s], traces.at[s, part(i)], trace_sem.at[h, i]
        )

    def trace_wait(h, i):
        place = traces.at[h * count : (h + 1) * count, part(i)]
        pltpu.make_async_copy(place, place, trace_sem.at[h, i]).wait()

    def gain_copy(i):
        return pltpu.make_async_copy(
            ker_ref.at[:, part(i)], gains.at[:, part(i)], gain_sem.at[i]
        )

    kept = (
        (summed_in, returned_ref),
        (image_in, imaged_ref),
        (normal_in, changed_ref),
        (win, win_ref),
        (spread, spread_ref),
        (gather, gather_ref),
    )

    def keep_copy(number):
        src, dst = kept[number]
        return pltpu.make_async_copy(src, dst, keep_sem.at[number])

    def across(number, src, dst, i, peer, slot):
        return pltpu.make_async_remote_copy(
            src_ref=src.at[i, peer],
            dst_ref=dst.at[i, slot],
            send_sem=out_sem.at[number],
            recv_sem=in_sem.at[number, i],
            device_id={"gx": peer},
            device_id_type=MESH,
        )

    def send_all(number, h, src, dst, i):
        src, dst, number = src.at[h], dst.at[h], number * halves + h

        def body(k):
            peer = lax.rem(me + k, n)
            across(number, src, dst, i, peer, me).start()

        loop(1, n, body)
        dst[i, me] = src[i, me]

    def receive_all(number, h, src, dst, i):
        number = number * halves + h
        others = pl.ds(0, n - 1)
        pltpu.make_async_remote_copy(
            src_ref=src.at[h, i, others],
            dst_ref=dst.at[h, i, others],
            send_sem=out_sem.at[number],
            recv_sem=in_sem.at[number, i],
            device_id={"gx": lax.rem(me + 1, n)},
            device_id_type=MESH,
        ).wait_recv()

    def finish_all(number, src, dst, many):
        others = pl.ds(0, n - 1)
        for h in both:
            pltpu.make_async_remote_copy(
                src_ref=src.at[h, :, others],
                dst_ref=dst.at[h, :, others],
                send_sem=out_sem.at[number * halves + h],
                recv_sem=in_sem.at[number * halves + h, 0],
                device_id={"gx": lax.rem(me + 1, n)},
                device_id_type=MESH,
            ).wait_send()

    def core_copy(h, stage, which, p):
        return pltpu.make_async_remote_copy(
            src_ref=core_out.at[h, stage, which, p],
            dst_ref=core_in.at[h, stage, which, p],
            send_sem=core_out_sem,
            recv_sem=core_in_sem.at[h, stage, which, p],
            device_id={"ma": core},
            device_id_type=MESH,
        )

    def line_copy(h, stage, p):
        return pltpu.make_async_remote_copy(
            src_ref=line_out.at[h, stage, p],
            dst_ref=line_in.at[h, stage, p],
            send_sem=line_out_sem,
            recv_sem=line_in_sem.at[h, stage, p],
            device_id={"ma": line},
            device_id_type=MESH,
        )

    def share_copy(h, which, p):
        source, slot, peer = ((0, 1, core), (0, 2, line), (2, 3, core))[which]
        return pltpu.make_async_remote_copy(
            src_ref=model.at[h, source, p],
            dst_ref=model.at[h, slot, p],
            send_sem=share_out_sem.at[which],
            recv_sem=share_in_sem.at[h, which, p],
            device_id={"ma": peer},
            device_id_type=MESH,
        )

    barrier = pltpu.get_barrier_semaphore()

    def greet(k):
        pl.semaphore_signal(
            barrier, inc=1, device_id={"gx": lax.rem(me + k, n)}, device_id_type=MESH
        )

    loop(1, n, greet)
    for peer in (core, line, corner):
        pl.semaphore_signal(barrier, inc=1, device_id={"ma": peer}, device_id_type=MESH)

    for h in both:
        loop(0, chunks, lambda i: loop(0, count, lambda s: trace_copy(h, i, s).start()))

    owners = iota((n, length), 0)
    bins = jnp.zeros_like(owners)
    for f in range(n):
        bins = jnp.where(owners == f, bins_ref[f], bins)
    angles = lax.rem(bins * iota((n, length), 1), length).astype(f32) * (2.0 * math.pi / length)
    scale = math.sqrt(2.0 / length)
    real, imaginary = jnp.cos(angles) * scale, -jnp.sin(angles) * scale
    rows = []
    for f in range(n):
        for values in (real, imaginary):
            rows.append(jnp.broadcast_to(values[f : f + 1], (count, length)))
    tall = jnp.concatenate(rows, 0)
    wide = tall.T
    row_place = lax.rem(iota((depth, length), 0), count)
    column_place = lax.rem(iota((length, depth), 1), count)
    for s in range(count):
        here = slice(s * length, (s + 1) * length)
        spread[:, here] = jnp.where(row_place == s, tall, 0.0).astype(bf16)
        gather[here] = jnp.where(column_place == s, wide, 0.0).astype(bf16)
    win[:sources] = (1 - start_ref[...]).astype(f32) * (1.0 / RAMP)
    win[sources:] = stop_ref[...].astype(f32) * (1.0 / RAMP)
    stats[...] = jnp.zeros_like(stats)
    if mixing:
        sides = []
        for axis in range(2):
            owner = iota((depth, depth), axis) // double
            values = jnp.zeros_like(owner)
            for f in range(n):
                values = jnp.where(owner == f, bins_ref[f], values)
            sides.append((values, lax.rem(iota((depth, depth), axis), double)))
        alike = (sides[0][0] == sides[1][0]) & (sides[0][1] == sides[1][1])
        same[...] = jnp.where(alike, 1.0, 0.0).astype(bf16)

    samples = iota((length, width), 0).astype(f32) * (1.0 / RAMP)

    def span(s, many=1):
        return pl.ds(pl.multiple_of(s * length, length), many * length)

    def transform(out, h, i):
        result = jnp.dot(spread[...], tapered[...], preferred_element_type=f32)
        out[h, i] = result.astype(bf16).reshape(n, double, width)

    def prepare(h, i):
        trace_wait(h, i)
        if h == 0:
            gain_copy(i).start()
        for k in range(count):
            s = h * count + k
            rising = jnp.clip(samples + win[s : s + 1, part(i)], 0.0, 1.0)
            falling = jnp.clip(win[sources + s : sources + s + 1, part(i)] - samples, 0.0, 1.0)
            weight = rising * falling
            window[i, span(s)] = weight.astype(bf16)
            tapered[k * length : (k + 1) * length] = (weight * traces[s, part(i)].T).astype(bf16)
        transform(first_out, h, i)

    def record(h, i):
        prepare(h, i)
        send_all(RECORDED, h, first_out, first_in, i)

    def turned(values, sign):
        half = double // 2
        wide_values = values.astype(f32)
        low, high = wide_values[:, :half], wide_values[:, half:]
        pair = [high, -low] if sign > 0 else [-high, low]
        return jnp.concatenate(pair, 1).reshape(depth, values.shape[2]).astype(bf16)

    def adjoint_part(held, h, i, columns):
        data = held[h, i]
        return jnp.dot(
            data.reshape(depth, width), gains[0, part(i), columns], preferred_element_type=f32
        ) + jnp.dot(turned(data, 1), gains[1, part(i), columns], preferred_element_type=f32)

    rounds = ((RECORDED, first_out, first_in), (SECOND, second_out, second_in))

    def accumulate(stage, h, i):
        number, src, held = rounds[stage]
        receive_all(number, h, src, held, i)
        if stage == 0 and h == 0:
            gain_copy(i).wait()

        def body(j):
            columns = pl.ds(pl.multiple_of(j * block, block), block)
            update = adjoint_part(held, h, i, columns)
            total[h, :, columns] = update if i == 0 else total[h, :, columns] + update

        loop(0, inner, body)

    last = chunks - 1

    def pack(values):
        return values.astype(bf16).reshape(n, double, piece)

    def whole(where):
        return pl.ds(pl.multiple_of(where * block, block), block)

    def close(stage, h, where):
        update = adjoint_part(rounds[stage][2], h, last, whole(where))
        return update if chunks == 1 else total[h, :, whole(where)] + update

    def column(where, p):
        return pl.ds(pl.multiple_of(where * block + p * piece, piece), piece)

    def from_core(stage, h, which, p):
        core_copy(h, stage, which, p).wait_recv()
        return core_in[h, stage, which, p].reshape(depth, piece).astype(f32)

    def reduce_core(stage, h):
        number, src, held = rounds[stage]
        receive_all(number, h, src, held, last)
        if stage == 0 and h == 0:
            gain_copy(last).wait()

        def to_core(which, where):
            values = close(stage, h, where)
            for p in range(pieces):
                core_out[h, stage, which, p] = pack(values[:, p * piece : (p + 1) * piece])
                core_copy(h, stage, which, p).start()

        to_core(0, corner)
        total[h, :, whole(line)] = close(stage, h, line)
        to_core(1, core)

    def reduce_line(stage, h):
        def to_line(p):
            values = total[h, :, column(line, p)] + from_core(stage, h, 0, p)
            line_out[h, stage, p] = pack(values)
            line_copy(h, stage, p).start()

        loop(0, pieces, to_line)
        total[h, :, whole(mine)] = close(stage, h, mine)

    def reduce_out(stage, h):
        reduce_core(stage, h)
        reduce_line(stage, h)

    def reduced(stage, h, p):
        values = total[h, :, column(mine, p)] + from_core(stage, h, 1, p)
        line_copy(h, stage, p).wait_recv()
        return pack(values + line_in[h, stage, p].reshape(depth, piece).astype(f32))

    def flat(values):
        return values.reshape(depth, values.shape[2]).astype(f32)

    def forward_part(h, slot, where, many, rows):
        dims = (((1,), (1,)), ((), ()))
        out = None
        for p in many:
            values = model[h, slot, p]
            for number, side in enumerate((values.reshape(depth, piece), turned(values, -1))):
                update = lax.dot_general(
                    gains[number, rows, column(where, p)], side, dims,
                    preferred_element_type=f32,
                )
                out = update if out is None else out + update
        return out

    def forward(h, slot, where, many, first=False):
        tile_rows = 2 * width if chunks % 2 == 0 else width

        def body(i):
            rows = pl.ds(pl.multiple_of(i * tile_rows, tile_rows), tile_rows)
            update = forward_part(h, slot, where, many, rows)
            product[h, rows] = update if first else product[h, rows] + update

        loop(0, points // tile_rows, body)

    def share(h, p):
        share_copy(h, 1, p).start()
        share_copy(h, 0, p).start()

    def keep(h, p):
        values = reduced(0, h, p)
        if mixing:
            summed[h, p] = values
            send_all(RETURNED, h, sent, summed_in, p)
        else:
            model[h, 0, p] = values
            share(h, p)
            if h == 0:
                send_all(RETURNED, h, sent, summed_in, p)
            held = flat(values)
            stats[0] += folded(held * held)

    def mix(h, p):
        receive_all(RETURNED, h, sent, summed_in, p)
        arrived = summed_in[h, p].reshape(depth, piece)
        values = jnp.dot(same[...], arrived, preferred_element_type=f32)
        mixed_out[h, p] = values.astype(bf16).reshape(n, double, piece)
        send_all(MIXED, h, mixed_out, model.at[:, 0], p)

    def unmix(h, p):
        receive_all(MIXED, h, mixed_out, model.at[:, 0], p)
        share(h, p)

    def own_forward(h):
        forward(h, 0, mine, range(pieces), first=True)
        for p in range(pieces):
            share_copy(h, 0, p).wait_recv()
        forward(h, 1, core, range(pieces))

    def relay(h, p):
        share_copy(h, 1, p).wait_recv()
        share_copy(h, 2, p).start()

    def from_line(h, p):
        relay(h, p)
        if p % 2:
            forward(h, 2, line, (p - 1, p))
        elif p == pieces - 1:
            forward(h, 2, line, (p,))

    def imaging(h):
        for p in range(pieces):
            share_copy(h, 2, p).wait_recv()

        def body(i):
            values = product[h, part(i)] + forward_part(h, 3, corner, range(pieces), part(i))
            image_out[h, i] = values.T.astype(bf16).reshape(n, double, width)
            send_all(IMAGED, h, image_out, image_in, i)

        loop(0, chunks, body)

    def again(h, i):
        receive_all(IMAGED, h, image_out, image_in, i)
        arrived = image_in[h, i].reshape(depth, width)
        for j in range(0, count, GROUP):
            weight = window[i, span(h * count + j, GROUP)].astype(f32)
            rows = slice(j * length, (j + GROUP) * length)
            values = jnp.dot(gather[rows], arrived, preferred_element_type=f32) * weight
            stats[1] += folded(values * values)
            tapered[rows] = (values * weight).astype(bf16)
        transform(second_out, h, i)
        send_all(SECOND, h, second_out, second_in, i)

    def change(h, p):
        values = reduced(1, h, p)
        normal[h, p] = values
        send_all(CHANGED, h, normal, normal_in, p)
        if not mixing:
            held = flat(values)
            stats[2] += folded(held * flat(model[h, 0, p]))
            stats[3] += folded(held * held)

    prepare(0, 0)
    pl.semaphore_wait(barrier, n + 2)
    send_all(RECORDED, 0, first_out, first_in, 0)
    for h in both:
        loop(0 if h else 1, chunks, lambda i: record(h, i))
    for number in (3, 4, 5):
        keep_copy(number).start()
    for i in range(last):
        accumulate(0, 0, i)
    reduce_out(0, 0)
    def each(body, h):
        loop(0, pieces, lambda p: body(h, p))

    for h in both:
        more = h + 1 < halves
        if more:
            for i in range(last):
                accumulate(0, h + 1, i)
            reduce_core(0, h + 1)
        if not mixing or h == 0:
            each(keep, h)
        if more:
            reduce_line(0, h + 1)
        if mixing:
            if h == 0:
                each(mix, h)
            if more:
                each(keep, h + 1)
            each(unmix, h)
            if more:
                each(mix, h + 1)
        own_forward(h)
        for p in range(max(chunks, pieces)):
            if h and p < chunks:
                again(h - 1, p)
            if p < pieces:
                from_line(h, p)
        imaging(h)
    other = halves - 1
    for i in range(last):
        accumulate(1, 0, i)
        if i and i <= chunks // 2:
            again(other, i - 1)
    reduce_out(1, 0)
    for i in range(chunks // 2 if last > chunks // 2 else max(last - 1, 0), chunks):
        again(other, i)
    for h in range(1, halves):
        if not mixing:
            loop(0, pieces, lambda p: send_all(RETURNED, h, sent, summed_in, p))
        for i in range(last):
            accumulate(1, h, i)
            if i < pieces:
                change(h - 1, i)
        reduce_out(1, h)
        for p in range(last, pieces):
            change(h - 1, p)
    each(change, other)
    keep_copy(1).start()
    if mixing:

        def norms(h, p):
            receive_all(CHANGED, h, normal, normal_in, p)
            before = summed_in[h, p].reshape(depth, piece)
            after = normal_in[h, p].reshape(depth, piece)
            mixed_before = jnp.dot(same[...], before, preferred_element_type=f32)
            mixed_after = jnp.dot(same[...], after, preferred_element_type=f32)
            stats[0] += folded(before.astype(f32) * mixed_before)
            stats[2] += folded(after.astype(f32) * mixed_before)
            stats[3] += folded(after.astype(f32) * mixed_after)

        keep_copy(0).start()
        for h in both:
            loop(0, pieces, lambda p: norms(h, p))
    else:
        for h in both:
            loop(0, pieces, lambda p: receive_all(RETURNED, h, sent, summed_in, p))
        keep_copy(0).start()

    def stats_copy(which, peer):
        return pltpu.make_async_remote_copy(
            src_ref=stats,
            dst_ref=stats_in.at[which],
            send_sem=stats_out_sem.at[which],
            recv_sem=stats_in_sem.at[which],
            device_id={"ma": peer},
            device_id_type=MESH,
        )

    near = [stats_copy(which, peer) for which, peer in enumerate((core, line, corner))]
    for copy in near:
        copy.start()
    for copy in near:
        copy.wait_recv()
    stats_in[3] = (stats[...] + stats_in[0]) + (stats_in[1] + stats_in[2])

    def stats_across(peer, slot):
        return pltpu.make_async_remote_copy(
            src_ref=stats_in.at[3],
            dst_ref=stats_all.at[slot],
            send_sem=stats_out_sem.at[3],
            recv_sem=stats_in_sem.at[3],
            device_id={"gx": peer},
            device_id_type=MESH,
        )

    loop(1, n, lambda k: stats_across(lax.rem(me + k, n), me).start())
    stats_all[me] = stats_in[3]
    others = stats_all.at[pl.ds(0, n - 1)]
    every = pltpu.make_async_remote_copy(
        src_ref=others,
        dst_ref=others,
        send_sem=stats_out_sem.at[3],
        recv_sem=stats_in_sem.at[3],
        device_id={"gx": lax.rem(me + 1, n)},
        device_id_type=MESH,
    )
    if not mixing:
        for h in both:
            loop(0, pieces, lambda p: receive_all(CHANGED, h, normal, normal_in, p))
    keep_copy(2).start()
    every.wait_recv()
    sums_ref[...] = jnp.sum(stats_all[...], axis=0)

    for copy in near:
        copy.wait_send()
    every.wait_send()
    finish_all(RECORDED, first_out, first_in, chunks)
    finish_all(RETURNED, sent, summed_in, pieces)
    finish_all(IMAGED, image_out, image_in, chunks)
    finish_all(SECOND, second_out, second_in, chunks)
    finish_all(CHANGED, normal, normal_in, pieces)
    if mixing:
        finish_all(MIXED, mixed_out, model.at[:, 0], pieces)

    def finish(src, dst, sem, peer):
        pltpu.make_async_remote_copy(
            src_ref=src,
            dst_ref=dst,
            send_sem=sem,
            recv_sem=stats_in_sem.at[0],
            device_id={"ma": peer},
            device_id_type=MESH,
        ).wait_send()

    finish(core_out, core_in, core_out_sem, core)
    finish(line_out, line_in, line_out_sem, line)
    for which, peer in ((0, core), (1, line), (2, core)):
        finish(model.at[:, 0], model.at[:, 1], share_out_sem.at[which], peer)
    for number in range(6):
        keep_copy(number).wait()


def iteration(outer, inner, mixing, freq_bins, recorded, kernel, window_start, window_stop):
    points, sources, length = recorded.shape
    columns = kernel.shape[2]
    halves = PARTS
    count = sources // halves
    double = 2 * count
    depth = outer * double
    block = columns // inner
    width, piece = min(256, points), min(256, block)
    chunks, pieces = points // width, block // piece
    f32, bf16 = jnp.float32, jnp.bfloat16
    by_chunk = (halves, chunks, outer, double, width)
    by_piece = (halves, pieces, outer, double, piece)
    stack = by_piece[1:]
    vmem = pl.BlockSpec(memory_space=pltpu.VMEM)
    hbm = pl.BlockSpec(memory_space=pl.ANY)
    dma = pltpu.SemaphoreType.DMA
    exchanges = 6 if mixing else 5
    extra = by_piece if mixing else (halves, 1, 1, 16, 128)
    return pl.pallas_call(
        functools.partial(iteration_kernel, outer, inner, mixing),
        out_shape=[
            jax.ShapeDtypeStruct(by_piece, bf16),
            jax.ShapeDtypeStruct(by_chunk, bf16),
            jax.ShapeDtypeStruct(by_piece, bf16),
            jax.ShapeDtypeStruct((4, 8, 128), f32),
            jax.ShapeDtypeStruct((2 * sources, points), f32),
            jax.ShapeDtypeStruct((depth, count * length), bf16),
            jax.ShapeDtypeStruct((count * length, depth), bf16),
        ],
        in_specs=[pl.BlockSpec(memory_space=pltpu.SMEM), hbm, hbm, vmem, vmem],
        out_specs=[hbm, hbm, hbm, vmem, hbm, hbm, hbm],
        scratch_shapes=[
            pltpu.VMEM((sources, points, length), f32),
            pltpu.VMEM((2, points, columns), bf16),
            pltpu.VMEM((chunks, sources * length, width), bf16),
            pltpu.VMEM((2 * sources, points), f32),
            pltpu.VMEM((depth, count * length), bf16),
            pltpu.VMEM((count * length, depth), bf16),
            pltpu.VMEM((count * length, width), bf16),
            pltpu.VMEM(by_chunk, bf16),
            pltpu.VMEM(by_chunk, bf16),
            pltpu.VMEM(by_chunk, bf16),
            pltpu.VMEM(by_chunk, bf16),
            pltpu.VMEM((halves, depth, columns), f32),
            pltpu.VMEM((halves, points, depth), f32),
            pltpu.VMEM(by_chunk, bf16),
            pltpu.VMEM(by_chunk, bf16),
            pltpu.VMEM((halves, 2, 2) + stack, bf16),
            pltpu.VMEM((halves, 2, 2) + stack, bf16),
            pltpu.VMEM((halves, 2) + stack, bf16),
            pltpu.VMEM((halves, 2) + stack, bf16),
            pltpu.VMEM((halves, 4) + stack, bf16),
            pltpu.VMEM(extra, bf16),
            pltpu.VMEM(by_piece, bf16),
            pltpu.VMEM(by_piece, bf16),
            pltpu.VMEM(by_piece, bf16),
            pltpu.VMEM(extra, bf16),
            pltpu.VMEM((depth, depth) if mixing else (16, 128), bf16),
            pltpu.VMEM((4, 8, 128), f32),
            pltpu.VMEM((4, 4, 8, 128), f32),
            pltpu.VMEM((outer, 4, 8, 128), f32),
            dma((halves, chunks)),
            dma((chunks,)),
            dma((6,)),
            dma((exchanges * halves,)),
            dma((exchanges * halves, max(chunks, pieces))),
            dma,
            dma((halves, 2, 2, pieces)),
            dma,
            dma((halves, 2, pieces)),
            dma((3,)),
            dma((halves, 3, pieces)),
            dma((4,)),
            dma((4,)),
        ],
        compiler_params=pltpu.CompilerParams(
            collective_id=6 if mixing else 5,
            has_side_effects=True,
            vmem_limit_bytes=67_000_000,
        ),
        name="iteration_mixed" if mixing else "iteration",
    )(freq_bins, recorded, kernel, window_start, window_stop)


def write_kernel(
    sums_ref, rec_ref, win_ref, spread_ref, gather_ref, ret_ref, ima_ref, cha_ref,
    sol_ref, res_ref, dir_ref, traces, solved, rest, ahead, in_sem, out_sem,
):
    sources, points, length = traces.shape
    halves, chunks, outer, double, width = ima_ref.shape
    depth = outer * double
    count = sources // halves
    f32, bf16 = jnp.float32, jnp.bfloat16

    def part(i):
        return pl.ds(pl.multiple_of(i * width, width), width)

    def load(i, s):
        return pltpu.make_async_copy(
            rec_ref.at[part(i), s], traces.at[s, part(i)], in_sem.at[i]
        )

    staged = ((solved, sol_ref), (ahead, dir_ref), (rest, res_ref))

    def store(number, i, s):
        src, dst = staged[number]
        return pltpu.make_async_copy(
            src.at[s, part(i)], dst.at[part(i), s], out_sem.at[number]
        )

    loop(0, chunks, lambda i: loop(0, sources, lambda s: load(i, s).start()))
    norm_start, norm_data = jnp.sum(sums_ref[0]), jnp.sum(sums_ref[1])
    cross, norm_change = jnp.sum(sums_ref[2]), jnp.sum(sums_ref[3])
    step_size = norm_start / (norm_data + epsilon)
    norm_final = norm_start - 2.0 * step_size * cross + step_size * step_size * norm_change
    ratio = norm_final / (norm_start + epsilon)
    samples = iota((length, width), 0).astype(f32) * (1.0 / RAMP)

    def chunk(i):
        place = traces.at[:, part(i)]
        pltpu.make_async_copy(place, place, in_sem.at[i]).wait()
        for h in range(halves):
            before = ret_ref[h, i].reshape(depth, width).astype(f32).T.astype(bf16)
            after = cha_ref[h, i].reshape(depth, width).astype(f32).T.astype(bf16)
            arrived = ima_ref[h, i].reshape(depth, width)

            def pair(j):
                spans = pl.ds(pl.multiple_of(j * 2 * length, length), 2 * length)
                table = spread_ref[:, spans]
                first = h * count + 2 * j
                for r in range(0, width, 128):
                    rows = pl.ds(pl.multiple_of(i * width + r, 128), 128)
                    gradient = jnp.dot(before[r : r + 128], table, preferred_element_type=f32)
                    change = jnp.dot(after[r : r + 128], table, preferred_element_type=f32)
                    for k in range(2):
                        here = slice(k * length, (k + 1) * length)
                        g, c = gradient[:, here], change[:, here]
                        solved[first + k, rows] = step_size * g
                        ahead[first + k, rows] = (g - step_size * c) + ratio * g
                for k in range(2):
                    s = first + k
                    store(0, i, s).start()
                    store(1, i, s).start()
                    rising = jnp.clip(samples + win_ref[pl.ds(s, 1), part(i)], 0.0, 1.0)
                    falling = jnp.clip(
                        win_ref[pl.ds(sources + s, 1), part(i)] - samples, 0.0, 1.0
                    )
                    spans = pl.ds(pl.multiple_of((2 * j + k) * length, length), length)
                    image = jnp.dot(gather_ref[spans], arrived, preferred_element_type=f32)
                    image = (rising * falling) * image
                    rest[s, part(i)] = traces[s, part(i)] - step_size * image.T
                    store(2, i, s).start()

            def some(j):
                for k in range(2):
                    pair(2 * j + k)

            loop(0, count // 4, some)

    loop(0, chunks, chunk)
    for number in range(3):
        src = staged[number][0]
        pltpu.make_async_copy(src, src, out_sem.at[number]).wait()


def write(recorded, returned, imaged, changed, sums, windows, spread, gather):
    points, sources, length = recorded.shape
    halves, chunks, outer, double, width = imaged.shape
    depth = outer * double
    vmem = pl.BlockSpec(memory_space=pltpu.VMEM)
    hbm = pl.BlockSpec(memory_space=pl.ANY)
    f32 = jnp.float32
    staged = pltpu.VMEM((sources, points, length), f32)
    return pl.pallas_call(
        write_kernel,
        out_shape=[jax.ShapeDtypeStruct(recorded.shape, f32)] * 3,
        in_specs=[vmem, hbm] + [vmem] * 6,
        out_specs=[hbm] * 3,
        scratch_shapes=[
            staged,
            staged,
            staged,
            staged,
            pltpu.SemaphoreType.DMA((chunks,)),
            pltpu.SemaphoreType.DMA((3,)),
        ],
        compiler_params=pltpu.CompilerParams(vmem_limit_bytes=56 * 1024 * 1024),
        cost_estimate=pl.CostEstimate(
            flops=6 * points * sources * depth * length,
            bytes_accessed=16 * points * sources * length,
            transcendentals=0,
        ),
        name="write",
    )(sums, recorded, windows, spread, gather, returned, imaged, changed)


def fused(outer, inner, recorded, kernel, freq_bins, window_start, window_stop):
    same = freq_bins[:, None] == freq_bins[None, :]
    repeated = jnp.sum(same.astype(jnp.int32)) > freq_bins.shape[0]
    gains = kernel.reshape(2, kernel.shape[2], kernel.shape[3])
    results = lax.cond(
        repeated,
        lambda *x: tuple(iteration(outer, inner, True, *x)),
        lambda *x: tuple(iteration(outer, inner, False, *x)),
        freq_bins, recorded, gains, window_start.T, window_stop.T,
    )
    return tuple(write(recorded, *results))


def fits(outer, inner, recorded, kernel):
    points, sources, length = recorded.shape
    columns = kernel.shape[3]
    return (
        inner == 4
        and kernel.shape[1] == 1
        and columns == inner * points
        and sources % (PARTS * 8) == 0
        and length % 128 == 0
        and points % 256 == 0
        and outer * 2 * (sources // PARTS) % 128 == 0
        and points * (4 * columns + 6 * sources * length) < 30_000_000
    )


def per_device(outer, inner, recorded, kernel, freq_bins, window_start, window_stop):
    if fits(outer, inner, recorded, kernel):
        return fused(outer, inner, recorded, kernel, freq_bins, window_start, window_stop)
    length = recorded.shape[2]
    table = phase_table(freq_bins, length)
    weights = taper_weights(window_start, window_stop, length)
    flat_kernel = kernel.reshape(2 * kernel.shape[2], kernel.shape[3])

    data = by_frequency(exchange(to_spectra(weights * recorded, table), outer, 0), outer)
    adjoint = adjoint_product(data, flat_kernel, inner)
    returned = lax.all_to_all(
        by_source(adjoint, outer), "gx", split_axis=0, concat_axis=0, tiled=True
    )

    same = freq_bins[:, None] == freq_bins[None, :]
    repeated = jnp.sum(same.astype(jnp.int32)) > freq_bins.shape[0]

    def combined(spectra):
        parts = lax.all_to_all(
            by_source(spectra, outer), "gx", split_axis=0, concat_axis=0, tiled=True
        )
        mixed = jnp.einsum(
            "gf,fxa->gxa",
            same.astype(jnp.bfloat16),
            parts,
            preferred_element_type=jnp.float32,
        ).astype(jnp.bfloat16)
        back = lax.all_to_all(mixed, "gx", split_axis=0, concat_axis=0, tiled=True)
        return by_frequency(back, outer)

    model = lax.cond(repeated, combined, lambda spectra: spectra, adjoint)
    outgoing = by_source(forward_product(model, flat_kernel, inner), outer)
    imaged = exchange(outgoing, outer, 1)
    image = weights * to_traces(imaged, table)
    second = by_frequency(exchange(to_spectra(weights * image, table), outer, 2), outer)
    normal = adjoint_product(second, flat_kernel, inner)
    changed = exchange(by_source(normal, outer), outer, 3)

    double, points = returned.shape[1:]
    depth = freq_bins.shape[0] * double
    eye = jnp.eye(double, dtype=jnp.bfloat16)
    mixing = (same.astype(jnp.bfloat16)[:, None, :, None] * eye[None, :, None, :]).reshape(
        depth, depth
    )
    flat_g = returned.reshape(depth, points)
    flat_h = changed.reshape(depth, points)
    mixed_g = jnp.dot(mixing, flat_g, preferred_element_type=jnp.float32)
    mixed_h = jnp.dot(mixing, flat_h, preferred_element_type=jnp.float32)
    sums = jnp.stack(
        [
            jnp.sum(flat_g.astype(jnp.float32) * mixed_g),
            jnp.sum(image * image),
            jnp.sum(mixed_g * flat_h.astype(jnp.float32)),
            jnp.sum(flat_h.astype(jnp.float32) * mixed_h),
        ]
    )
    sums = total(jnp.broadcast_to(jnp.tile(sums, 2)[:, None], (8, 128)), outer, inner, 4)
    if recorded.shape[1] % 8 == 0:
        return tuple(
            final_step(
                sums, recorded, window_start, window_stop, returned, imaged, changed, table
            )
        )
    gradient = to_traces(returned, table)
    change = to_traces(changed, table)
    norm_start, norm_data, cross, norm_change = sums[0, 0], sums[1, 0], sums[2, 0], sums[3, 0]
    step_size = norm_start / (norm_data + epsilon)
    norm_final = norm_start - 2.0 * step_size * cross + step_size * step_size * norm_change
    solution = step_size * gradient
    residual = recorded - step_size * image
    direction = gradient - step_size * change + norm_final / (norm_start + epsilon) * gradient
    return (solution, residual, direction)


def solution(mesh):
    in_specs = (P("ma", "gx", None), P(None, "gx", "ma", None), P(), P("ma", "gx"), P("ma", "gx"))
    out_specs = (P("ma", "gx", None), P("ma", "gx", None), P("ma", "gx", None))
    return jax.shard_map(
        functools.partial(per_device, mesh.shape["gx"], mesh.shape["ma"]),
        mesh=mesh,
        in_specs=in_specs,
        out_specs=out_specs,
        check_vma=False,
    )
```

```python
import functools
import math

import jax
import jax.numpy as jnp
from jax import lax
from jax.experimental import pallas as pl
from jax.experimental.pallas import tpu as pltpu
from jax.sharding import PartitionSpec as P

RAMP = 8
MESH = pl.DeviceIdType.MESH

epsilon = 1e-06


def phase_table(freq_bins, length):
    samples = jnp.arange(length, dtype=jnp.int32)
    angles = (freq_bins[:, None] * samples[None, :] % length).astype(jnp.float32) * (
        2.0 * math.pi / length
    )
    return jnp.stack([jnp.cos(angles), -jnp.sin(angles)], 1) * math.sqrt(2.0 / length)


def taper_weights(window_start, window_stop, length):
    samples = jnp.arange(length, dtype=jnp.float32)
    rising = jnp.clip(
        (samples[None, None, :] - window_start[:, :, None].astype(jnp.float32) + 1.0) / RAMP,
        0.0,
        1.0,
    )
    falling = jnp.clip(
        (window_stop[:, :, None].astype(jnp.float32) - samples[None, None, :]) / RAMP, 0.0, 1.0
    )
    return rising * falling


def exchange_kernel(n, x_ref, o_ref, send_sem, recv_sem, own_sem):
    me = lax.axis_index("gx")
    barrier = pltpu.get_barrier_semaphore()
    for k in range(1, n):
        pl.semaphore_signal(
            barrier, inc=1, device_id={"gx": lax.rem(me + k, n)}, device_id_type=MESH
        )
    own = pltpu.make_async_copy(x_ref.at[me], o_ref.at[me], own_sem)
    own.start()
    pl.semaphore_wait(barrier, n - 1)
    copies = []
    for k in range(1, n):
        peer = lax.rem(me + k, n)
        copy = pltpu.make_async_remote_copy(
            src_ref=x_ref.at[peer],
            dst_ref=o_ref.at[me],
            send_sem=send_sem.at[k],
            recv_sem=recv_sem.at[k],
            device_id={"gx": peer},
            device_id_type=MESH,
        )
        copy.start()
        copies.append(copy)
    own.wait()
    for copy in copies:
        copy.wait()


def exchange(x, n, number):
    return pl.pallas_call(
        functools.partial(exchange_kernel, n),
        out_shape=jax.ShapeDtypeStruct(x.shape, x.dtype),
        in_specs=[pl.BlockSpec(memory_space=pltpu.VMEM)],
        out_specs=pl.BlockSpec(memory_space=pltpu.VMEM),
        scratch_shapes=[
            pltpu.SemaphoreType.DMA((n,)),
            pltpu.SemaphoreType.DMA((n,)),
            pltpu.SemaphoreType.DMA,
        ],
        compiler_params=pltpu.CompilerParams(collective_id=number, has_side_effects=True),
        name=f"exchange{number}",
    )(x)


def total_kernel(outer, inner, x_ref, o_ref, held, send_sem, recv_sem):
    n = outer * inner
    me = lax.axis_index("gx") * inner + lax.axis_index("ma")
    barrier = pltpu.get_barrier_semaphore()

    def place(k):
        peer = lax.rem(me + k, n)
        return (peer // inner, lax.rem(peer, inner))

    for k in range(1, n):
        pl.semaphore_signal(barrier, inc=1, device_id=place(k), device_id_type=MESH)
    pl.semaphore_wait(barrier, n - 1)
    copies = []
    for k in range(1, n):
        copy = pltpu.make_async_remote_copy(
            src_ref=x_ref,
            dst_ref=held.at[me],
            send_sem=send_sem.at[k],
            recv_sem=recv_sem.at[k],
            device_id=place(k),
            device_id_type=MESH,
        )
        copy.start()
        copies.append(copy)
    held[me] = x_ref[...]
    for copy in copies:
        copy.wait()
    o_ref[...] = jnp.sum(held[...], axis=0)


def total(x, outer, inner, number):
    n = outer * inner
    return pl.pallas_call(
        functools.partial(total_kernel, outer, inner),
        out_shape=jax.ShapeDtypeStruct(x.shape, x.dtype),
        in_specs=[pl.BlockSpec(memory_space=pltpu.VMEM)],
        out_specs=pl.BlockSpec(memory_space=pltpu.VMEM),
        scratch_shapes=[
            pltpu.VMEM((n,) + x.shape, x.dtype),
            pltpu.SemaphoreType.DMA((n,)),
            pltpu.SemaphoreType.DMA((n,)),
        ],
        compiler_params=pltpu.CompilerParams(collective_id=number, has_side_effects=True),
        name=f"total{number}",
    )(x)


def pairs(n, bit):
    return [(i, i ^ bit) for i in range(n)]


def scatter_sum(partial, n):
    rows, block = partial.shape[1:]
    me = lax.axis_index("ma")
    held = partial
    bit = 1
    while bit < n:
        own = (me // bit) % 2
        parts = held.reshape(-1, 2, rows, block)
        keep = lax.dynamic_index_in_dim(parts, own, 1, keepdims=False)
        send = lax.dynamic_index_in_dim(parts, 1 - own, 1, keepdims=False)
        got = lax.ppermute(send, "ma", pairs(n, bit))
        held = (keep.astype(jnp.float32) + got.astype(jnp.float32)).astype(jnp.bfloat16)
        bit *= 2
    return held.reshape(rows, block)


def gather_all(x, n):
    rows, block = x.shape
    me = lax.axis_index("ma")
    held = x.reshape(rows, 1, block)
    bit = n // 2
    while bit >= 1:
        own = (me // bit) % 2
        got = lax.ppermute(held, "ma", pairs(n, bit))
        first = jnp.where(own == 0, held, got)
        second = jnp.where(own == 0, got, held)
        held = jnp.stack([first, second], 2).reshape(rows, -1, block)
        bit //= 2
    return held.reshape(rows, n * block)


def to_spectra(traces, table):
    freqs = table.shape[0]
    flat = table.reshape(2 * freqs, table.shape[2]).astype(jnp.bfloat16)
    out = jnp.einsum(
        "ast,kt->ksa", traces.astype(jnp.bfloat16), flat, preferred_element_type=jnp.float32
    ).astype(jnp.bfloat16)
    return out.reshape(freqs, 2 * out.shape[1], out.shape[2])


def to_traces(spectra, table):
    freqs, double, points = spectra.shape
    sources = double // 2
    length = table.shape[2]
    depth = freqs * double
    across = spectra.reshape(depth, points).T
    owner = jnp.arange(depth, dtype=jnp.int32) % sources
    mask = (owner[None, :] == jnp.arange(sources, dtype=jnp.int32)[:, None]).astype(jnp.bfloat16)
    spread = (across[:, None, :] * mask[None]).reshape(points * sources, depth)
    tall = jnp.repeat(table.reshape(2 * freqs, length).astype(jnp.bfloat16), sources, axis=0)
    out = jnp.dot(spread, tall, preferred_element_type=jnp.float32)
    return out.reshape(points, sources, length)


def by_frequency(arrived, n):
    sources = arrived.shape[1] // 2
    points = arrived.shape[2]
    return arrived.reshape(n, 2, sources, points).transpose(1, 0, 2, 3).reshape(2, -1, points)


def by_source(spectra, n):
    points = spectra.shape[2]
    sources = spectra.shape[1] // n
    return spectra.reshape(2, n, sources, points).transpose(1, 0, 2, 3).reshape(n, -1, points)


def adjoint_kernel(d_ref, k_ref, o_ref):
    half = d_ref.shape[0] // 2
    data = d_ref[...]
    first = jnp.dot(data, k_ref[0], preferred_element_type=jnp.float32)
    second = jnp.dot(data, k_ref[1], preferred_element_type=jnp.float32)
    o_ref[0, :half] = (first[:half] + second[half:]).astype(o_ref.dtype)
    o_ref[0, half:] = (first[half:] - second[:half]).astype(o_ref.dtype)


def adjoint_product(data, flat_kernel, inner):
    sources, rows = data.shape[1], data.shape[2]
    columns = flat_kernel.shape[1]
    block = columns // inner
    tile = min(512, block)
    per_block = block // tile
    partial = pl.pallas_call(
        adjoint_kernel,
        grid=(columns // tile,),
        out_shape=jax.ShapeDtypeStruct((inner, 2 * sources, block), jnp.bfloat16),
        in_specs=[
            pl.BlockSpec((2 * sources, rows), lambda j: (0, 0)),
            pl.BlockSpec((2, rows, tile), lambda j: (0, 0, j)),
        ],
        out_specs=pl.BlockSpec(
            (1, 2 * sources, tile), lambda j: (j // per_block, 0, j % per_block)
        ),
        compiler_params=pltpu.CompilerParams(vmem_limit_bytes=60 * 1024 * 1024),
        cost_estimate=pl.CostEstimate(
            flops=8 * sources * rows * columns,
            bytes_accessed=4 * rows * columns + 4 * sources * (rows + columns),
            transcendentals=0,
        ),
        name="adjoint",
    )(data.reshape(2 * sources, rows), flat_kernel.reshape(2, rows, columns))
    return scatter_sum(partial, inner).reshape(2, sources, block)


def final_kernel(
    sums_ref, rec_ref, win_ref, g_ref, d_ref, h_ref, tall_ref, mask_ref, pick_ref,
    sol_ref, res_ref, dir_ref,
):
    tile, sources, length = rec_ref.shape
    norm_start, norm_data = sums_ref[0, 0], sums_ref[1, 0]
    cross, norm_change = sums_ref[2, 0], sums_ref[3, 0]
    step_size = norm_start / (norm_data + epsilon)
    norm_final = norm_start - 2.0 * step_size * cross + step_size * step_size * norm_change
    ratio = norm_final / (norm_start + epsilon)
    tall = tall_ref[...]

    def rows(values, mask):
        return (values[:, None, :] * mask[None]).reshape(tile * sources, -1).astype(jnp.bfloat16)

    def traces(ref):
        spread = rows(ref[...].astype(jnp.float32), mask_ref[...])
        out = jnp.dot(spread, tall, preferred_element_type=jnp.float32)
        return out.reshape(tile, sources, length)

    gradient = traces(g_ref)
    change = traces(h_ref)
    sol_ref[...] = step_size * gradient
    dir_ref[...] = (gradient - step_size * change) + ratio * gradient
    window = win_ref[...]
    ones = jnp.ones((window.shape[1], length), jnp.bfloat16)
    shape = (tile, sources, length)
    start = jnp.dot(rows(window, pick_ref[0]), ones, preferred_element_type=jnp.float32)
    stop = jnp.dot(rows(window, pick_ref[1]), ones, preferred_element_type=jnp.float32)
    samples = lax.broadcasted_iota(jnp.int32, shape, 2).astype(jnp.float32)
    rising = jnp.clip((samples - start.reshape(shape) + 1.0) / RAMP, 0.0, 1.0)
    falling = jnp.clip((stop.reshape(shape) - samples) / RAMP, 0.0, 1.0)
    image = (rising * falling) * traces(d_ref)
    res_ref[...] = rec_ref[...] - step_size * image


def final_step(sums, recorded, window_start, window_stop, returned, arrived, changed, table):
    points, sources, length = recorded.shape
    depth = returned.shape[0] * returned.shape[1]
    tile = min(128, points)

    def across(x):
        return x.reshape(depth, points).T

    place = jnp.arange(sources, dtype=jnp.int32)
    owner = jnp.arange(depth, dtype=jnp.int32) % sources
    mask = (owner[None, :] == place[:, None]).astype(jnp.float32)
    column = jnp.arange(2 * sources, dtype=jnp.int32)
    pick = jnp.stack(
        [column[None, :] == place[:, None], column[None, :] == place[:, None] + sources]
    ).astype(jnp.float32)
    tall = jnp.repeat(table.reshape(-1, length).astype(jnp.bfloat16), sources, axis=0)
    window = jnp.concatenate([window_start, window_stop], 1).astype(jnp.float32)
    whole3 = pl.BlockSpec((tile, sources, length), lambda i: (i, 0, 0))
    strip = pl.BlockSpec((tile, depth), lambda i: (i, 0))
    return pl.pallas_call(
        final_kernel,
        grid=(points // tile,),
        out_shape=[jax.ShapeDtypeStruct(recorded.shape, jnp.float32)] * 3,
        in_specs=[
            pl.BlockSpec(memory_space=pltpu.SMEM),
            whole3,
            pl.BlockSpec((tile, 2 * sources), lambda i: (i, 0)),
            strip,
            strip,
            strip,
            pl.BlockSpec((depth, length), lambda i: (0, 0)),
            pl.BlockSpec((sources, depth), lambda i: (0, 0)),
            pl.BlockSpec((2, sources, 2 * sources), lambda i: (0, 0, 0)),
        ],
        out_specs=[whole3] * 3,
        compiler_params=pltpu.CompilerParams(vmem_limit_bytes=48 * 1024 * 1024),
        cost_estimate=pl.CostEstimate(
            flops=8 * points * sources * depth * length,
            bytes_accessed=16 * points * sources * length,
            transcendentals=0,
        ),
        name="final",
    )(sums, recorded, window, across(returned), across(arrived), across(changed), tall, mask, pick)


def forward_product(model, flat_kernel, inner):
    sources = model.shape[1]
    incoming = gather_all(model.reshape(2 * sources, -1), inner)
    product = lax.dot_general(
        incoming, flat_kernel, (((1,), (1,)), ((), ())), preferred_element_type=jnp.float32
    )
    half = flat_kernel.shape[0] // 2
    real_part = product[:sources, :half] - product[sources:, half:]
    imaginary = product[sources:, :half] + product[:sources, half:]
    return jnp.stack([real_part, imaginary], 0).astype(jnp.bfloat16)


RECORDED, RETURNED, IMAGED, SECOND, CHANGED, MIXED = range(6)
PARTS = 2
GROUP = 4


def loop(start, stop, body):
    def step(i, carry):
        body(i)
        return carry

    lax.fori_loop(start, stop, step, 0)


def iota(shape, axis):
    return lax.broadcasted_iota(jnp.int32, shape, axis)


def folded(values):
    rows, columns = values.shape
    parts = values.reshape(rows // 8, 8, columns).sum(0)
    out = parts[:, :128]
    for j in range(1, columns // 128):
        out = out + parts[:, j * 128 : (j + 1) * 128]
    return out


def iteration_kernel(
    outer, inner, mixing, bins_ref, rec_ref, ker_ref, start_ref, stop_ref,
    returned_ref, imaged_ref, changed_ref, sums_ref, win_ref, spread_ref, gather_ref,
    traces, gains, window, win, spread, gather, tapered, first_out, first_in, second_out,
    second_in, total, product, image_out, image_in, core_out, core_in, line_out, line_in, model,
    summed, summed_in, normal, normal_in, mixed_out, same, stats, stats_in, stats_all,
    trace_sem, gain_sem, keep_sem, out_sem, in_sem, core_out_sem, core_in_sem, line_out_sem,
    line_in_sem, share_out_sem, share_in_sem, stats_out_sem, stats_in_sem,
):
    n = outer
    sources, points, length = traces.shape
    halves, chunks, _, double, width = first_out.shape
    pieces, piece = model.shape[2], model.shape[5]
    count = sources // halves
    depth = n * double
    block = pieces * piece
    f32, bf16 = jnp.float32, jnp.bfloat16
    me, mine = lax.axis_index("gx"), lax.axis_index("ma")
    core = mine + 1 - 2 * lax.rem(mine, 2)
    line = lax.rem(mine + 2, 4)
    corner = lax.rem(core + 2, 4)
    both = range(halves)
    sent = summed if mixing else model.at[:, 0]

    def part(i):
        return pl.ds(pl.multiple_of(i * width, width), width)

    def trace_copy(h, i, s):
        s = h * count + s
        return pltpu.make_async_copy(
            rec_ref.at[part(i), s], traces.at[s, part(i)], trace_sem.at[h, i]
        )

    def trace_wait(h, i):
        place = traces.at[h * count : (h + 1) * count, part(i)]
        pltpu.make_async_copy(place, place, trace_sem.at[h, i]).wait()

    def gain_copy(i):
        return pltpu.make_async_copy(
            ker_ref.at[:, part(i)], gains.at[:, part(i)], gain_sem.at[i]
        )

    kept = (
        (summed_in, returned_ref),
        (image_in, imaged_ref),
        (normal_in, changed_ref),
        (win, win_ref),
        (spread, spread_ref),
        (gather, gather_ref),
    )

    def keep_copy(number):
        src, dst = kept[number]
        return pltpu.make_async_copy(src, dst, keep_sem.at[number])

    def across(number, src, dst, i, peer, slot):
        return pltpu.make_async_remote_copy(
            src_ref=src.at[i, peer],
            dst_ref=dst.at[i, slot],
            send_sem=out_sem.at[number],
            recv_sem=in_sem.at[number, i],
            device_id={"gx": peer},
            device_id_type=MESH,
        )

    def send_all(number, h, src, dst, i):
        src, dst, number = src.at[h], dst.at[h], number * halves + h

        def body(k):
            peer = lax.rem(me + k, n)
            across(number, src, dst, i, peer, me).start()

        loop(1, n, body)
        dst[i, me] = src[i, me]

    def receive_all(number, h, src, dst, i):
        number = number * halves + h
        others = pl.ds(0, n - 1)
        pltpu.make_async_remote_copy(
            src_ref=src.at[h, i, others],
            dst_ref=dst.at[h, i, others],
            send_sem=out_sem.at[number],
            recv_sem=in_sem.at[number, i],
            device_id={"gx": lax.rem(me + 1, n)},
            device_id_type=MESH,
        ).wait_recv()

    def finish_all(number, src, dst, many):
        others = pl.ds(0, n - 1)
        for h in both:
            pltpu.make_async_remote_copy(
                src_ref=src.at[h, :, others],
                dst_ref=dst.at[h, :, others],
                send_sem=out_sem.at[number * halves + h],
                recv_sem=in_sem.at[number * halves + h, 0],
                device_id={"gx": lax.rem(me + 1, n)},
                device_id_type=MESH,
            ).wait_send()

    def core_copy(h, stage, which, p):
        return pltpu.make_async_remote_copy(
            src_ref=core_out.at[h, stage, which, p],
            dst_ref=core_in.at[h, stage, which, p],
            send_sem=core_out_sem,
            recv_sem=core_in_sem.at[h, stage, which, p],
            device_id={"ma": core},
            device_id_type=MESH,
        )

    def line_copy(h, stage, p):
        return pltpu.make_async_remote_copy(
            src_ref=line_out.at[h, stage, p],
            dst_ref=line_in.at[h, stage, p],
            send_sem=line_out_sem,
            recv_sem=line_in_sem.at[h, stage, p],
            device_id={"ma": line},
            device_id_type=MESH,
        )

    def share_copy(h, which, p):
        source, slot, peer = ((0, 1, core), (0, 2, line), (2, 3, core))[which]
        return pltpu.make_async_remote_copy(
            src_ref=model.at[h, source, p],
            dst_ref=model.at[h, slot, p],
            send_sem=share_out_sem.at[which],
            recv_sem=share_in_sem.at[h, which, p],
            device_id={"ma": peer},
            device_id_type=MESH,
        )

    barrier = pltpu.get_barrier_semaphore()

    def greet(k):
        pl.semaphore_signal(
            barrier, inc=1, device_id={"gx": lax.rem(me + k, n)}, device_id_type=MESH
        )

    loop(1, n, greet)
    for peer in (core, line, corner):
        pl.semaphore_signal(barrier, inc=1, device_id={"ma": peer}, device_id_type=MESH)

    for h in both:
        loop(0, chunks, lambda i: loop(0, count, lambda s: trace_copy(h, i, s).start()))

    owners = iota((n, length), 0)
    bins = jnp.zeros_like(owners)
    for f in range(n):
        bins = jnp.where(owners == f, bins_ref[f], bins)
    angles = lax.rem(bins * iota((n, length), 1), length).astype(f32) * (2.0 * math.pi / length)
    scale = math.sqrt(2.0 / length)
    real, imaginary = jnp.cos(angles) * scale, -jnp.sin(angles) * scale
    rows = []
    for f in range(n):
        for values in (real, imaginary):
            rows.append(jnp.broadcast_to(values[f : f + 1], (count, length)))
    tall = jnp.concatenate(rows, 0)
    wide = tall.T
    row_place = lax.rem(iota((depth, length), 0), count)
    column_place = lax.rem(iota((length, depth), 1), count)
    for s in range(count):
        here = slice(s * length, (s + 1) * length)
        spread[:, here] = jnp.where(row_place == s, tall, 0.0).astype(bf16)
        gather[here] = jnp.where(column_place == s, wide, 0.0).astype(bf16)
    win[:sources] = (1 - start_ref[...]).astype(f32) * (1.0 / RAMP)
    win[sources:] = stop_ref[...].astype(f32) * (1.0 / RAMP)
    stats[...] = jnp.zeros_like(stats)
    if mixing:
        sides = []
        for axis in range(2):
            owner = iota((depth, depth), axis) // double
            values = jnp.zeros_like(owner)
            for f in range(n):
                values = jnp.where(owner == f, bins_ref[f], values)
            sides.append((values, lax.rem(iota((depth, depth), axis), double)))
        alike = (sides[0][0] == sides[1][0]) & (sides[0][1] == sides[1][1])
        same[...] = jnp.where(alike, 1.0, 0.0).astype(bf16)

    samples = iota((length, width), 0).astype(f32) * (1.0 / RAMP)

    def span(s, many=1):
        return pl.ds(pl.multiple_of(s * length, length), many * length)

    def transform(out, h, i):
        result = jnp.dot(spread[...], tapered[...], preferred_element_type=f32)
        out[h, i] = result.astype(bf16).reshape(n, double, width)

    def prepare(h, i):
        trace_wait(h, i)
        if h == 0:
            gain_copy(i).start()
        for k in range(count):
            s = h * count + k
            rising = jnp.clip(samples + win[s : s + 1, part(i)], 0.0, 1.0)
            falling = jnp.clip(win[sources + s : sources + s + 1, part(i)] - samples, 0.0, 1.0)
            weight = rising * falling
            window[i, span(s)] = weight.astype(bf16)
            tapered[k * length : (k + 1) * length] = (weight * traces[s, part(i)].T).astype(bf16)
        transform(first_out, h, i)

    def record(h, i):
        prepare(h, i)
        send_all(RECORDED, h, first_out, first_in, i)

    def turned(values, sign):
        half = double // 2
        wide_values = values.astype(f32)
        low, high = wide_values[:, :half], wide_values[:, half:]
        pair = [high, -low] if sign > 0 else [-high, low]
        return jnp.concatenate(pair, 1).reshape(depth, values.shape[2]).astype(bf16)

    def adjoint_part(held, h, i, columns):
        data = held[h, i]
        return jnp.dot(
            data.reshape(depth, width), gains[0, part(i), columns], preferred_element_type=f32
        ) + jnp.dot(turned(data, 1), gains[1, part(i), columns], preferred_element_type=f32)

    rounds = ((RECORDED, first_out, first_in), (SECOND, second_out, second_in))

    def accumulate(stage, h, i):
        number, src, held = rounds[stage]
        receive_all(number, h, src, held, i)
        if stage == 0 and h == 0:
            gain_copy(i).wait()

        def body(j):
            columns = pl.ds(pl.multiple_of(j * block, block), block)
            update = adjoint_part(held, h, i, columns)
            total[h, :, columns] = update if i == 0 else total[h, :, columns] + update

        loop(0, inner, body)

    last = chunks - 1

    def pack(values):
        return values.astype(bf16).reshape(n, double, piece)

    def whole(where):
        return pl.ds(pl.multiple_of(where * block, block), block)

    def close(stage, h, where):
        update = adjoint_part(rounds[stage][2], h, last, whole(where))
        return update if chunks == 1 else total[h, :, whole(where)] + update

    def column(where, p):
        return pl.ds(pl.multiple_of(where * block + p * piece, piece), piece)

    def from_core(stage, h, which, p):
        core_copy(h, stage, which, p).wait_recv()
        return core_in[h, stage, which, p].reshape(depth, piece).astype(f32)

    def reduce_core(stage, h):
        number, src, held = rounds[stage]
        receive_all(number, h, src, held, last)
        if stage == 0 and h == 0:
            gain_copy(last).wait()

        def to_core(which, where):
            values = close(stage, h, where)
            for p in range(pieces):
                core_out[h, stage, which, p] = pack(values[:, p * piece : (p + 1) * piece])
                core_copy(h, stage, which, p).start()

        to_core(0, corner)
        total[h, :, whole(line)] = close(stage, h, line)
        to_core(1, core)

    def reduce_line(stage, h):
        def to_line(p):
            values = total[h, :, column(line, p)] + from_core(stage, h, 0, p)
            line_out[h, stage, p] = pack(values)
            line_copy(h, stage, p).start()

        loop(0, pieces, to_line)
        total[h, :, whole(mine)] = close(stage, h, mine)

    def reduce_out(stage, h):
        reduce_core(stage, h)
        reduce_line(stage, h)

    def reduced(stage, h, p):
        values = total[h, :, column(mine, p)] + from_core(stage, h, 1, p)
        line_copy(h, stage, p).wait_recv()
        return pack(values + line_in[h, stage, p].reshape(depth, piece).astype(f32))

    def flat(values):
        return values.reshape(depth, values.shape[2]).astype(f32)

    def forward_part(h, slot, where, many, rows):
        dims = (((1,), (1,)), ((), ()))
        out = None
        for p in many:
            values = model[h, slot, p]
            for number, side in enumerate((values.reshape(depth, piece), turned(values, -1))):
                update = lax.dot_general(
                    gains[number, rows, column(where, p)], side, dims,
                    preferred_element_type=f32,
                )
                out = update if out is None else out + update
        return out

    def forward(h, slot, where, many, first=False):
        tile_rows = 2 * width if chunks % 2 == 0 else width

        def body(i):
            rows = pl.ds(pl.multiple_of(i * tile_rows, tile_rows), tile_rows)
            update = forward_part(h, slot, where, many, rows)
            product[h, rows] = update if first else product[h, rows] + update

        loop(0, points // tile_rows, body)

    def share(h, p):
        share_copy(h, 1, p).start()
        share_copy(h, 0, p).start()

    def keep(h, p):
        values = reduced(0, h, p)
        if mixing:
            summed[h, p] = values
            send_all(RETURNED, h, sent, summed_in, p)
        else:
            model[h, 0, p] = values
            share(h, p)
            if h == 0:
                send_all(RETURNED, h, sent, summed_in, p)
            held = flat(values)
            stats[0] += folded(held * held)

    def mix(h, p):
        receive_all(RETURNED, h, sent, summed_in, p)
        arrived = summed_in[h, p].reshape(depth, piece)
        values = jnp.dot(same[...], arrived, preferred_element_type=f32)
        mixed_out[h, p] = values.astype(bf16).reshape(n, double, piece)
        send_all(MIXED, h, mixed_out, model.at[:, 0], p)

    def unmix(h, p):
        receive_all(MIXED, h, mixed_out, model.at[:, 0], p)
        share(h, p)

    def own_forward(h):
        forward(h, 0, mine, range(pieces), first=True)
        for p in range(pieces):
            share_copy(h, 0, p).wait_recv()
        forward(h, 1, core, range(pieces))

    def relay(h, p):
        share_copy(h, 1, p).wait_recv()
        share_copy(h, 2, p).start()

    def from_line(h, p):
        relay(h, p)
        if p % 2:
            forward(h, 2, line, (p - 1, p))
        elif p == pieces - 1:
            forward(h, 2, line, (p,))

    def imaging(h):
        for p in range(pieces):
            share_copy(h, 2, p).wait_recv()

        def body(i):
            values = product[h, part(i)] + forward_part(h, 3, corner, range(pieces), part(i))
            image_out[h, i] = values.T.astype(bf16).reshape(n, double, width)
            send_all(IMAGED, h, image_out, image_in, i)

        loop(0, chunks, body)

    def again(h, i):
        receive_all(IMAGED, h, image_out, image_in, i)
        arrived = image_in[h, i].reshape(depth, width)
        for j in range(0, count, GROUP):
            weight = window[i, span(h * count + j, GROUP)].astype(f32)
            rows = slice(j * length, (j + GROUP) * length)
            values = jnp.dot(gather[rows], arrived, preferred_element_type=f32) * weight
            stats[1] += folded(values * values)
            tapered[rows] = (values * weight).astype(bf16)
        transform(second_out, h, i)
        send_all(SECOND, h, second_out, second_in, i)

    def change(h, p):
        values = reduced(1, h, p)
        normal[h, p] = values
        send_all(CHANGED, h, normal, normal_in, p)
        if not mixing:
            held = flat(values)
            stats[2] += folded(held * flat(model[h, 0, p]))
            stats[3] += folded(held * held)

    prepare(0, 0)
    pl.semaphore_wait(barrier, n + 2)
    send_all(RECORDED, 0, first_out, first_in, 0)
    for h in both:
        loop(0 if h else 1, chunks, lambda i: record(h, i))
    for number in (3, 4, 5):
        keep_copy(number).start()
    for i in range(last):
        accumulate(0, 0, i)
    reduce_out(0, 0)
    def each(body, h):
        loop(0, pieces, lambda p: body(h, p))

    for h in both:
        more = h + 1 < halves
        if more:
            for i in range(last):
                accumulate(0, h + 1, i)
            reduce_core(0, h + 1)
        if not mixing or h == 0:
            each(keep, h)
        if more:
            reduce_line(0, h + 1)
        if mixing:
            if h == 0:
                each(mix, h)
            if more:
                each(keep, h + 1)
            each(unmix, h)
            if more:
                each(mix, h + 1)
        own_forward(h)
        for p in range(max(chunks, pieces)):
            if h and p < chunks:
                again(h - 1, p)
            if p < pieces:
                from_line(h, p)
        imaging(h)
    other = halves - 1
    for i in range(last):
        accumulate(1, 0, i)
        if i and i <= chunks // 2:
            again(other, i - 1)
    reduce_out(1, 0)
    for i in range(chunks // 2 if last > chunks // 2 else max(last - 1, 0), chunks):
        again(other, i)
    for h in range(1, halves):
        if not mixing:
            loop(0, pieces, lambda p: send_all(RETURNED, h, sent, summed_in, p))
        for i in range(last):
            accumulate(1, h, i)
            if i < pieces:
                change(h - 1, i)
        reduce_out(1, h)
        for p in range(last, pieces):
            change(h - 1, p)
    each(change, other)
    keep_copy(1).start()
    if mixing:

        def norms(h, p):
            receive_all(CHANGED, h, normal, normal_in, p)
            before = summed_in[h, p].reshape(depth, piece)
            after = normal_in[h, p].reshape(depth, piece)
            mixed_before = jnp.dot(same[...], before, preferred_element_type=f32)
            mixed_after = jnp.dot(same[...], after, preferred_element_type=f32)
            stats[0] += folded(before.astype(f32) * mixed_before)
            stats[2] += folded(after.astype(f32) * mixed_before)
            stats[3] += folded(after.astype(f32) * mixed_after)

        keep_copy(0).start()
        for h in both:
            loop(0, pieces, lambda p: norms(h, p))
    else:
        for h in both:
            loop(0, pieces, lambda p: receive_all(RETURNED, h, sent, summed_in, p))
        keep_copy(0).start()

    def stats_copy(which, peer):
        return pltpu.make_async_remote_copy(
            src_ref=stats,
            dst_ref=stats_in.at[which],
            send_sem=stats_out_sem.at[which],
            recv_sem=stats_in_sem.at[which],
            device_id={"ma": peer},
            device_id_type=MESH,
        )

    near = [stats_copy(which, peer) for which, peer in enumerate((core, line, corner))]
    for copy in near:
        copy.start()
    for copy in near:
        copy.wait_recv()
    stats_in[3] = (stats[...] + stats_in[0]) + (stats_in[1] + stats_in[2])

    def stats_across(peer, slot):
        return pltpu.make_async_remote_copy(
            src_ref=stats_in.at[3],
            dst_ref=stats_all.at[slot],
            send_sem=stats_out_sem.at[3],
            recv_sem=stats_in_sem.at[3],
            device_id={"gx": peer},
            device_id_type=MESH,
        )

    loop(1, n, lambda k: stats_across(lax.rem(me + k, n), me).start())
    stats_all[me] = stats_in[3]
    others = stats_all.at[pl.ds(0, n - 1)]
    every = pltpu.make_async_remote_copy(
        src_ref=others,
        dst_ref=others,
        send_sem=stats_out_sem.at[3],
        recv_sem=stats_in_sem.at[3],
        device_id={"gx": lax.rem(me + 1, n)},
        device_id_type=MESH,
    )
    if not mixing:
        for h in both:
            loop(0, pieces, lambda p: receive_all(CHANGED, h, normal, normal_in, p))
    keep_copy(2).start()
    every.wait_recv()
    sums_ref[...] = jnp.sum(stats_all[...], axis=0)

    for copy in near:
        copy.wait_send()
    every.wait_send()
    finish_all(RECORDED, first_out, first_in, chunks)
    finish_all(RETURNED, sent, summed_in, pieces)
    finish_all(IMAGED, image_out, image_in, chunks)
    finish_all(SECOND, second_out, second_in, chunks)
    finish_all(CHANGED, normal, normal_in, pieces)
    if mixing:
        finish_all(MIXED, mixed_out, model.at[:, 0], pieces)

    def finish(src, dst, sem, peer):
        pltpu.make_async_remote_copy(
            src_ref=src,
            dst_ref=dst,
            send_sem=sem,
            recv_sem=stats_in_sem.at[0],
            device_id={"ma": peer},
            device_id_type=MESH,
        ).wait_send()

    finish(core_out, core_in, core_out_sem, core)
    finish(line_out, line_in, line_out_sem, line)
    for which, peer in ((0, core), (1, line), (2, core)):
        finish(model.at[:, 0], model.at[:, 1], share_out_sem.at[which], peer)
    for number in range(6):
        keep_copy(number).wait()


def iteration(outer, inner, mixing, freq_bins, recorded, kernel, window_start, window_stop):
    points, sources, length = recorded.shape
    columns = kernel.shape[2]
    halves = PARTS
    count = sources // halves
    double = 2 * count
    depth = outer * double
    block = columns // inner
    width, piece = min(256, points), min(256, block)
    chunks, pieces = points // width, block // piece
    f32, bf16 = jnp.float32, jnp.bfloat16
    by_chunk = (halves, chunks, outer, double, width)
    by_piece = (halves, pieces, outer, double, piece)
    stack = by_piece[1:]
    vmem = pl.BlockSpec(memory_space=pltpu.VMEM)
    hbm = pl.BlockSpec(memory_space=pl.ANY)
    dma = pltpu.SemaphoreType.DMA
    exchanges = 6 if mixing else 5
    extra = by_piece if mixing else (halves, 1, 1, 16, 128)
    return pl.pallas_call(
        functools.partial(iteration_kernel, outer, inner, mixing),
        out_shape=[
            jax.ShapeDtypeStruct(by_piece, bf16),
            jax.ShapeDtypeStruct(by_chunk, bf16),
            jax.ShapeDtypeStruct(by_piece, bf16),
            jax.ShapeDtypeStruct((4, 8, 128), f32),
            jax.ShapeDtypeStruct((2 * sources, points), f32),
            jax.ShapeDtypeStruct((depth, count * length), bf16),
            jax.ShapeDtypeStruct((count * length, depth), bf16),
        ],
        in_specs=[pl.BlockSpec(memory_space=pltpu.SMEM), hbm, hbm, vmem, vmem],
        out_specs=[hbm, hbm, hbm, vmem, hbm, hbm, hbm],
        scratch_shapes=[
            pltpu.VMEM((sources, points, length), f32),
            pltpu.VMEM((2, points, columns), bf16),
            pltpu.VMEM((chunks, sources * length, width), bf16),
            pltpu.VMEM((2 * sources, points), f32),
            pltpu.VMEM((depth, count * length), bf16),
            pltpu.VMEM((count * length, depth), bf16),
            pltpu.VMEM((count * length, width), bf16),
            pltpu.VMEM(by_chunk, bf16),
            pltpu.VMEM(by_chunk, bf16),
            pltpu.VMEM(by_chunk, bf16),
            pltpu.VMEM(by_chunk, bf16),
            pltpu.VMEM((halves, depth, columns), f32),
            pltpu.VMEM((halves, points, depth), f32),
            pltpu.VMEM(by_chunk, bf16),
            pltpu.VMEM(by_chunk, bf16),
            pltpu.VMEM((halves, 2, 2) + stack, bf16),
            pltpu.VMEM((halves, 2, 2) + stack, bf16),
            pltpu.VMEM((halves, 2) + stack, bf16),
            pltpu.VMEM((halves, 2) + stack, bf16),
            pltpu.VMEM((halves, 4) + stack, bf16),
            pltpu.VMEM(extra, bf16),
            pltpu.VMEM(by_piece, bf16),
            pltpu.VMEM(by_piece, bf16),
            pltpu.VMEM(by_piece, bf16),
            pltpu.VMEM(extra, bf16),
            pltpu.VMEM((depth, depth) if mixing else (16, 128), bf16),
            pltpu.VMEM((4, 8, 128), f32),
            pltpu.VMEM((4, 4, 8, 128), f32),
            pltpu.VMEM((outer, 4, 8, 128), f32),
            dma((halves, chunks)),
            dma((chunks,)),
            dma((6,)),
            dma((exchanges * halves,)),
            dma((exchanges * halves, max(chunks, pieces))),
            dma,
            dma((halves, 2, 2, pieces)),
            dma,
            dma((halves, 2, pieces)),
            dma((3,)),
            dma((halves, 3, pieces)),
            dma((4,)),
            dma((4,)),
        ],
        compiler_params=pltpu.CompilerParams(
            collective_id=6 if mixing else 5,
            has_side_effects=True,
            vmem_limit_bytes=67_000_000,
        ),
        name="iteration_mixed" if mixing else "iteration",
    )(freq_bins, recorded, kernel, window_start, window_stop)


def write_kernel(
    sums_ref, rec_ref, win_ref, spread_ref, gather_ref, ret_ref, ima_ref, cha_ref,
    sol_ref, res_ref, dir_ref, traces, solved, rest, ahead, in_sem, out_sem,
):
    sources, points, length = traces.shape
    halves, chunks, outer, double, width = ima_ref.shape
    depth = outer * double
    count = sources // halves
    f32, bf16 = jnp.float32, jnp.bfloat16

    def part(i):
        return pl.ds(pl.multiple_of(i * width, width), width)

    def load(i, s):
        return pltpu.make_async_copy(
            rec_ref.at[part(i), s], traces.at[s, part(i)], in_sem.at[i]
        )

    staged = ((solved, sol_ref), (ahead, dir_ref), (rest, res_ref))

    def store(number, i, s):
        src, dst = staged[number]
        return pltpu.make_async_copy(
            src.at[s, part(i)], dst.at[part(i), s], out_sem.at[number]
        )

    loop(0, chunks, lambda i: loop(0, sources, lambda s: load(i, s).start()))
    norm_start, norm_data = jnp.sum(sums_ref[0]), jnp.sum(sums_ref[1])
    cross, norm_change = jnp.sum(sums_ref[2]), jnp.sum(sums_ref[3])
    step_size = norm_start / (norm_data + epsilon)
    norm_final = norm_start - 2.0 * step_size * cross + step_size * step_size * norm_change
    ratio = norm_final / (norm_start + epsilon)
    samples = iota((length, width), 0).astype(f32) * (1.0 / RAMP)

    def chunk(i):
        place = traces.at[:, part(i)]
        pltpu.make_async_copy(place, place, in_sem.at[i]).wait()
        for h in range(halves):
            before = ret_ref[h, i].reshape(depth, width).astype(f32).T.astype(bf16)
            after = cha_ref[h, i].reshape(depth, width).astype(f32).T.astype(bf16)
            arrived = ima_ref[h, i].reshape(depth, width)

            def pair(j):
                spans = pl.ds(pl.multiple_of(j * 2 * length, length), 2 * length)
                table = spread_ref[:, spans]
                first = h * count + 2 * j
                for r in range(0, width, 128):
                    rows = pl.ds(pl.multiple_of(i * width + r, 128), 128)
                    gradient = jnp.dot(before[r : r + 128], table, preferred_element_type=f32)
                    change = jnp.dot(after[r : r + 128], table, preferred_element_type=f32)
                    for k in range(2):
                        here = slice(k * length, (k + 1) * length)
                        g, c = gradient[:, here], change[:, here]
                        solved[first + k, rows] = step_size * g
                        ahead[first + k, rows] = (g - step_size * c) + ratio * g
                for k in range(2):
                    s = first + k
                    store(0, i, s).start()
                    store(1, i, s).start()
                    rising = jnp.clip(samples + win_ref[pl.ds(s, 1), part(i)], 0.0, 1.0)
                    falling = jnp.clip(
                        win_ref[pl.ds(sources + s, 1), part(i)] - samples, 0.0, 1.0
                    )
                    spans = pl.ds(pl.multiple_of((2 * j + k) * length, length), length)
                    image = jnp.dot(gather_ref[spans], arrived, preferred_element_type=f32)
                    image = (rising * falling) * image
                    rest[s, part(i)] = traces[s, part(i)] - step_size * image.T
                    store(2, i, s).start()

            def some(j):
                for k in range(4):
                    pair(4 * j + k)

            loop(0, count // 8, some)

    loop(0, chunks, chunk)
    for number in range(3):
        src = staged[number][0]
        pltpu.make_async_copy(src, src, out_sem.at[number]).wait()


def write(recorded, returned, imaged, changed, sums, windows, spread, gather):
    points, sources, length = recorded.shape
    halves, chunks, outer, double, width = imaged.shape
    depth = outer * double
    vmem = pl.BlockSpec(memory_space=pltpu.VMEM)
    hbm = pl.BlockSpec(memory_space=pl.ANY)
    f32 = jnp.float32
    staged = pltpu.VMEM((sources, points, length), f32)
    return pl.pallas_call(
        write_kernel,
        out_shape=[jax.ShapeDtypeStruct(recorded.shape, f32)] * 3,
        in_specs=[vmem, hbm] + [vmem] * 6,
        out_specs=[hbm] * 3,
        scratch_shapes=[
            staged,
            staged,
            staged,
            staged,
            pltpu.SemaphoreType.DMA((chunks,)),
            pltpu.SemaphoreType.DMA((3,)),
        ],
        compiler_params=pltpu.CompilerParams(vmem_limit_bytes=56 * 1024 * 1024),
        cost_estimate=pl.CostEstimate(
            flops=6 * points * sources * depth * length,
            bytes_accessed=16 * points * sources * length,
            transcendentals=0,
        ),
        name="write",
    )(sums, recorded, windows, spread, gather, returned, imaged, changed)


def fused(outer, inner, recorded, kernel, freq_bins, window_start, window_stop):
    same = freq_bins[:, None] == freq_bins[None, :]
    repeated = jnp.sum(same.astype(jnp.int32)) > freq_bins.shape[0]
    gains = kernel.reshape(2, kernel.shape[2], kernel.shape[3])
    results = lax.cond(
        repeated,
        lambda *x: tuple(iteration(outer, inner, True, *x)),
        lambda *x: tuple(iteration(outer, inner, False, *x)),
        freq_bins, recorded, gains, window_start.T, window_stop.T,
    )
    return tuple(write(recorded, *results))


def fits(outer, inner, recorded, kernel):
    points, sources, length = recorded.shape
    columns = kernel.shape[3]
    return (
        inner == 4
        and kernel.shape[1] == 1
        and columns == inner * points
        and sources % (PARTS * 8) == 0
        and length % 128 == 0
        and points % 256 == 0
        and outer * 2 * (sources // PARTS) % 128 == 0
        and points * (4 * columns + 6 * sources * length) < 30_000_000
    )


def per_device(outer, inner, recorded, kernel, freq_bins, window_start, window_stop):
    if fits(outer, inner, recorded, kernel):
        return fused(outer, inner, recorded, kernel, freq_bins, window_start, window_stop)
    length = recorded.shape[2]
    table = phase_table(freq_bins, length)
    weights = taper_weights(window_start, window_stop, length)
    flat_kernel = kernel.reshape(2 * kernel.shape[2], kernel.shape[3])

    data = by_frequency(exchange(to_spectra(weights * recorded, table), outer, 0), outer)
    adjoint = adjoint_product(data, flat_kernel, inner)
    returned = lax.all_to_all(
        by_source(adjoint, outer), "gx", split_axis=0, concat_axis=0, tiled=True
    )

    same = freq_bins[:, None] == freq_bins[None, :]
    repeated = jnp.sum(same.astype(jnp.int32)) > freq_bins.shape[0]

    def combined(spectra):
        parts = lax.all_to_all(
            by_source(spectra, outer), "gx", split_axis=0, concat_axis=0, tiled=True
        )
        mixed = jnp.einsum(
            "gf,fxa->gxa",
            same.astype(jnp.bfloat16),
            parts,
            preferred_element_type=jnp.float32,
        ).astype(jnp.bfloat16)
        back = lax.all_to_all(mixed, "gx", split_axis=0, concat_axis=0, tiled=True)
        return by_frequency(back, outer)

    model = lax.cond(repeated, combined, lambda spectra: spectra, adjoint)
    outgoing = by_source(forward_product(model, flat_kernel, inner), outer)
    imaged = exchange(outgoing, outer, 1)
    image = weights * to_traces(imaged, table)
    second = by_frequency(exchange(to_spectra(weights * image, table), outer, 2), outer)
    normal = adjoint_product(second, flat_kernel, inner)
    changed = exchange(by_source(normal, outer), outer, 3)

    double, points = returned.shape[1:]
    depth = freq_bins.shape[0] * double
    eye = jnp.eye(double, dtype=jnp.bfloat16)
    mixing = (same.astype(jnp.bfloat16)[:, None, :, None] * eye[None, :, None, :]).reshape(
        depth, depth
    )
    flat_g = returned.reshape(depth, points)
    flat_h = changed.reshape(depth, points)
    mixed_g = jnp.dot(mixing, flat_g, preferred_element_type=jnp.float32)
    mixed_h = jnp.dot(mixing, flat_h, preferred_element_type=jnp.float32)
    sums = jnp.stack(
        [
            jnp.sum(flat_g.astype(jnp.float32) * mixed_g),
            jnp.sum(image * image),
            jnp.sum(mixed_g * flat_h.astype(jnp.float32)),
            jnp.sum(flat_h.astype(jnp.float32) * mixed_h),
        ]
    )
    sums = total(jnp.broadcast_to(jnp.tile(sums, 2)[:, None], (8, 128)), outer, inner, 4)
    if recorded.shape[1] % 8 == 0:
        return tuple(
            final_step(
                sums, recorded, window_start, window_stop, returned, imaged, changed, table
            )
        )
    gradient = to_traces(returned, table)
    change = to_traces(changed, table)
    norm_start, norm_data, cross, norm_change = sums[0, 0], sums[1, 0], sums[2, 0], sums[3, 0]
    step_size = norm_start / (norm_data + epsilon)
    norm_final = norm_start - 2.0 * step_size * cross + step_size * step_size * norm_change
    solution = step_size * gradient
    residual = recorded - step_size * image
    direction = gradient - step_size * change + norm_final / (norm_start + epsilon) * gradient
    return (solution, residual, direction)


def solution(mesh):
    in_specs = (P("ma", "gx", None), P(None, "gx", "ma", None), P(), P("ma", "gx"), P("ma", "gx"))
    out_specs = (P("ma", "gx", None), P("ma", "gx", None), P("ma", "gx", None))
    return jax.shard_map(
        functools.partial(per_device, mesh.shape["gx"], mesh.shape["ma"]),
        mesh=mesh,
        in_specs=in_specs,
        out_specs=out_specs,
        check_vma=False,
    )
```
